256 devices in a mesh: pipe: 2 (over core), seq: 16 (over z, x_hi), tp: 8 (over y, x_lo).
Axes of the slice: x: 4 (x_hi: 2, x_lo: 2; x = x_hi * 2 + x_lo), y: 4, z: 8, core: 2. Of those that a mesh axis runs over, the one named last changes fastest.
Arguments:
- hidden_in: bfloat16 [1, 8192, 2560], P(None, ('seq', 'tp')), may hold values from -6 to 6
- doc_ids: int32 [1, 8192], P(None, 'seq'), may hold values from 0 to 1, never falling along the last dimension, each value on 1 to 6144 neighbouring positions
- norm_gain: float32 [2, 2560], P('pipe'), may hold values from 0.1 to 1.9
- in_zx: bfloat16 [2, 2560, 2, 5120], P('pipe', None, None, 'tp'), may hold values from -0.125 to 0.125
- in_bc: bfloat16 [2, 2560, 256], P('pipe'), may hold values from -0.125 to 0.125
- in_dt: bfloat16 [2, 2560, 80], P('pipe', None, 'tp'), may hold values from -0.125 to 0.125
- conv_x: float32 [2, 4, 5120], P('pipe', None, 'tp'), may hold values from -3 to 3
- conv_bc: float32 [2, 4, 256], P('pipe'), may hold values from -3 to 3
- bias_x: float32 [2, 5120], P('pipe', 'tp'), may hold values from -3 to 3
- bias_bc: float32 [2, 256], P('pipe'), may hold values from -3 to 3
- dt_bias: float32 [2, 80], P('pipe', 'tp'), may hold values from -2 to 1
- a_log: float32 [2, 80], P('pipe', 'tp'), may hold values from -12 to 0, as said below
- d_skip: float32 [2, 80], P('pipe', 'tp'), may hold values from 0.5 to 1.5
- gated_gain: float32 [2, 5120], P('pipe', 'tp'), may hold values from 0.1 to 1.9
- out_w: bfloat16 [2, 5120, 2560], P('pipe', 'tp'), may hold values from -0.078125 to 0.078125
Outputs:
- section_out: bfloat16 [2, 1, 8192, 2560], P('pipe', None, ('seq', 'tp'))
The draws below stay inside these ranges and needn't reach their ends.
Inputs may be any that keep to these rules, and one draw needn't show every extreme that they name: `doc_ids`: in each row the document numbers start at 0, never fall, and rise by one where a new document begins; every document spans 1 to 6144 positions. `a_log`: logarithms of rates between 0.5 / 8192 and 1.
All inputs are finite; a program needn't handle non-finite values.
Results may differ from the reference program's by a relative error of at most 0.02.
Values may be sent and summed in bfloat16 or wider, within the bound.
A program may use at most 128 MiB of HBM per device.

```python
import math
import jax
import jax.numpy as jnp
import numpy as np
from jax import lax

D = 2560
E = 5120
H = 80
HEADDIM = 64
NS = 128
KW = 4
BLOCK = 256
MB = 1
SEQLEN = 8192
LAYERS = 2


def draw_a_log(key, part):
    uniform_draw = jax.random.uniform(key, (LAYERS, H), jnp.float32)
    lowest = math.log(0.5 / SEQLEN)
    return (lowest * (1.0 - uniform_draw)).astype(jnp.float32)


def block_scale(stream_key, extent, pieces, least, high):
    def one(axis_at, blocks):
        steps = jax.random.uniform(jax.random.fold_in(jax.random.fold_in(stream_key, 6), axis_at), (blocks,), jnp.float32, least / len(pieces), high / len(pieces))
        return jnp.repeat(jnp.exp(steps), extent[axis_at] // blocks).reshape((-1,) + (1,) * (len(extent) - axis_at - 1))

    loudness = one(*pieces[0])
    for cut in pieces[1:]:
        loudness = loudness * one(*cut)
    return loudness


def profile(count, total, bound, slope):
    portions = [(1 << 20) // math.isqrt(standing ** slope) + 1 for standing in range(2, count + 1)]
    spare, given = total - bound - (count - 1), [1] * (count - 1)
    while spare > 0:
        movable = [i for i in range(count - 1) if given[i] < bound]
        whole, remaining = sum([portions[i] for i in movable]), spare
        for i in movable:
            addition = min(bound - given[i], max(1, remaining * portions[i] // whole), spare)
            given[i] = given[i] + addition
            spare = spare - addition
    return np.array([bound] + given)


def uneven(own_key, number_of, total, limit, lean):
    if number_of == 2:
        one = jax.random.randint(own_key, (), max(1, total - limit), min(limit, total - 1) + 1)
        return jnp.stack([one, total - one])
    tallies = jnp.asarray(profile(number_of, total, limit, lean), jnp.int32)
    couples = (number_of - 1) // 2
    source_of, taker = tallies[1:1 + 2 * couples:2], tallies[2:2 + 2 * couples:2]
    slack = jnp.minimum(source_of - 1, limit - taker)
    passed = jax.random.randint(jax.random.fold_in(own_key, 1), (couples,), 0, 1 << 20) % (slack + 1)
    tallies = tallies.at[1:1 + 2 * couples:2].set(source_of - passed).at[2:2 + 2 * couples:2].set(taker + passed)
    return tallies[jax.random.permutation(jax.random.fold_in(own_key, 2), number_of)]


def gaussian(key, extent, scale, bound, shards=(), dtype=jnp.bfloat16):
    entries = scale * jax.random.normal(key, extent, jnp.float32)
    if shards:
        entries = entries * block_scale(key, extent, shards, -0.22, 0.18)
    return jnp.clip(entries, -bound, bound).astype(dtype)


def setup_inputs(seed: int = 0) -> dict:
    arg_keys = jax.random.split(jax.random.key(seed), 16)
    hidden_in = gaussian(arg_keys[0], (MB, SEQLEN, D), 1.0, 6.0, ((1, 128),))
    doc_ids = jax.vmap(lambda own: jnp.searchsorted(jnp.cumsum(uneven(own, 2, SEQLEN, 3 * SEQLEN // 4, 0)), jnp.arange(SEQLEN), side="right"))(jax.random.split(arg_keys[1], MB)).reshape((MB, SEQLEN)).astype(jnp.int32)
    norm_gain = jnp.clip(1.0 + 0.18 * jax.random.normal(arg_keys[2], (LAYERS, D), jnp.float32), 0.1, 1.9)
    in_zx = gaussian(arg_keys[3], (LAYERS, D, 2, E), D ** -0.5, 0.125, ((0, 2), (3, 8)))
    in_bc = gaussian(arg_keys[4], (LAYERS, D, 2 * NS), D ** -0.5, 0.125, ((0, 2),))
    in_dt = gaussian(arg_keys[5], (LAYERS, D, H), D ** -0.5, 0.125, ((0, 2), (2, 8)))
    conv_x = gaussian(arg_keys[6], (LAYERS, KW, E), KW ** -0.5, 3.0, ((0, 2), (2, 8)), jnp.float32)
    conv_bc = gaussian(arg_keys[7], (LAYERS, KW, 2 * NS), KW ** -0.5, 3.0, ((0, 2),), jnp.float32)
    bias_x = gaussian(arg_keys[8], (LAYERS, E), 0.5, 3.0, ((0, 2), (1, 8)), jnp.float32)
    bias_bc = gaussian(arg_keys[9], (LAYERS, 2 * NS), 0.5, 3.0, ((0, 2),), jnp.float32)
    dt_bias = jnp.clip(-2.0 + 3.0 * jax.random.uniform(arg_keys[10], (LAYERS, H), jnp.float32) ** block_scale(arg_keys[10], (LAYERS, H), ((0, 2), (1, 8)), -0.2, 0.2), -2.0, 1.0)
    a_log = draw_a_log(jax.random.fold_in(arg_keys[15], 71), 0)
    d_skip = jnp.clip(0.5 + 1.0 * jax.random.uniform(arg_keys[12], (LAYERS, H), jnp.float32) ** block_scale(arg_keys[12], (LAYERS, H), ((0, 2), (1, 8)), -0.2, 0.2), 0.5, 1.5)
    gated_gain = jnp.clip(1.0 + 0.18 * jax.random.normal(arg_keys[13], (LAYERS, E), jnp.float32), 0.1, 1.9)
    out_w = gaussian(arg_keys[14], (LAYERS, E, D), E ** -0.5, 0.078125, ((0, 2), (1, 8)))
    return dict(hidden_in=hidden_in, doc_ids=doc_ids, norm_gain=norm_gain, in_zx=in_zx, in_bc=in_bc, in_dt=in_dt, conv_x=conv_x, conv_bc=conv_bc, bias_x=bias_x, bias_bc=bias_bc, dt_bias=dt_bias, a_log=a_log, d_skip=d_skip, gated_gain=gated_gain, out_w=out_w)


epsilon = 1e-05
highest = lax.Precision.HIGHEST

def conv_mix(row_block, edge_rows, row_ids, edge_ids, weight, shift_bias):
    padded = jnp.concatenate([edge_rows, row_block], 0)
    padded_ids = jnp.concatenate([edge_ids, row_ids], 0)
    row_count = row_block.shape[0]
    running = jnp.zeros_like(row_block) + shift_bias[None, :]
    for offset in range(weight.shape[0]):
        keep_mask = (padded_ids[offset:offset + row_count] == row_ids).astype(jnp.float32)
        running = running + keep_mask[:, None] * weight[offset][None, :] * padded[offset:offset + row_count]
    return jax.nn.silu(running)

def block_step(state_in, inputs, decay_rates):
    x_block, step_sizes, b_block, c_block, seg_block, prev_id = inputs
    log_decay = jnp.cumsum(step_sizes * decay_rates[:, None], axis=1)
    block_length = seg_block.shape[0]
    causal_mask = jnp.arange(block_length)[:, None] >= jnp.arange(block_length)[None, :]
    same_doc = causal_mask & (seg_block[:, None] == seg_block[None, :])
    spread = log_decay[:, :, None] - log_decay[:, None, :]
    mixing = jnp.where(same_doc[None], jnp.exp(jnp.where(same_doc[None], spread, 0.0)), 0.0)
    gram_matrix = jnp.dot(c_block, b_block.T, precision=highest)
    weights = mixing * gram_matrix[None] * step_sizes[:, None, :]
    outputs = jnp.einsum('hps,hts->hpt', x_block, weights, precision=highest)
    carried = (seg_block == prev_id).astype(jnp.float32)
    outputs = outputs + jnp.exp(log_decay)[:, None, :] * carried[None, None, :] * jnp.einsum('hpn,tn->hpt', state_in, c_block, precision=highest)
    end_weight = jnp.exp(log_decay[:, -1:] - log_decay) * (seg_block == seg_block[-1]).astype(jnp.float32)[None, :] * step_sizes
    fresh_state = jnp.einsum('hps,sn->hpn', x_block * end_weight[:, None, :], b_block, precision=highest)
    keep_all = jnp.exp(log_decay[:, -1]) * (seg_block[-1] == prev_id).astype(jnp.float32)
    return (keep_all[:, None, None] * state_in + fresh_state, outputs)

def mamba_layer(hidden, row_ids, norm_scale, weight_zx, weight_bc, weight_dt, kernel_x, kernel_bc, offset_x, offset_bc, dt_shift, log_rate, skip_scale, gate_scale, weight_out):
    hidden_f = hidden.astype(jnp.float32)
    normed = (hidden_f * lax.rsqrt(lax.optimization_barrier(jnp.mean(hidden_f * hidden_f, axis=1, keepdims=True)) + epsilon) * norm_scale[None, :]).astype(jnp.bfloat16)
    gate_in = jnp.dot(normed, weight_zx[:, 0, :], preferred_element_type=jnp.float32)
    x_raw = jnp.dot(normed, weight_zx[:, 1, :], preferred_element_type=jnp.float32)
    bc_raw = jnp.dot(normed, weight_bc, preferred_element_type=jnp.float32)
    dt_raw = jnp.dot(normed, weight_dt, preferred_element_type=jnp.float32)
    pre_conv = jnp.concatenate([x_raw, bc_raw], 1)
    kernel = jnp.concatenate([kernel_x, kernel_bc], 1)
    kernel_bias = jnp.concatenate([offset_x, offset_bc], 0)
    edge_rows = jnp.zeros((KW - 1, E + 2 * NS), jnp.float32)
    edge_ids = jnp.full((KW - 1,), -1, jnp.int32)
    conv_out = conv_mix(pre_conv, edge_rows, row_ids, edge_ids, kernel, kernel_bias)
    x_heads = conv_out[:, :E].T.reshape(H, HEADDIM, SEQLEN)
    b_conv = conv_out[:, E:E + NS]
    c_conv = conv_out[:, E + NS:]
    step_sizes = jax.nn.softplus(dt_raw + dt_shift[None, :]).T
    decay_rates = -jnp.exp(log_rate)
    blocks = SEQLEN // BLOCK
    prev_ids = jnp.concatenate([row_ids[:1], row_ids[BLOCK - 1:SEQLEN - 1:BLOCK]], 0)
    stacked = (x_heads.reshape(H, HEADDIM, blocks, BLOCK).transpose(2, 0, 1, 3), step_sizes.reshape(H, blocks, BLOCK).transpose(1, 0, 2), b_conv.reshape(blocks, BLOCK, NS), c_conv.reshape(blocks, BLOCK, NS), row_ids.reshape(blocks, BLOCK), prev_ids)

    def scan_body(state_in, inputs):
        return block_step(state_in, inputs, decay_rates)
    final_state, outputs = lax.scan(scan_body, jnp.zeros((H, HEADDIM, NS), jnp.float32), stacked)
    outputs = outputs.transpose(1, 2, 0, 3).reshape(H, HEADDIM, SEQLEN)
    outputs = outputs + skip_scale[:, None, None] * x_heads
    gated_rows = outputs.reshape(E, SEQLEN).T * jax.nn.silu(gate_in)
    branch_in = (gated_rows * lax.rsqrt(lax.optimization_barrier(jnp.mean(gated_rows * gated_rows, axis=1, keepdims=True)) + epsilon) * gate_scale[None, :]).astype(jnp.bfloat16)
    return (hidden_f + jnp.dot(branch_in, weight_out, preferred_element_type=jnp.float32)).astype(jnp.bfloat16)

def reference(hidden_in, doc_ids, norm_gain, in_zx, in_bc, in_dt, conv_x, conv_bc, bias_x, bias_bc, dt_bias, a_log, d_skip, gated_gain, out_w):
    per_layer = [[None] * MB for layer_index in range(LAYERS)]
    for micro_index in range(MB):
        hidden = hidden_in[micro_index]
        row_ids = doc_ids[micro_index]
        for layer_index in range(LAYERS):
            hidden = mamba_layer(hidden, row_ids, norm_gain[layer_index], in_zx[layer_index], in_bc[layer_index], in_dt[layer_index], conv_x[layer_index], conv_bc[layer_index], bias_x[layer_index], bias_bc[layer_index], dt_bias[layer_index], a_log[layer_index], d_skip[layer_index], gated_gain[layer_index], out_w[layer_index])
            per_layer[layer_index][micro_index] = hidden
    return jnp.stack([jnp.stack(micro_list) for micro_list in per_layer])
```

```python
import functools

import jax
import jax.numpy as jnp
from jax import lax
from jax.experimental import pallas as pl
from jax.experimental.pallas import tpu as pltpu
from jax.sharding import PartitionSpec as P

BLOCK = 256
EPS = 1e-05
F32 = jnp.float32
BF16 = jnp.bfloat16
MESH = pl.DeviceIdType.MESH


def lanes_of(v, spread):
    hi = v.astype(BF16)
    lo = (v - hi.astype(F32)).astype(BF16)
    return jnp.dot(hi, spread, preferred_element_type=F32) + jnp.dot(
        lo, spread, preferred_element_type=F32
    )


def layer_kernel(
    geo,
    hidden_hbm,
    ids_ref,
    norm_gain,
    zx_hbm,
    bc_hbm,
    dt_hbm,
    conv_x,
    conv_bc,
    bias_x,
    bias_bc,
    dt_bias,
    a_log,
    d_skip,
    gated_gain,
    out_hbm,
    result,
    w_zx,
    w_bc,
    w_dt,
    w_out,
    hid,
    rows_all,
    pre,
    gate,
    xc,
    bcm,
    xp,
    acc,
    idc,
    dtp,
    prm,
    ldb,
    st,
    a_out,
    a_in,
    k_out,
    k_in,
    i_out,
    i_in,
    part,
    xl_in,
    ql,
    yl2,
    yl1,
    yr2,
    yr1,
    qr,
    qx,
    xr_in,
    sq_out,
    sq_in,
    sqc,
    send_sem,
    recv_sem,
    load_sem,
):
    n_seq, n_tp, n_y, d, el, nh, cl = geo
    pipe, seq, tp = lax.axis_index("pipe"), lax.axis_index("seq"), lax.axis_index("tp")
    y, xl = tp // 2, tp % 2
    rows = hid.shape[0]
    toks = n_tp * rows
    half = rows // 2
    n_blocks = toks // BLOCK
    ng = 128 // n_seq
    up, down = lax.rem(y + 1, n_y), lax.rem(y + n_y - 1, n_y)
    far = lax.rem(y + 2, n_y)
    at_up = {"tp": up * 2 + xl}
    at_down = {"tp": down * 2 + xl}
    at_x = {"tp": y * 2 + (1 - xl)}
    left, right = pl.ds(0, cl), pl.ds(cl, d - cl)
    counter = [0]
    sent = []

    def remote(src, dst, where):
        k = counter[0]
        counter[0] += 1
        copy = pltpu.make_async_remote_copy(
            src_ref=src,
            dst_ref=dst,
            send_sem=send_sem.at[k],
            recv_sem=recv_sem.at[k],
            device_id=where,
            device_id_type=MESH,
        )
        return copy

    def push(src, dst, where):
        copy = remote(src, dst, where)
        copy.start()
        sent.append(copy)
        return copy

    loads = [
        pltpu.make_async_copy(s, t, load_sem.at[k])
        for k, (s, t) in enumerate(
            [(zx_hbm, w_zx), (bc_hbm, w_bc), (dt_hbm, w_dt), (out_hbm, w_out)]
        )
    ]
    first_load = pltpu.make_async_copy(hidden_hbm, hid, load_sem.at[4])

    @pl.when(pipe == 0)
    def _():
        first_load.start()

    for copy in loads:
        copy.start()

    barrier = pltpu.get_barrier_semaphore()
    pl.semaphore_signal(barrier, inc=1, device_id={"pipe": 1 - pipe}, device_id_type=MESH)
    for k in range(1, n_tp):
        pl.semaphore_signal(
            barrier, inc=1, device_id={"tp": lax.rem(tp + k, n_tp)}, device_id_type=MESH
        )
    for k in range(1, n_seq):
        pl.semaphore_signal(
            barrier, inc=1, device_id={"seq": lax.rem(seq + k, n_seq)}, device_id_type=MESH
        )

    prm[...] = jnp.zeros_like(prm)
    prm[0:1, 0:nh] = dt_bias[...]
    prm[1:2, 0:nh] = -jnp.exp(a_log[...])
    prm[2:3, 0:nh] = d_skip[...]
    ids_row = ids_ref[...].astype(F32)
    idc[8 : 8 + toks, :] = jnp.broadcast_to(ids_row, (128, toks)).T
    head = lax.broadcasted_iota(jnp.int32, (128, el), 0)
    lane = lax.broadcasted_iota(jnp.int32, (128, el), 1)
    spread = jnp.where((lane // 64) == head, 1.0, 0.0).astype(BF16)

    pl.semaphore_wait(barrier, n_tp + n_seq - 1)
    nxt = {"seq": lax.rem(seq + 1, n_seq)}
    id_edge = push(idc.at[pl.ds(toks, 8)], idc.at[pl.ds(0, 8)], nxt)
    handoff = remote(result, hid, {"pipe": 1 - pipe})

    @pl.when(pipe == 0)
    def _():
        first_load.wait()

    @pl.when(pipe == 1)
    def _():
        handoff.wait_recv()

    h = hid[...].astype(F32)
    scale = lax.rsqrt(jnp.mean(h * h, axis=1, keepdims=True) + EPS)
    rows_all[tp] = (h * scale * norm_gain[...]).astype(BF16)

    def slot(yy, xx, cols, r0=0, n=rows):
        return rows_all.at[yy * 2 + xx, pl.ds(r0, n), cols]

    def hop(yy, xx, cols, where, r0=0, n=rows):
        s = slot(yy, xx, cols, r0, n)
        return push(s, s, where)

    other = 1 - xl
    u1, d1 = hop(y, xl, left, at_up), hop(y, xl, left, at_down)
    x1 = hop(y, xl, right, at_x)
    u2, d2 = hop(y, xl, right, at_up), hop(y, xl, right, at_down)
    x2 = hop(y, xl, left, at_x)
    x1.wait_recv()
    u3, d3 = hop(y, other, right, at_up), hop(y, other, right, at_down)
    u1.wait_recv()
    u4 = hop(down, xl, left, at_up, 0, half)
    x3 = hop(down, xl, left, at_x)
    d1.wait_recv()
    d4 = hop(up, xl, left, at_down, half, half)
    x4 = hop(up, xl, left, at_x)
    u2.wait_recv()
    u3.wait_recv()
    u5 = hop(down, 0, right, at_up)
    d2.wait_recv()
    d3.wait_recv()
    d5 = hop(up, 1, right, at_down)
    u4.wait_recv()
    d4.wait_recv()
    x5 = hop(far, xl, left, at_x)
    id_edge.wait_recv()
    idc[0:8, :] = jnp.where(seq > 0, idc[0:8, :], -1.0)
    loads[0].wait()
    loads[1].wait()
    loads[2].wait()
    for copy in (x2, x3, x4, u5, d5, x5):
        copy.wait_recv()

    n_half = n_tp // 2
    m_half = n_half * rows

    def project(weight, w0, width, target, t0, r0):
        full = width // 256

        def tile(c0, w):
            for i in range(2):
                lhs = rows_all[n_half * i : n_half * (i + 1)].reshape(m_half, d)
                target[pl.ds(r0 + i * m_half, m_half), pl.ds(t0 + c0, w)] = jnp.dot(
                    lhs, weight[:, pl.ds(w0 + c0, w)], preferred_element_type=F32
                )

        def step(i, carry):
            tile(pl.multiple_of(i * 256, 256), 256)
            return carry

        lax.fori_loop(0, full, step, 0)
        if width % 256:
            tile(full * 256, width % 256)

    project(w_zx, el, el, pre, 0, 8)
    project(w_bc, 0, 256, pre, el, 8)
    dtp[...] = jnp.zeros_like(dtp)
    for i in range(2):
        lhs = rows_all[n_half * i : n_half * (i + 1)].reshape(m_half, d)
        dtp[i * m_half : (i + 1) * m_half, 0:nh] = lax.dot_general(
            lhs, w_dt[...], (((1,), (1,)), ((), ())), preferred_element_type=F32
        )
    edge = push(pre.at[pl.ds(toks, 8)], pre.at[pl.ds(0, 8)], nxt)

    step_all = jax.nn.softplus(dtp[...] + prm[0:1, :])
    dtp[...] = step_all
    rate = step_all * prm[1:2, :]
    ti = lax.broadcasted_iota(jnp.int32, (BLOCK, BLOCK), 0)
    si = lax.broadcasted_iota(jnp.int32, (BLOCK, BLOCK), 1)
    tri = jnp.where(ti >= si, 1.0, 0.0)
    for b in range(n_blocks):
        ldb[b] = jnp.dot(
            tri,
            rate[b * BLOCK : (b + 1) * BLOCK],
            precision=lax.Precision.HIGHEST,
            preferred_element_type=F32,
        )

    edge.wait_recv()
    for r in range(toks // 64):
        r0 = r * 64
        own = idc[8 + r0 : 72 + r0, :][:, 0:1]
        run_x = jnp.broadcast_to(bias_x[...], (64, el))
        run_bc = jnp.broadcast_to(bias_bc[...], (64, 256))
        for k in range(4):
            at = r0 + 5 + k
            keep = jnp.where(idc[at : at + 64, :][:, 0:1] == own, 1.0, 0.0)
            run_x = run_x + keep * conv_x[k : k + 1, :] * pre[at : at + 64, 0:el]
            run_bc = run_bc + keep * conv_bc[k : k + 1, :] * pre[at : at + 64, el : el + 256]
        xc[r0 : r0 + 64, :] = jax.nn.silu(run_x)
        bcm[r0 : r0 + 64, :] = jax.nn.silu(run_bc).astype(BF16)

    keeps = []
    for b in range(n_blocks):
        r0 = b * BLOCK
        ld = ldb[b]
        ld_end = ld[BLOCK - 1 : BLOCK, :]
        seg = idc[8 + r0 : 8 + r0 + BLOCK, :]
        seg_end = seg[BLOCK - 1 : BLOCK, :]
        prev = idc[7 + r0 : 8 + r0, :]
        step_b = dtp[r0 : r0 + BLOCK, :]
        to_end = jnp.exp(ld_end - ld) * jnp.where(seg == seg_end, 1.0, 0.0) * step_b
        x_b = xc[r0 : r0 + BLOCK, :]
        xp[r0 : r0 + BLOCK, :] = (x_b * lanes_of(step_b, spread)).astype(BF16)
        x_w = (x_b * lanes_of(to_end, spread)).astype(BF16)
        st[b] = lax.dot_general(
            bcm[r0 : r0 + BLOCK, 0:128],
            x_w,
            (((0,), (0,)), ((), ())),
            preferred_element_type=F32,
        )
        keep = jnp.exp(ld_end) * jnp.where(seg_end == prev, 1.0, 0.0)
        keeps.append(jnp.broadcast_to(keep, (8, 128)))
    keep_lanes = [lanes_of(k, spread)[0:1, :] for k in keeps]
    total = st[0]
    keep_shard = keeps[0]
    for b in range(1, n_blocks):
        total = keep_lanes[b] * total + st[b]
        keep_shard = keep_shard * keeps[b]
    a_out[...] = total.reshape(n_seq, ng, el).astype(BF16)
    k_out[...] = keep_shard

    project(w_zx, 0, el, gate, 0, 0)

    state_copies, keep_copies = [], []
    for k in range(1, n_seq):
        peer = lax.rem(seq + k, n_seq)
        where = {"seq": peer}
        keep_copies.append(push(k_out, k_in.at[seq], where))
        state_copies.append(push(a_out.at[peer], a_in.at[seq], where))
    a_in[seq] = a_out[seq]
    k_in[seq] = k_out[...]

    for b in range(n_blocks):
        r0 = b * BLOCK
        ld = ldb[b]
        ld_t = ld.T
        seg = idc[8 + r0 : 8 + r0 + BLOCK, :]
        seg_t = seg.T
        same = seg[:, 0:1] == seg_t[0:1, :]
        gram = lax.dot_general(
            bcm[r0 : r0 + BLOCK, 128:256],
            bcm[r0 : r0 + BLOCK, 0:128],
            (((1,), (1,)), ((), ())),
            preferred_element_type=F32,
        )
        gram = jnp.where(same & (ti >= si), gram, 0.0)
        for pair in range(nh // 2):
            cols = slice(pair * 128, pair * 128 + 128)
            x_pair = xp[r0 : r0 + BLOCK, cols]
            outs = []
            for j in range(2):
                hh = pair * 2 + j
                a = ld[:, hh : hh + 1]
                bb = ld_t[hh : hh + 1, :]
                w0 = jnp.exp(jnp.minimum(a[0:128] - bb[:, 0:128], 0.0)) * gram[0:128, 0:128]
                w1 = jnp.exp(jnp.minimum(a[128:] - bb, 0.0)) * gram[128:, :]
                outs.append(
                    (
                        jnp.dot(w0.astype(BF16), x_pair[0:128], preferred_element_type=F32),
                        jnp.dot(w1.astype(BF16), x_pair, preferred_element_type=F32),
                    )
                )
            first = lax.broadcasted_iota(jnp.int32, (128, 128), 1) < 64
            acc[r0 : r0 + 128, cols] = jnp.where(first, outs[0][0], outs[1][0])
            acc[r0 + 128 : r0 + 256, cols] = jnp.where(first, outs[0][1], outs[1][1])

        if b == 0:
            for copy in keep_copies + state_copies:
                copy.wait_recv()
            decay = lanes_of(k_in[...].reshape(n_seq * 8, 128), spread)
            run = jnp.zeros((ng, el), F32)
            for s in range(n_seq):
                i_out[s] = run.astype(BF16)
                run = decay[s * 8 : s * 8 + 1, :] * run + a_in[s].astype(F32)
            back_copies = []
            for k in range(1, n_seq):
                peer = lax.rem(seq + k, n_seq)
                back_copies.append(push(i_out.at[peer], i_in.at[seq], {"seq": peer}))
            i_in[seq] = i_out[seq]

    loads[3].wait()
    for copy in back_copies:
        copy.wait_recv()

    state = i_in[...].astype(F32).reshape(128, el)
    skip = lanes_of(jnp.broadcast_to(prm[2:3, :], (8, 128)), spread)[0:1, :]
    for b in range(n_blocks):
        r0 = b * BLOCK
        seg = idc[8 + r0 : 8 + r0 + BLOCK, :]
        prev = idc[7 + r0 : 8 + r0, :]
        reach = lanes_of(jnp.exp(ldb[b]) * jnp.where(seg == prev, 1.0, 0.0), spread)
        inter = jnp.dot(
            bcm[r0 : r0 + BLOCK, 128:256], state.astype(BF16), preferred_element_type=F32
        )
        out = acc[r0 : r0 + BLOCK, :] + reach * inter + skip * xc[r0 : r0 + BLOCK, :]
        gated = out * jax.nn.silu(gate[r0 : r0 + BLOCK, :])
        sq = jnp.sum(gated * gated, axis=1, keepdims=True)
        xp[r0 : r0 + BLOCK, :] = (gated * gated_gain[...]).astype(BF16)
        for q in range(2):
            col = jnp.broadcast_to(sq[q * 128 : q * 128 + 128], (128, 128))
            sq_out[b * 2 + q] = col.T[0:8, :]
        state = keep_lanes[b] * state + st[b]

    def out_rows(yy):
        lhs = xp[pl.ds(pl.multiple_of(yy * 2 * rows, 2 * rows), 2 * rows), :]
        wide = 512 if d % 512 == 0 else 256

        def step(i, carry):
            cols = pl.ds(pl.multiple_of(i * wide, wide), wide)
            part[yy, :, cols] = jnp.dot(
                lhs, w_out[:, cols], preferred_element_type=F32
            ).astype(BF16)
            return carry

        lax.fori_loop(0, d // wide, step, 0)

    def mine(xx):
        return pl.ds(pl.multiple_of(xx * rows, rows), rows)

    out_rows(far)
    sq_copies = []
    for k in range(1, n_tp):
        peer = lax.rem(tp + k, n_tp)
        sq_copies.append(push(sq_out.at[peer // 2], sq_in.at[tp], {"tp": peer}))
    sq_in[tp] = sq_out[y]
    out_rows(up)
    r2u = push(part.at[far, pl.ds(0, rows), right], yr2.at[0], at_up)
    r2d = push(part.at[far, pl.ds(rows, rows), right], yr2.at[1], at_down)
    l_far = push(part.at[far, mine(other), left], xl_in.at[far], at_x)
    out_rows(down)
    r3u = push(part.at[up, pl.ds(rows, rows), right], yr1.at[0, 1], at_up)
    l_up = push(part.at[up, mine(other), left], xl_in.at[up], at_x)
    out_rows(y)
    r3d = push(part.at[down, pl.ds(0, rows), right], yr1.at[1, 0], at_down)
    l_down = push(part.at[down, mine(other), left], xl_in.at[down], at_x)
    l_own = push(part.at[y, mine(other), left], xl_in.at[y], at_x)

    l_far.wait_recv()
    ql[far] = (
        part[far, mine(xl), left].astype(F32) + xl_in[far].astype(F32)
    ).astype(BF16)
    r2u.wait_recv()
    qr[0] = (part[up, pl.ds(0, rows), right].astype(F32) + yr2[0].astype(F32)).astype(BF16)
    l2u = push(ql.at[far, pl.ds(0, half)], yl2.at[0], at_up)
    l2d = push(ql.at[far, pl.ds(half, half)], yl2.at[1], at_down)
    r2d.wait_recv()
    qr[1] = (part[down, pl.ds(rows, rows), right].astype(F32) + yr2[1].astype(F32)).astype(BF16)
    r4u = push(qr.at[0], yr1.at[0, 0], at_up)
    l_up.wait_recv()
    ql[up] = (part[up, mine(xl), left].astype(F32) + xl_in[up].astype(F32)).astype(BF16)
    r4d = push(qr.at[1], yr1.at[1, 1], at_down)
    l_down.wait_recv()
    ql[down] = (part[down, mine(xl), left].astype(F32) + xl_in[down].astype(F32)).astype(BF16)
    l2u.wait_recv()
    ql[up, pl.ds(0, half), :] = (
        ql[up, pl.ds(0, half), :].astype(F32) + yl2[0].astype(F32)
    ).astype(BF16)
    l2d.wait_recv()
    ql[down, pl.ds(half, half), :] = (
        ql[down, pl.ds(half, half), :].astype(F32) + yl2[1].astype(F32)
    ).astype(BF16)
    l3u = push(ql.at[up], yl1.at[0], at_up)
    l3d = push(ql.at[down], yl1.at[1], at_down)
    for copy in (r3u, r3d, r4u, r4d):
        copy.wait_recv()

    def right_sum(xx):
        return (
            part[y, mine(xx), right].astype(F32)
            + yr1[0, xx].astype(F32)
            + yr1[1, xx].astype(F32)
        )

    qx[...] = right_sum(other).astype(BF16)

    for copy in sq_copies:
        copy.wait_recv()
    x6 = push(qx, xr_in, at_x)
    tot = sq_in[0]
    for k in range(1, n_tp):
        tot = tot + sq_in[k]
    sqc[...] = jnp.broadcast_to(tot[0:1, :], (128, 128)).T
    factor = lax.rsqrt(sqc[mine(xl), :][:, 0:1] / (el * n_tp) + EPS)

    l_own.wait_recv()
    l3u.wait_recv()
    l3d.wait_recv()
    own_l = (
        part[y, mine(xl), left].astype(F32)
        + xl_in[y].astype(F32)
        + yl1[0].astype(F32)
        + yl1[1].astype(F32)
    )
    result[:, left] = (hid[:, left].astype(F32) + factor * own_l).astype(BF16)
    mine_r = right_sum(xl)
    x6.wait_recv()
    own_r = mine_r + xr_in[...].astype(F32)
    result[:, right] = (hid[:, right].astype(F32) + factor * own_r).astype(BF16)

    for copy in sent:
        copy.wait_send()

    @pl.when(pipe == 0)
    def _():
        handoff.start()
        handoff.wait_send()


def local(geo, *args):
    n_seq, n_tp, n_y, d, el, nh, cl = geo
    (
        hidden_in,
        doc_ids,
        norm_gain,
        in_zx,
        in_bc,
        in_dt,
        conv_x,
        conv_bc,
        bias_x,
        bias_bc,
        dt_bias,
        a_log,
        d_skip,
        gated_gain,
        out_w,
    ) = args
    rows = hidden_in.shape[1]
    toks = rows * n_tp
    ng = 128 // n_seq
    cr = d - cl
    n_blocks = toks // BLOCK
    n_msg = 19 + 3 * (n_seq - 1) + (n_tp - 1) + 15
    vmem = pl.BlockSpec(memory_space=pltpu.VMEM)
    anyw = pl.BlockSpec(memory_space=pl.ANY)
    scratch = [
        pltpu.VMEM((d, 2 * el), BF16),
        pltpu.VMEM((d, 256), BF16),
        pltpu.VMEM((nh, d), BF16),
        pltpu.VMEM((el, d), BF16),
        pltpu.VMEM((rows, d), BF16),
        pltpu.VMEM((n_tp, rows, d), BF16),
        pltpu.VMEM((toks + 8, el + 256), F32),
        pltpu.VMEM((toks, el), F32),
        pltpu.VMEM((toks, el), F32),
        pltpu.VMEM((toks, 256), BF16),
        pltpu.VMEM((toks, el), BF16),
        pltpu.VMEM((toks, el), F32),
        pltpu.VMEM((toks + 8, 128), F32),
        pltpu.VMEM((toks, 128), F32),
        pltpu.VMEM((8, 128), F32),
        pltpu.VMEM((n_blocks, BLOCK, 128), F32),
        pltpu.VMEM((n_blocks, 128, el), F32),
        pltpu.VMEM((n_seq, ng, el), BF16),
        pltpu.VMEM((n_seq, ng, el), BF16),
        pltpu.VMEM((8, 128), F32),
        pltpu.VMEM((n_seq, 8, 128), F32),
        pltpu.VMEM((n_seq, ng, el), BF16),
        pltpu.VMEM((n_seq, ng, el), BF16),
        pltpu.VMEM((n_y, 2 * rows, d), BF16),
        pltpu.VMEM((n_y, rows, cl), BF16),
        pltpu.VMEM((n_y, rows, cl), BF16),
        pltpu.VMEM((2, rows // 2, cl), BF16),
        pltpu.VMEM((2, rows, cl), BF16),
        pltpu.VMEM((2, rows, cr), BF16),
        pltpu.VMEM((2, 2, rows, cr), BF16),
        pltpu.VMEM((2, rows, cr), BF16),
        pltpu.VMEM((rows, cr), BF16),
        pltpu.VMEM((rows, cr), BF16),
        pltpu.VMEM((n_y, 8, 128), F32),
        pltpu.VMEM((n_tp, 8, 128), F32),
        pltpu.VMEM((128, 128), F32),
        pltpu.SemaphoreType.DMA((n_msg,)),
        pltpu.SemaphoreType.DMA((n_msg,)),
        pltpu.SemaphoreType.DMA((5,)),
    ]
    out = pl.pallas_call(
        functools.partial(layer_kernel, geo),
        out_shape=jax.ShapeDtypeStruct((rows, d), BF16),
        in_specs=[anyw, vmem, vmem, anyw, anyw, anyw] + [vmem] * 8 + [anyw],
        out_specs=vmem,
        scratch_shapes=scratch,
        name="mixer_section",
        compiler_params=pltpu.CompilerParams(
            collective_id=0, has_side_effects=True, vmem_limit_bytes=60 * 1024 * 1024
        ),
    )(
        hidden_in[0],
        doc_ids,
        norm_gain,
        in_zx[0].reshape(d, 2 * el),
        in_bc[0],
        in_dt[0].T,
        conv_x[0],
        conv_bc[0],
        bias_x,
        bias_bc,
        dt_bias,
        a_log,
        d_skip,
        gated_gain,
        out_w[0],
    )
    return out[None, None]


def build(mesh, d, e, h):
    n_seq, n_tp = mesh.shape["seq"], mesh.shape["tp"]
    cl = max(128, (d * 9 // 20) // 128 * 128)
    geo = (n_seq, n_tp, n_tp // 2, d, e // n_tp, h // n_tp, cl)
    in_specs = (
        P(None, ("seq", "tp"), None),
        P(None, "seq"),
        P("pipe", None),
        P("pipe", None, None, "tp"),
        P("pipe", None, None),
        P("pipe", None, "tp"),
        P("pipe", None, "tp"),
        P("pipe", None, None),
        P("pipe", "tp"),
        P("pipe", None),
        P("pipe", "tp"),
        P("pipe", "tp"),
        P("pipe", "tp"),
        P("pipe", "tp"),
        P("pipe", "tp", None),
    )
    out_specs = P("pipe", None, ("seq", "tp"), None)
    return jax.shard_map(
        functools.partial(local, geo),
        mesh=mesh,
        in_specs=in_specs,
        out_specs=out_specs,
        check_vma=False,
    )


def solution(mesh):
    return build(mesh, 2560, 5120, 80)
```

```python
import functools

import jax
import jax.numpy as jnp
from jax import lax
from jax.experimental import pallas as pl
from jax.experimental.pallas import tpu as pltpu
from jax.sharding import PartitionSpec as P

BLOCK = 256
EPS = 1e-05
F32 = jnp.float32
BF16 = jnp.bfloat16
MESH = pl.DeviceIdType.MESH


def lanes_of(v, spread):
    hi = v.astype(BF16)
    lo = (v - hi.astype(F32)).astype(BF16)
    return jnp.dot(hi, spread, preferred_element_type=F32) + jnp.dot(
        lo, spread, preferred_element_type=F32
    )


def layer_kernel(
    geo,
    hidden_hbm,
    ids_ref,
    norm_gain,
    zx_hbm,
    bc_hbm,
    dt_hbm,
    conv_x,
    conv_bc,
    bias_x,
    bias_bc,
    dt_bias,
    a_log,
    d_skip,
    gated_gain,
    out_hbm,
    result,
    w_raw,
    w_gate,
    w_x,
    w_bc,
    w_dt,
    w_out,
    hid,
    rows_all,
    pre,
    gate,
    xc,
    bcm,
    xp,
    acc,
    idc,
    dtp,
    prm,
    ldb,
    st,
    grams,
    a_out,
    a_in,
    i_out,
    i_in,
    part,
    xl_in,
    ql,
    yl2,
    yl1,
    yr2,
    yr1,
    qr,
    qx,
    xr_in,
    sq_out,
    sq_in,
    sqc,
    send_sem,
    recv_sem,
    load_sem,
):
    n_seq, n_tp, n_y, d, el, nh, pieces = geo
    pipe, seq, tp = lax.axis_index("pipe"), lax.axis_index("seq"), lax.axis_index("tp")
    y, xl = tp // 2, tp % 2
    other = 1 - xl
    rows = hid.shape[0]
    toks = n_tp * rows
    half = rows // 2
    n_blocks = toks // BLOCK
    ng = 128 // n_seq
    up, down = lax.rem(y + 1, n_y), lax.rem(y + n_y - 1, n_y)
    far = lax.rem(y + 2, n_y)
    at_up = {"tp": up * 2 + xl}
    at_down = {"tp": down * 2 + xl}
    at_x = {"tp": y * 2 + other}
    nxt = {"seq": lax.rem(seq + 1, n_seq)}
    every = range(len(pieces))
    rights = [i for i in every if pieces[i][2]]
    lefts = [i for i in every if not pieces[i][2]]
    cols = [pl.ds(c0, w) for c0, w, _ in pieces]
    counter = [0]
    sent = []

    def remote(src, dst, where):
        k = counter[0]
        counter[0] += 1
        return pltpu.make_async_remote_copy(
            src_ref=src,
            dst_ref=dst,
            send_sem=send_sem.at[k],
            recv_sem=recv_sem.at[k],
            device_id=where,
            device_id_type=MESH,
        )

    def push(src, dst, where):
        copy = remote(src, dst, where)
        copy.start()
        sent.append(copy)
        return copy

    loads = [
        pltpu.make_async_copy(s, t, load_sem.at[k])
        for k, (s, t) in enumerate(
            [(zx_hbm, w_raw), (dt_hbm, w_dt), (bc_hbm, w_bc), (out_hbm, w_out)]
        )
    ]
    first_load = pltpu.make_async_copy(hidden_hbm, hid, load_sem.at[4])

    @pl.when(pipe == 0)
    def _():
        first_load.start()

    for copy in loads:
        copy.start()

    barrier = pltpu.get_barrier_semaphore()
    for k in range(1, n_seq):
        pl.semaphore_signal(
            barrier, inc=1, device_id={"seq": lax.rem(seq + k, n_seq)}, device_id_type=MESH
        )
    for k in range(1, n_tp):
        pl.semaphore_signal(
            barrier, inc=1, device_id={"tp": lax.rem(tp + k, n_tp)}, device_id_type=MESH
        )
    pl.semaphore_signal(barrier, inc=1, device_id={"pipe": 1 - pipe}, device_id_type=MESH)

    prm[...] = jnp.zeros_like(prm)
    prm[0:1, 0:nh] = dt_bias[...]
    prm[1:2, 0:nh] = -jnp.exp(a_log[...])
    prm[2:3, 0:nh] = d_skip[...]
    ids_row = ids_ref[...].astype(F32)
    idc[8 : 8 + toks, :] = jnp.broadcast_to(ids_row, (128, toks)).T
    head = lax.broadcasted_iota(jnp.int32, (128, el), 0)
    lane = lax.broadcasted_iota(jnp.int32, (128, el), 1)
    spread = jnp.where((lane // 64) == head, 1.0, 0.0).astype(BF16)
    ti = lax.broadcasted_iota(jnp.int32, (BLOCK, BLOCK), 0)
    si = lax.broadcasted_iota(jnp.int32, (BLOCK, BLOCK), 1)

    def lay_out(lo, hi):
        def step(i, carry):
            r = pl.multiple_of(i * 64, 64)
            both = jnp.swapaxes(w_raw[pl.ds(r, 64)].astype(F32), 0, 1)
            w_gate[pl.ds(r, 64), :] = both[0].astype(BF16)
            w_x[pl.ds(r, 64), 0:el] = both[1].astype(BF16)
            return carry

        lax.fori_loop(lo, hi, step, 0)

    def lay_out_dt():
        unit = jnp.where(
            lax.broadcasted_iota(jnp.int32, (nh, 128), 0)
            == lax.broadcasted_iota(jnp.int32, (nh, 128), 1),
            1.0,
            0.0,
        ).astype(BF16)
        for r in range(0, d, 256):
            w_x[r : r + 256, el : el + 128] = lax.dot_general(
                w_dt[:, r : r + 256],
                unit,
                (((0,), (0,)), ((), ())),
                preferred_element_type=F32,
            ).astype(BF16)

    n_lay = d // 64
    loads[1].wait()
    lay_out_dt()

    pl.semaphore_wait(barrier, n_tp + n_seq - 1)
    id_edge = push(idc.at[pl.ds(toks, 8)], idc.at[pl.ds(0, 8)], nxt)
    handoff = [remote(result.at[:, c], hid.at[:, c], {"pipe": 1 - pipe}) for c in cols]

    @pl.when(pipe == 0)
    def _():
        first_load.wait()

    loads[0].wait()

    @pl.when(pipe == 1)
    def _():
        lay_out(0, n_lay)
        for copy in handoff:
            copy.wait_recv()

    h = hid[...].astype(F32)
    scale = lax.rsqrt(jnp.mean(h * h, axis=1, keepdims=True) + EPS)
    rows_all[tp] = (h * scale * norm_gain[...]).astype(BF16)

    def hop(yy, xx, i, where, r0=0, n=rows):
        s = rows_all.at[yy * 2 + xx, pl.ds(r0, n), cols[i]]
        return push(s, s, where)

    u1, d1, x1 = {}, {}, {}
    for i in every:
        u1[i], d1[i] = hop(y, xl, i, at_up), hop(y, xl, i, at_down)
        x1[i] = hop(y, xl, i, at_x)

    @pl.when(pipe == 0)
    def _():
        lay_out(0, n_lay // 2)

    u2, d2, x2, x3 = {}, {}, {}, {}
    for i in every:
        if i in rights:
            x1[i].wait_recv()
            u2[i], d2[i] = hop(y, other, i, at_up), hop(y, other, i, at_down)
        else:
            u1[i].wait_recv()
            u2[i] = hop(down, xl, i, at_up, 0, half)
            x2[i] = hop(down, xl, i, at_x)
            d1[i].wait_recv()
            d2[i] = hop(up, xl, i, at_down, half, half)
            x3[i] = hop(up, xl, i, at_x)

    @pl.when(pipe == 0)
    def _():
        lay_out(n_lay // 2, n_lay)

    u3, d3, x4 = {}, {}, {}
    for i in every:
        if i in rights:
            u1[i].wait_recv()
            u2[i].wait_recv()
            u3[i] = hop(down, 0, i, at_up)
            d1[i].wait_recv()
            d2[i].wait_recv()
            d3[i] = hop(up, 1, i, at_down)
        else:
            u2[i].wait_recv()
            d2[i].wait_recv()
            x4[i] = hop(far, xl, i, at_x)

    id_edge.wait_recv()
    idc[0:8, :] = jnp.where(seq > 0, idc[0:8, :], -1.0)
    loads[2].wait()
    n_half = n_tp // 2
    m_half = n_half * rows

    def project(weight, w0, w, target, t0, r0, i):
        for j in range(2):
            lhs = rows_all[n_half * j : n_half * (j + 1), :, cols[i]].reshape(
                m_half, pieces[i][1]
            )
            at = (pl.ds(r0 + j * m_half, m_half), pl.ds(t0, w))
            term = jnp.dot(lhs, weight[cols[i], pl.ds(w0, w)], preferred_element_type=F32)
            target[at] = term if i == 0 else target[at] + term

    for i in every:
        if i in rights:
            u3[i].wait_recv()
            d3[i].wait_recv()
        else:
            for copy in (x1[i], x2[i], x3[i], x4[i]):
                copy.wait_recv()

        def step(t, carry, i=i):
            c0 = pl.multiple_of(t * 256, 256)
            project(w_x, c0, 256, pre, c0, 8, i)
            return carry

        lax.fori_loop(0, (el + 128) // 256, step, 0)
        project(w_bc, 0, 256, pre, el + 128, 8, i)

    step_all = jax.nn.softplus(pre[8 : 8 + toks, el : el + 128] + prm[0:1, :])
    dtp[...] = step_all
    edge = push(pre.at[pl.ds(toks, 8)], pre.at[pl.ds(0, 8)], nxt)
    rate = step_all * prm[1:2, :]
    tri = jnp.where(ti >= si, 1.0, 0.0)
    for b in range(n_blocks):
        ldb[b] = jnp.dot(
            tri,
            rate[b * BLOCK : (b + 1) * BLOCK],
            precision=lax.Precision.HIGHEST,
            preferred_element_type=F32,
        )

    def convolve(r):
        r0 = r * 64
        own = idc[8 + r0 : 72 + r0, :][:, 0:1]
        run_x = jnp.broadcast_to(bias_x[...], (64, el))
        run_bc = jnp.broadcast_to(bias_bc[...], (64, 256))
        for k in range(4):
            at = r0 + 5 + k
            keep = jnp.where(idc[at : at + 64, :][:, 0:1] == own, 1.0, 0.0)
            run_x = run_x + keep * conv_x[k : k + 1, :] * pre[at : at + 64, 0:el]
            run_bc = run_bc + keep * conv_bc[k : k + 1, :] * pre[at : at + 64, el + 128 :]
        xc[r0 : r0 + 64, :] = jax.nn.silu(run_x)
        bcm[r0 : r0 + 64, :] = jax.nn.silu(run_bc).astype(BF16)

    for r in range(1, toks // 64):
        convolve(r)

    def project_gate(c0, w):
        for j in range(2):
            lhs = rows_all[n_half * j : n_half * (j + 1)].reshape(m_half, d)
            gate[pl.ds(j * m_half, m_half), pl.ds(c0, w)] = jnp.dot(
                lhs, w_gate[:, pl.ds(c0, w)], preferred_element_type=F32
            )

    gate_tiles = [(c0, min(256, el - c0)) for c0 in range(0, el, 256)]
    for tile in gate_tiles[:-1]:
        project_gate(*tile)

    edge.wait_recv()
    convolve(0)

    keeps = []
    for b in range(n_blocks):
        r0 = b * BLOCK
        ld = ldb[b]
        ld_end = ld[BLOCK - 1 : BLOCK, :]
        seg = idc[8 + r0 : 8 + r0 + BLOCK, :]
        seg_end = seg[BLOCK - 1 : BLOCK, :]
        prev = idc[7 + r0 : 8 + r0, :]
        step_b = dtp[r0 : r0 + BLOCK, :]
        to_end = jnp.exp(ld_end - ld) * jnp.where(seg == seg_end, 1.0, 0.0) * step_b
        x_b = xc[r0 : r0 + BLOCK, :]
        x_w = (x_b * lanes_of(to_end, spread)).astype(BF16)
        st[b] = lax.dot_general(
            bcm[r0 : r0 + BLOCK, 0:128],
            x_w,
            (((0,), (0,)), ((), ())),
            preferred_element_type=F32,
        )
        keep = jnp.exp(ld_end) * jnp.where(seg_end == prev, 1.0, 0.0)
        keeps.append(jnp.broadcast_to(keep, (8, 128)))
    keep_lanes = [lanes_of(k, spread)[0:1, :] for k in keeps]
    total = st[0]
    keep_shard = keeps[0]
    for b in range(1, n_blocks):
        total = keep_lanes[b] * total + st[b]
        keep_shard = keep_shard * keeps[b]
    a_out[:, :, 0:el] = total.reshape(n_seq, ng, el).astype(BF16)
    keep_row = jnp.broadcast_to(keep_shard[0:1, :], (ng, 128))
    k_hi = keep_row.astype(BF16).astype(F32)
    k_mid = (keep_row - k_hi).astype(BF16).astype(F32)
    k_lo = keep_row - k_hi - k_mid
    which = lax.broadcasted_iota(jnp.int32, (ng, 128), 0)
    k_rows = jnp.where(
        which == 0, k_hi, jnp.where(which == 1, k_mid, jnp.where(which == 2, k_lo, 0.0))
    ).astype(BF16)
    for s in range(n_seq):
        a_out[s, :, el : el + 128] = k_rows

    for b in range(n_blocks):
        r0 = b * BLOCK
        seg = idc[8 + r0 : 8 + r0 + BLOCK, :]
        same = seg[:, 0:1] == seg.T[0:1, :]
        gram = lax.dot_general(
            bcm[r0 : r0 + BLOCK, 128:256],
            bcm[r0 : r0 + BLOCK, 0:128],
            (((1,), (1,)), ((), ())),
            preferred_element_type=F32,
        )
        grams[b] = jnp.where(same & (ti >= si), gram, 0.0)

    state_copies = []
    for k in range(1, n_seq):
        peer = lax.rem(seq + k, n_seq)
        state_copies.append(push(a_out.at[peer], a_in.at[seq], {"seq": peer}))
    a_in[seq] = a_out[seq]
    project_gate(*gate_tiles[-1])
    for b in range(n_blocks):
        r0 = b * BLOCK
        xp[r0 : r0 + BLOCK, :] = (
            xc[r0 : r0 + BLOCK, :] * lanes_of(dtp[r0 : r0 + BLOCK, :], spread)
        ).astype(BF16)

    def inside(b):
        r0 = b * BLOCK
        ld = ldb[b]
        ld_t = ld.T
        gram = grams[b]
        for pair in range(nh // 2):
            cs = slice(pair * 128, pair * 128 + 128)
            x_pair = xp[r0 : r0 + BLOCK, cs]
            outs = []
            for j in range(2):
                hh = pair * 2 + j
                a = ld[:, hh : hh + 1]
                bb = ld_t[hh : hh + 1, :]
                w0 = jnp.exp(jnp.minimum(a[0:128] - bb[:, 0:128], 0.0)) * gram[0:128, 0:128]
                w1 = jnp.exp(jnp.minimum(a[128:] - bb, 0.0)) * gram[128:, :]
                outs.append(
                    (
                        jnp.dot(w0.astype(BF16), x_pair[0:128], preferred_element_type=F32),
                        jnp.dot(w1.astype(BF16), x_pair, preferred_element_type=F32),
                    )
                )
            first = lax.broadcasted_iota(jnp.int32, (128, 128), 1) < 64
            acc[r0 : r0 + 128, cs] = jnp.where(first, outs[0][0], outs[1][0])
            acc[r0 + 128 : r0 + 256, cs] = jnp.where(first, outs[0][1], outs[1][1])

    inside(0)

    for copy in state_copies:
        copy.wait_recv()

    decay = jnp.dot(
        a_in[:, :, el : el + 128].reshape(n_seq * ng, 128), spread, preferred_element_type=F32
    )
    run = jnp.zeros((ng, el), F32)
    for s in range(n_seq):
        i_out[s] = run.astype(BF16)
        k0 = s * ng
        keep = decay[k0 : k0 + 1, :] + decay[k0 + 1 : k0 + 2, :] + decay[k0 + 2 : k0 + 3, :]
        run = keep * run + a_in[s, :, 0:el].astype(F32)
    back_copies = []
    for k in range(1, n_seq):
        peer = lax.rem(seq + k, n_seq)
        back_copies.append(push(i_out.at[peer], i_in.at[seq], {"seq": peer}))
    i_in[seq] = i_out[seq]
    for b in range(1, n_blocks):
        inside(b)
    loads[3].wait()

    for copy in back_copies:
        copy.wait_recv()

    state = i_in[...].astype(F32).reshape(128, el)
    skip = lanes_of(jnp.broadcast_to(prm[2:3, :], (8, 128)), spread)[0:1, :]
    for b in range(n_blocks):
        r0 = b * BLOCK
        seg = idc[8 + r0 : 8 + r0 + BLOCK, :]
        prev = idc[7 + r0 : 8 + r0, :]
        reach = lanes_of(jnp.exp(ldb[b]) * jnp.where(seg == prev, 1.0, 0.0), spread)
        inter = jnp.dot(
            bcm[r0 : r0 + BLOCK, 128:256], state.astype(BF16), preferred_element_type=F32
        )
        out = acc[r0 : r0 + BLOCK, :] + reach * inter + skip * xc[r0 : r0 + BLOCK, :]
        gated = out * jax.nn.silu(gate[r0 : r0 + BLOCK, :])
        sq = jnp.sum(gated * gated, axis=1, keepdims=True)
        xp[r0 : r0 + BLOCK, :] = (gated * gated_gain[...]).astype(BF16)
        for q in range(2):
            col = jnp.broadcast_to(sq[q * 128 : q * 128 + 128], (128, 128))
            sq_out[b * 2 + q] = col.T[0:8, :]
        state = keep_lanes[b] * state + st[b]

    def out_cols(i):
        for q in range(2):
            term = jnp.dot(
                xp[q * m_half : (q + 1) * m_half, :],
                w_out[:, cols[i]],
                preferred_element_type=F32,
            ).astype(BF16)
            part[q * (n_y // 2) : (q + 1) * (n_y // 2), :, cols[i]] = term.reshape(
                n_y // 2, 2 * rows, pieces[i][1]
            )

    def mine(xx):
        return pl.ds(pl.multiple_of(xx * rows, rows), rows)

    zero, one = pl.ds(0, rows), pl.ds(rows, rows)
    r2u, r2d, r3u, r3d, r4u, r4d, x6 = {}, {}, {}, {}, {}, {}, {}
    lx = {}
    l2u, l2d, l3u, l3d = {}, {}, {}, {}

    def first_sends(i):
        if i in rights:
            r2u[i] = push(part.at[far, zero, cols[i]], yr2.at[0, :, cols[i]], at_up)
            r2d[i] = push(part.at[far, one, cols[i]], yr2.at[1, :, cols[i]], at_down)
        else:
            lx[i] = [
                push(part.at[yy, mine(other), cols[i]], xl_in.at[yy, :, cols[i]], at_x)
                for yy in (far, up, down, y)
            ]

    def second_sends(i):
        r3u[i] = push(part.at[up, one, cols[i]], yr1.at[0, 1, :, cols[i]], at_up)
        r3d[i] = push(part.at[down, zero, cols[i]], yr1.at[1, 0, :, cols[i]], at_down)

    for i in every:
        out_cols(i)
        if i > 0:
            first_sends(i - 1)
    sq_copies = []
    for k in range(1, n_tp):
        peer = lax.rem(tp + k, n_tp)
        sq_copies.append(push(sq_out.at[peer // 2], sq_in.at[tp], {"tp": peer}))
    sq_in[tp] = sq_out[y]
    first_sends(len(pieces) - 1)
    for i in rights:
        second_sends(i)

    def sum_of(*refs):
        tot = refs[0].astype(F32)
        for r in refs[1:]:
            tot = tot + r.astype(F32)
        return tot

    for i in every:
        c = cols[i]
        if i in rights:
            r2u[i].wait_recv()
            qr[0, :, c] = sum_of(part[up, zero, c], yr2[0, :, c]).astype(BF16)
            r2d[i].wait_recv()
            qr[1, :, c] = sum_of(part[down, one, c], yr2[1, :, c]).astype(BF16)
            r4u[i] = push(qr.at[0, :, c], yr1.at[0, 0, :, c], at_up)
            r4d[i] = push(qr.at[1, :, c], yr1.at[1, 1, :, c], at_down)
        else:
            lx[i][0].wait_recv()
            ql[far, :, c] = sum_of(part[far, mine(xl), c], xl_in[far, :, c]).astype(BF16)
            l2u[i] = push(ql.at[far, pl.ds(0, half), c], yl2.at[0, :, c], at_up)
            l2d[i] = push(ql.at[far, pl.ds(half, half), c], yl2.at[1, :, c], at_down)

    for i in lefts:
        c = cols[i]
        lx[i][1].wait_recv()
        q_up = sum_of(part[up, mine(xl), c], xl_in[up, :, c])
        lx[i][2].wait_recv()
        q_down = sum_of(part[down, mine(xl), c], xl_in[down, :, c])
        l2u[i].wait_recv()
        ql[up, pl.ds(0, half), c] = (q_up[0:half] + yl2[0, :, c].astype(F32)).astype(BF16)
        ql[up, pl.ds(half, half), c] = q_up[half:].astype(BF16)
        l2d[i].wait_recv()
        ql[down, pl.ds(0, half), c] = q_down[0:half].astype(BF16)
        ql[down, pl.ds(half, half), c] = (q_down[half:] + yl2[1, :, c].astype(F32)).astype(BF16)
        l3u[i] = push(ql.at[up, :, c], yl1.at[0, :, c], at_up)
        l3d[i] = push(ql.at[down, :, c], yl1.at[1, :, c], at_down)

    for copy in sq_copies:
        copy.wait_recv()
    tot = sq_in[0]
    for k in range(1, n_tp):
        tot = tot + sq_in[k]
    sqc[...] = jnp.broadcast_to(tot[0:1, :], (128, 128)).T
    factor = lax.rsqrt(sqc[mine(xl), :][:, 0:1] / (el * n_tp) + EPS)

    def right_sum(xx, c):
        return sum_of(part[y, mine(xx), c], yr1[0, xx, :, c], yr1[1, xx, :, c])

    for i in rights:
        c = cols[i]
        for copy in (r3u[i], r3d[i], r4u[i], r4d[i]):
            copy.wait_recv()
        qx[:, c] = right_sum(other, c).astype(BF16)
        x6[i] = push(qx.at[:, c], xr_in.at[:, c], at_x)

    def finish(i, total):
        c = cols[i]
        result[:, c] = (hid[:, c].astype(F32) + factor * total).astype(BF16)

    done = []

    def hand(i):
        done.append(i)

        @pl.when(pipe == 0)
        def _():
            handoff[i].start()

    for i in lefts:
        c = cols[i]
        lx[i][3].wait_recv()
        l3u[i].wait_recv()
        l3d[i].wait_recv()
        finish(i, sum_of(part[y, mine(xl), c], xl_in[y, :, c], yl1[0, :, c], yl1[1, :, c]))
    waiting = list(lefts)
    for i in rights:
        c = cols[i]
        own = right_sum(xl, c)
        x6[i].wait_recv()
        for j in waiting:
            hand(j)
        finish(i, own + xr_in[:, c].astype(F32))
        waiting = [i]
    for j in waiting:
        hand(j)

    for copy in sent:
        copy.wait_send()

    @pl.when(pipe == 0)
    def _():
        for copy in handoff:
            copy.wait_send()


def local(geo, *args):
    n_seq, n_tp, n_y, d, el, nh, pieces = geo
    (
        hidden_in,
        doc_ids,
        norm_gain,
        in_zx,
        in_bc,
        in_dt,
        conv_x,
        conv_bc,
        bias_x,
        bias_bc,
        dt_bias,
        a_log,
        d_skip,
        gated_gain,
        out_w,
    ) = args
    rows = hidden_in.shape[1]
    toks = rows * n_tp
    ng = 128 // n_seq
    n_blocks = toks // BLOCK
    n_right = sum(1 for p in pieces if p[2])
    n_left = len(pieces) - n_right
    n_msg = (
        2 + len(pieces) + 2 * (n_seq - 1) + (n_tp - 1) + 14 * n_right + 16 * n_left
    )
    vmem = pl.BlockSpec(memory_space=pltpu.VMEM)
    anyw = pl.BlockSpec(memory_space=pl.ANY)
    scratch = [
        pltpu.VMEM((d, 2, el), BF16),
        pltpu.VMEM((d, el), BF16),
        pltpu.VMEM((d, el + 128), BF16),
        pltpu.VMEM((d, 256), BF16),
        pltpu.VMEM((nh, d), BF16),
        pltpu.VMEM((el, d), BF16),
        pltpu.VMEM((rows, d), BF16),
        pltpu.VMEM((n_tp, rows, d), BF16),
        pltpu.VMEM((toks + 8, el + 384), F32),
        pltpu.VMEM((toks, el), F32),
        pltpu.VMEM((toks, el), F32),
        pltpu.VMEM((toks, 256), BF16),
        pltpu.VMEM((toks, el), BF16),
        pltpu.VMEM((toks, el), F32),
        pltpu.VMEM((toks + 8, 128), F32),
        pltpu.VMEM((toks, 128), F32),
        pltpu.VMEM((8, 128), F32),
        pltpu.VMEM((n_blocks, BLOCK, 128), F32),
        pltpu.VMEM((n_blocks, 128, el), F32),
        pltpu.VMEM((n_blocks, BLOCK, BLOCK), F32),
        pltpu.VMEM((n_seq, ng, el + 128), BF16),
        pltpu.VMEM((n_seq, ng, el + 128), BF16),
        pltpu.VMEM((n_seq, ng, el), BF16),
        pltpu.VMEM((n_seq, ng, el), BF16),
        pltpu.VMEM((n_y, 2 * rows, d), BF16),
        pltpu.VMEM((n_y, rows, d), BF16),
        pltpu.VMEM((n_y, rows, d), BF16),
        pltpu.VMEM((2, rows // 2, d), BF16),
        pltpu.VMEM((2, rows, d), BF16),
        pltpu.VMEM((2, rows, d), BF16),
        pltpu.VMEM((2, 2, rows, d), BF16),
        pltpu.VMEM((2, rows, d), BF16),
        pltpu.VMEM((rows, d), BF16),
        pltpu.VMEM((rows, d), BF16),
        pltpu.VMEM((n_y, 8, 128), F32),
        pltpu.VMEM((n_tp, 8, 128), F32),
        pltpu.VMEM((128, 128), F32),
        pltpu.SemaphoreType.DMA((n_msg,)),
        pltpu.SemaphoreType.DMA((n_msg,)),
        pltpu.SemaphoreType.DMA((5,)),
    ]
    out = pl.pallas_call(
        functools.partial(layer_kernel, geo),
        out_shape=jax.ShapeDtypeStruct((rows, d), BF16),
        in_specs=[anyw, vmem, vmem, anyw, anyw, anyw] + [vmem] * 8 + [anyw],
        out_specs=vmem,
        scratch_shapes=scratch,
        name="mixer_section",
        compiler_params=pltpu.CompilerParams(
            collective_id=0, has_side_effects=True, vmem_limit_bytes=60 * 1024 * 1024
        ),
    )(
        hidden_in[0],
        doc_ids,
        norm_gain,
        in_zx[0],
        in_bc[0],
        in_dt[0].T,
        conv_x[0],
        conv_bc[0],
        bias_x,
        bias_bc,
        dt_bias,
        a_log,
        d_skip,
        gated_gain,
        out_w[0],
    )
    return out[None, None]


def build(mesh, d, e, h):
    n_seq, n_tp = mesh.shape["seq"], mesh.shape["tp"]
    wide = 512 if d % 512 == 0 else 128
    pieces = tuple((c, wide, (c // wide) % 2 == 0) for c in range(0, d, wide))
    geo = (n_seq, n_tp, n_tp // 2, d, e // n_tp, h // n_tp, pieces)
    in_specs = (
        P(None, ("seq", "tp"), None),
        P(None, "seq"),
        P("pipe", None),
        P("pipe", None, None, "tp"),
        P("pipe", None, None),
        P("pipe", None, "tp"),
        P("pipe", None, "tp"),
        P("pipe", None, None),
        P("pipe", "tp"),
        P("pipe", None),
        P("pipe", "tp"),
        P("pipe", "tp"),
        P("pipe", "tp"),
        P("pipe", "tp"),
        P("pipe", "tp", None),
    )
    out_specs = P("pipe", None, ("seq", "tp"), None)
    return jax.shard_map(
        functools.partial(local, geo),
        mesh=mesh,
        in_specs=in_specs,
        out_specs=out_specs,
        check_vma=False,
    )


def solution(mesh):
    return build(mesh, 2560, 5120, 80)
```

```python
import functools

import jax
import jax.numpy as jnp
from jax import lax
from jax.experimental import pallas as pl
from jax.experimental.pallas import tpu as pltpu
from jax.sharding import PartitionSpec as P

BLOCK = 256
EPS = 1e-05
F32 = jnp.float32
BF16 = jnp.bfloat16
MESH = pl.DeviceIdType.MESH


def lanes_of(v, spread):
    hi = v.astype(BF16)
    lo = (v - hi.astype(F32)).astype(BF16)
    return jnp.dot(hi, spread, preferred_element_type=F32) + jnp.dot(
        lo, spread, preferred_element_type=F32
    )


def layer_kernel(
    geo,
    hidden_hbm,
    ids_ref,
    norm_gain,
    zx_hbm,
    bc_hbm,
    dt_hbm,
    conv_x,
    conv_bc,
    bias_x,
    bias_bc,
    dt_bias,
    a_log,
    d_skip,
    gated_gain,
    out_hbm,
    result,
    w_raw,
    w_gate,
    w_x,
    w_bc,
    w_dt,
    w_out,
    hid,
    rows_all,
    pre,
    gate,
    xc,
    bcm,
    xp,
    acc,
    idc,
    dtp,
    prm,
    ldb,
    st,
    grams,
    a_out,
    a_in,
    i_out,
    i_in,
    part,
    xl_in,
    ql,
    yl2,
    yl1,
    yr2,
    yr1,
    qr,
    qx,
    xr_in,
    sq_out,
    sq_in,
    sqc,
    send_sem,
    recv_sem,
    load_sem,
):
    n_seq, n_tp, n_y, d, el, nh, pieces = geo
    pipe, seq, tp = lax.axis_index("pipe"), lax.axis_index("seq"), lax.axis_index("tp")
    y, xl = tp // 2, tp % 2
    other = 1 - xl
    rows = hid.shape[0]
    toks = n_tp * rows
    half = rows // 2
    n_blocks = toks // BLOCK
    ng = 128 // n_seq
    up, down = lax.rem(y + 1, n_y), lax.rem(y + n_y - 1, n_y)
    far = lax.rem(y + 2, n_y)
    at_up = {"tp": up * 2 + xl}
    at_down = {"tp": down * 2 + xl}
    at_x = {"tp": y * 2 + other}
    nxt = {"seq": lax.rem(seq + 1, n_seq)}
    every = range(len(pieces))
    rights = [i for i in every if pieces[i][2]]
    lefts = [i for i in every if not pieces[i][2]]
    cols = [pl.ds(c0, w) for c0, w, _ in pieces]
    counter = [0]
    sent = []

    def remote(src, dst, where):
        k = counter[0]
        counter[0] += 1
        return pltpu.make_async_remote_copy(
            src_ref=src,
            dst_ref=dst,
            send_sem=send_sem.at[k],
            recv_sem=recv_sem.at[k],
            device_id=where,
            device_id_type=MESH,
        )

    def push(src, dst, where):
        copy = remote(src, dst, where)
        copy.start()
        sent.append(copy)
        return copy

    top, bottom = pl.ds(0, d // 2), pl.ds(d // 2, d // 2)
    load_dt, load_top, load_bottom, load_bc, load_out = loads = [
        pltpu.make_async_copy(s, t, load_sem.at[k])
        for k, (s, t) in enumerate(
            [
                (dt_hbm, w_dt),
                (zx_hbm.at[top], w_raw.at[top]),
                (zx_hbm.at[bottom], w_raw.at[bottom]),
                (bc_hbm, w_bc),
                (out_hbm, w_out),
            ]
        )
    ]
    first_load = pltpu.make_async_copy(hidden_hbm, hid, load_sem.at[5])

    @pl.when(pipe == 0)
    def _():
        first_load.start()

    for copy in loads:
        copy.start()

    far_first = sorted(range(1, n_seq), key=lambda k: abs(2 * k - n_seq))
    barrier = pltpu.get_barrier_semaphore()
    for k in far_first:
        pl.semaphore_signal(
            barrier, inc=1, device_id={"seq": lax.rem(seq + k, n_seq)}, device_id_type=MESH
        )
    for k in range(1, n_tp):
        pl.semaphore_signal(
            barrier, inc=1, device_id={"tp": lax.rem(tp + k, n_tp)}, device_id_type=MESH
        )
    pl.semaphore_signal(barrier, inc=1, device_id={"pipe": 1 - pipe}, device_id_type=MESH)

    prm[...] = jnp.zeros_like(prm)
    prm[0:1, 0:nh] = dt_bias[...]
    prm[1:2, 0:nh] = -jnp.exp(a_log[...])
    prm[2:3, 0:nh] = d_skip[...]
    ids_row = ids_ref[...].astype(F32)
    idc[8 : 8 + toks, :] = jnp.broadcast_to(ids_row, (128, toks)).T
    head = lax.broadcasted_iota(jnp.int32, (128, el), 0)
    lane = lax.broadcasted_iota(jnp.int32, (128, el), 1)
    spread = jnp.where((lane // 64) == head, 1.0, 0.0).astype(BF16)
    ti = lax.broadcasted_iota(jnp.int32, (BLOCK, BLOCK), 0)
    si = lax.broadcasted_iota(jnp.int32, (BLOCK, BLOCK), 1)

    def lay_out(lo, hi):
        def step(i, carry):
            r = pl.multiple_of(i * 64, 64)
            both = jnp.swapaxes(w_raw[pl.ds(r, 64)].astype(F32), 0, 1)
            w_gate[pl.ds(r, 64), :] = both[0].astype(BF16)
            w_x[pl.ds(r, 64), 0:el] = both[1].astype(BF16)
            return carry

        lax.fori_loop(lo, hi, step, 0)

    def lay_out_dt():
        unit = jnp.where(
            lax.broadcasted_iota(jnp.int32, (nh, 128), 0)
            == lax.broadcasted_iota(jnp.int32, (nh, 128), 1),
            1.0,
            0.0,
        ).astype(BF16)
        for r in range(0, d, 256):
            w_x[r : r + 256, el : el + 128] = lax.dot_general(
                w_dt[:, r : r + 256],
                unit,
                (((0,), (0,)), ((), ())),
                preferred_element_type=F32,
            ).astype(BF16)

    n_lay = d // 64
    load_dt.wait()
    lay_out_dt()
    load_top.wait()
    lay_out(0, n_lay // 2)

    pl.semaphore_wait(barrier, n_tp + n_seq - 1)
    id_edge = push(idc.at[pl.ds(toks, 8)], idc.at[pl.ds(0, 8)], nxt)
    handoff = [remote(result.at[:, c], hid.at[:, c], {"pipe": 1 - pipe}) for c in cols]

    @pl.when(pipe == 0)
    def _():
        first_load.wait()

    load_bottom.wait()

    @pl.when(pipe == 1)
    def _():
        lay_out(n_lay // 2, n_lay)
        for copy in handoff:
            copy.wait_recv()

    h = hid[...].astype(F32)
    scale = lax.rsqrt(jnp.mean(h * h, axis=1, keepdims=True) + EPS)
    rows_all[tp] = (h * scale * norm_gain[...]).astype(BF16)

    def hop(yy, xx, i, where, r0=0, n=rows):
        s = rows_all.at[yy * 2 + xx, pl.ds(r0, n), cols[i]]
        return push(s, s, where)

    u1, d1, x1 = {}, {}, {}
    for i in every:
        u1[i], d1[i] = hop(y, xl, i, at_up), hop(y, xl, i, at_down)
        x1[i] = hop(y, xl, i, at_x)

    @pl.when(pipe == 0)
    def _():
        lay_out(n_lay // 2, n_lay)

    u2, d2, x2, x3 = {}, {}, {}, {}
    for i in every:
        if i in rights:
            x1[i].wait_recv()
            u2[i], d2[i] = hop(y, other, i, at_up), hop(y, other, i, at_down)
        else:
            u1[i].wait_recv()
            u2[i] = hop(down, xl, i, at_up, 0, half)
            x2[i] = hop(down, xl, i, at_x)
            d1[i].wait_recv()
            d2[i] = hop(up, xl, i, at_down, half, half)
            x3[i] = hop(up, xl, i, at_x)

    load_bc.wait()
    for i in lefts:
        x1[i].wait_recv()
    n_tiles = (el + 128) // 256

    def project(pairs, weight, w0, t0):
        lhs = jnp.concatenate(
            [rows_all[pl.ds(yy * 2, 2)].reshape(2 * rows, d) for yy in pairs], axis=0
        )
        term = jnp.dot(lhs, weight[:, pl.ds(w0, 256)], preferred_element_type=F32)
        for k, yy in enumerate(pairs):
            at = pl.ds(pl.multiple_of(8 + yy * 2 * rows, 8), 2 * rows)
            pre[at, pl.ds(t0, 256)] = term[k * 2 * rows : (k + 1) * 2 * rows]

    def project_own(t):
        if t < n_tiles:
            project((y,), w_x, t * 256, t * 256)
        elif t == n_tiles:
            project((y,), w_bc, 0, el + 128)

    project_own(0)
    project_own(1)
    u3, d3, x4 = {}, {}, {}
    for i in every:
        if i in rights:
            u1[i].wait_recv()
            u2[i].wait_recv()
            u3[i] = hop(down, 0, i, at_up)
            d1[i].wait_recv()
            d2[i].wait_recv()
            d3[i] = hop(up, 1, i, at_down)
        else:
            u2[i].wait_recv()
            d2[i].wait_recv()
            x4[i] = hop(far, xl, i, at_x)
        if i == 1:
            project_own(2)
    project_own(3)

    id_edge.wait_recv()
    idc[0:8, :] = jnp.where(seq > 0, idc[0:8, :], -1.0)
    n_half = n_tp // 2
    m_half = n_half * rows
    for i in every:
        for copy in (u3[i], d3[i]) if i in rights else (x2[i], x3[i], x4[i]):
            copy.wait_recv()

    def step(t, carry):
        c0 = pl.multiple_of(t * 256, 256)
        project((up, far, down), w_x, c0, c0)
        return carry

    lax.fori_loop(0, n_tiles, step, 0)
    project((up, far, down), w_bc, 0, el + 128)

    step_all = jax.nn.softplus(pre[8 : 8 + toks, el : el + 128] + prm[0:1, :])
    dtp[...] = step_all
    edge = push(pre.at[pl.ds(toks, 8)], pre.at[pl.ds(0, 8)], nxt)
    rate = step_all * prm[1:2, :]
    tri = jnp.where(ti >= si, 1.0, 0.0)
    for b in range(n_blocks):
        ldb[b] = jnp.dot(
            tri,
            rate[b * BLOCK : (b + 1) * BLOCK],
            precision=lax.Precision.HIGHEST,
            preferred_element_type=F32,
        )

    def convolve(r):
        r0 = r * 64
        own = idc[8 + r0 : 72 + r0, :][:, 0:1]
        run_x = jnp.broadcast_to(bias_x[...], (64, el))
        run_bc = jnp.broadcast_to(bias_bc[...], (64, 256))
        for k in range(4):
            at = r0 + 5 + k
            keep = jnp.where(idc[at : at + 64, :][:, 0:1] == own, 1.0, 0.0)
            run_x = run_x + keep * conv_x[k : k + 1, :] * pre[at : at + 64, 0:el]
            run_bc = run_bc + keep * conv_bc[k : k + 1, :] * pre[at : at + 64, el + 128 :]
        xc[r0 : r0 + 64, :] = jax.nn.silu(run_x)
        bcm[r0 : r0 + 64, :] = jax.nn.silu(run_bc).astype(BF16)

    for r in range(1, toks // 64):
        convolve(r)

    def project_gate(c0, w):
        for j in range(2):
            lhs = rows_all[n_half * j : n_half * (j + 1)].reshape(m_half, d)
            gate[pl.ds(j * m_half, m_half), pl.ds(c0, w)] = jnp.dot(
                lhs, w_gate[:, pl.ds(c0, w)], preferred_element_type=F32
            )

    gate_tiles = [(c0, min(256, el - c0)) for c0 in range(0, el, 256)]
    for tile in gate_tiles[:-2]:
        project_gate(*tile)

    edge.wait_recv()
    convolve(0)

    keeps = []
    for b in range(n_blocks):
        r0 = b * BLOCK
        ld = ldb[b]
        ld_end = ld[BLOCK - 1 : BLOCK, :]
        seg = idc[8 + r0 : 8 + r0 + BLOCK, :]
        seg_end = seg[BLOCK - 1 : BLOCK, :]
        prev = idc[7 + r0 : 8 + r0, :]
        step_b = dtp[r0 : r0 + BLOCK, :]
        to_end = jnp.exp(ld_end - ld) * jnp.where(seg == seg_end, 1.0, 0.0) * step_b
        x_b = xc[r0 : r0 + BLOCK, :]
        x_w = (x_b * lanes_of(to_end, spread)).astype(BF16)
        st[b] = lax.dot_general(
            bcm[r0 : r0 + BLOCK, 0:128],
            x_w,
            (((0,), (0,)), ((), ())),
            preferred_element_type=F32,
        )
        keep = jnp.exp(ld_end) * jnp.where(seg_end == prev, 1.0, 0.0)
        keeps.append(jnp.broadcast_to(keep, (8, 128)))
    keep_lanes = [lanes_of(k, spread)[0:1, :] for k in keeps]
    total = st[0]
    keep_shard = keeps[0]
    for b in range(1, n_blocks):
        total = keep_lanes[b] * total + st[b]
        keep_shard = keep_shard * keeps[b]
    a_out[:, :, 0:el] = total.reshape(n_seq, ng, el).astype(BF16)
    keep_row = jnp.broadcast_to(keep_shard[0:1, :], (ng, 128))
    k_hi = keep_row.astype(BF16).astype(F32)
    k_mid = (keep_row - k_hi).astype(BF16).astype(F32)
    k_lo = keep_row - k_hi - k_mid
    which = lax.broadcasted_iota(jnp.int32, (ng, 128), 0)
    k_rows = jnp.where(
        which == 0, k_hi, jnp.where(which == 1, k_mid, jnp.where(which == 2, k_lo, 0.0))
    ).astype(BF16)
    for s in range(n_seq):
        a_out[s, :, el : el + 128] = k_rows

    for b in range(n_blocks):
        r0 = b * BLOCK
        seg = idc[8 + r0 : 8 + r0 + BLOCK, :]
        same = seg[:, 0:1] == seg.T[0:1, :]
        gram = lax.dot_general(
            bcm[r0 : r0 + BLOCK, 128:256],
            bcm[r0 : r0 + BLOCK, 0:128],
            (((1,), (1,)), ((), ())),
            preferred_element_type=F32,
        )
        grams[b] = jnp.where(same & (ti >= si), gram, 0.0)

    state_copies = []
    for k in far_first:
        peer = lax.rem(seq + k, n_seq)
        state_copies.append(push(a_out.at[peer], a_in.at[seq], {"seq": peer}))
    a_in[seq] = a_out[seq]
    for tile in gate_tiles[-2:]:
        project_gate(*tile)
    for b in range(n_blocks):
        r0 = b * BLOCK
        xp[r0 : r0 + BLOCK, :] = (
            xc[r0 : r0 + BLOCK, :] * lanes_of(dtp[r0 : r0 + BLOCK, :], spread)
        ).astype(BF16)

    def inside(b):
        r0 = b * BLOCK
        ld = ldb[b]
        ld_t = ld.T
        gram = grams[b]
        for pair in range(nh // 2):
            cs = slice(pair * 128, pair * 128 + 128)
            x_pair = xp[r0 : r0 + BLOCK, cs]
            outs = []
            for j in range(2):
                hh = pair * 2 + j
                a = ld[:, hh : hh + 1]
                bb = ld_t[hh : hh + 1, :]
                w0 = jnp.exp(jnp.minimum(a[0:128] - bb[:, 0:128], 0.0)) * gram[0:128, 0:128]
                w1 = jnp.exp(jnp.minimum(a[128:] - bb, 0.0)) * gram[128:, :]
                outs.append(
                    (
                        jnp.dot(w0.astype(BF16), x_pair[0:128], preferred_element_type=F32),
                        jnp.dot(w1.astype(BF16), x_pair, preferred_element_type=F32),
                    )
                )
            first = lax.broadcasted_iota(jnp.int32, (128, 128), 1) < 64
            acc[r0 : r0 + 128, cs] = jnp.where(first, outs[0][0], outs[1][0])
            acc[r0 + 128 : r0 + 256, cs] = jnp.where(first, outs[0][1], outs[1][1])

    inside(0)

    for copy in state_copies:
        copy.wait_recv()

    decay = jnp.dot(
        a_in[:, :, el : el + 128].reshape(n_seq * ng, 128), spread, preferred_element_type=F32
    )
    run = jnp.zeros((ng, el), F32)
    for s in range(n_seq):
        i_out[s] = run.astype(BF16)
        k0 = s * ng
        keep = decay[k0 : k0 + 1, :] + decay[k0 + 1 : k0 + 2, :] + decay[k0 + 2 : k0 + 3, :]
        run = keep * run + a_in[s, :, 0:el].astype(F32)
    back_copies = []
    for k in far_first:
        peer = lax.rem(seq + k, n_seq)
        back_copies.append(push(i_out.at[peer], i_in.at[seq], {"seq": peer}))
    i_in[seq] = i_out[seq]
    for b in range(1, n_blocks):
        inside(b)
    load_out.wait()

    skip = lanes_of(jnp.broadcast_to(prm[2:3, :], (8, 128)), spread)[0:1, :]
    for b in range(n_blocks):
        r0 = b * BLOCK
        rs = slice(r0, r0 + BLOCK)
        seg = idc[8 + r0 : 8 + r0 + BLOCK, :]
        prev = idc[7 + r0 : 8 + r0, :]
        acc[rs, :] = acc[rs, :] + skip * xc[rs, :]
        gate[rs, :] = jax.nn.silu(gate[rs, :])
        xc[rs, :] = lanes_of(jnp.exp(ldb[b]) * jnp.where(seg == prev, 1.0, 0.0), spread)

    for copy in back_copies:
        copy.wait_recv()

    state = i_in[...].astype(F32).reshape(128, el)
    for b in range(n_blocks):
        r0 = b * BLOCK
        inter = jnp.dot(
            bcm[r0 : r0 + BLOCK, 128:256], state.astype(BF16), preferred_element_type=F32
        )
        out = acc[r0 : r0 + BLOCK, :] + xc[r0 : r0 + BLOCK, :] * inter
        gated = out * gate[r0 : r0 + BLOCK, :]
        sq = jnp.sum(gated * gated, axis=1, keepdims=True)
        xp[r0 : r0 + BLOCK, :] = (gated * gated_gain[...]).astype(BF16)
        for q in range(2):
            col = jnp.broadcast_to(sq[q * 128 : q * 128 + 128], (128, 128))
            sq_out[b * 2 + q] = col.T[0:8, :]
        state = keep_lanes[b] * state + st[b]

    def mine(xx):
        return pl.ds(pl.multiple_of(xx * rows, rows), rows)

    zero, one = pl.ds(0, rows), pl.ds(rows, rows)
    r2u, r2d, r3u, r3d, r4u, r4d, x6 = {}, {}, {}, {}, {}, {}, {}
    lx = {}
    l2u, l2d, l3u, l3d = {}, {}, {}, {}

    def out_cols(i, between):
        for q in range(2):
            term = jnp.dot(
                xp[q * m_half : (q + 1) * m_half, :],
                w_out[:, cols[i]],
                preferred_element_type=F32,
            ).astype(BF16)
            part[q * (n_y // 2) : (q + 1) * (n_y // 2), :, cols[i]] = term.reshape(
                n_y // 2, 2 * rows, pieces[i][1]
            )
            if q == 0:
                between()

    def cross(i, yy):
        lx[i, len([k for k in lx if k[0] == i])] = push(
            part.at[yy, mine(other), cols[i]], xl_in.at[yy, :, cols[i]], at_x
        )

    def send_r3(i):
        r3u[i] = push(part.at[up, one, cols[i]], yr1.at[0, 1, :, cols[i]], at_up)
        r3d[i] = push(part.at[down, zero, cols[i]], yr1.at[1, 0, :, cols[i]], at_down)

    def first_sends(i):
        if i in rights:
            r2u[i] = push(part.at[far, zero, cols[i]], yr2.at[0, :, cols[i]], at_up)
            r2d[i] = push(part.at[far, one, cols[i]], yr2.at[1, :, cols[i]], at_down)
            if i == rights[0]:
                send_r3(i)
        else:
            cross(i, far)
            if i == lefts[0]:
                cross(i, up)
            if i == lefts[-1]:
                for yy in (up, down, y):
                    for j in lefts:
                        if not (yy is up and j == lefts[0]):
                            cross(j, yy)

    sq_copies = []

    def send_sq():
        for k in range(1, n_tp):
            peer = lax.rem(tp + k, n_tp)
            sq_copies.append(push(sq_out.at[peer // 2], sq_in.at[tp], {"tp": peer}))

    for i in every:
        out_cols(i, (lambda: first_sends(i - 1)) if i else send_sq)
    sq_in[tp] = sq_out[y]
    first_sends(len(pieces) - 1)
    for i in rights[1:2]:
        send_r3(i)

    def sum_of(*refs):
        tot = refs[0].astype(F32)
        for r in refs[1:]:
            tot = tot + r.astype(F32)
        return tot

    for i in every:
        c = cols[i]
        if i in rights:
            r2u[i].wait_recv()
            qr[0, :, c] = sum_of(part[up, zero, c], yr2[0, :, c]).astype(BF16)
            r2d[i].wait_recv()
            qr[1, :, c] = sum_of(part[down, one, c], yr2[1, :, c]).astype(BF16)
            if i in rights[2:]:
                send_r3(i)
            r4u[i] = push(qr.at[0, :, c], yr1.at[0, 0, :, c], at_up)
            r4d[i] = push(qr.at[1, :, c], yr1.at[1, 1, :, c], at_down)
        else:
            lx[i, 0].wait_recv()
            ql[far, :, c] = sum_of(part[far, mine(xl), c], xl_in[far, :, c]).astype(BF16)
            l2u[i] = push(ql.at[far, pl.ds(0, half), c], yl2.at[0, :, c], at_up)
            l2d[i] = push(ql.at[far, pl.ds(half, half), c], yl2.at[1, :, c], at_down)

    def right_sum(xx, c):
        return sum_of(part[y, mine(xx), c], yr1[0, xx, :, c], yr1[1, xx, :, c])

    for i in every:
        c = cols[i]
        if i in rights:
            for copy in (r3u[i], r3d[i], r4u[i], r4d[i]):
                copy.wait_recv()
            qx[:, c] = right_sum(other, c).astype(BF16)
            x6[i] = push(qx.at[:, c], xr_in.at[:, c], at_x)
        else:
            lx[i, 1].wait_recv()
            q_up = sum_of(part[up, mine(xl), c], xl_in[up, :, c])
            lx[i, 2].wait_recv()
            q_down = sum_of(part[down, mine(xl), c], xl_in[down, :, c])
            l2u[i].wait_recv()
            ql[up, pl.ds(0, half), c] = (q_up[0:half] + yl2[0, :, c].astype(F32)).astype(BF16)
            ql[up, pl.ds(half, half), c] = q_up[half:].astype(BF16)
            l2d[i].wait_recv()
            ql[down, pl.ds(0, half), c] = q_down[0:half].astype(BF16)
            ql[down, pl.ds(half, half), c] = (q_down[half:] + yl2[1, :, c].astype(F32)).astype(
                BF16
            )
            l3u[i] = push(ql.at[up, :, c], yl1.at[0, :, c], at_up)
            l3d[i] = push(ql.at[down, :, c], yl1.at[1, :, c], at_down)

    for copy in sq_copies:
        copy.wait_recv()
    tot = sq_in[0]
    for k in range(1, n_tp):
        tot = tot + sq_in[k]
    sqc[...] = jnp.broadcast_to(tot[0:1, :], (128, 128)).T
    factor = lax.rsqrt(sqc[mine(xl), :][:, 0:1] / (el * n_tp) + EPS)

    def finish(i, total):
        c = cols[i]
        result[:, c] = (hid[:, c].astype(F32) + factor * total).astype(BF16)

    def hand(i):
        @pl.when(pipe == 0)
        def _():
            handoff[i].start()

    for i in every:
        c = cols[i]
        if i in rights:
            own = right_sum(xl, c)
            x6[i].wait_recv()
            finish(i, own + xr_in[:, c].astype(F32))
        else:
            own = sum_of(part[y, mine(xl), c])
            for copy in (lx[i, 3], l3u[i], l3d[i]):
                copy.wait_recv()
            finish(i, own + sum_of(xl_in[y, :, c], yl1[0, :, c], yl1[1, :, c]))
        if i:
            hand(i - 1)

    for copy in sent[:8]:
        copy.wait_send()
    hand(len(pieces) - 1)
    for copy in sent[8:]:
        copy.wait_send()

    @pl.when(pipe == 0)
    def _():
        for copy in handoff:
            copy.wait_send()


def local(geo, *args):
    n_seq, n_tp, n_y, d, el, nh, pieces = geo
    (
        hidden_in,
        doc_ids,
        norm_gain,
        in_zx,
        in_bc,
        in_dt,
        conv_x,
        conv_bc,
        bias_x,
        bias_bc,
        dt_bias,
        a_log,
        d_skip,
        gated_gain,
        out_w,
    ) = args
    rows = hidden_in.shape[1]
    toks = rows * n_tp
    ng = 128 // n_seq
    n_blocks = toks // BLOCK
    n_right = sum(1 for p in pieces if p[2])
    n_left = len(pieces) - n_right
    n_msg = (
        2 + len(pieces) + 2 * (n_seq - 1) + (n_tp - 1) + 14 * n_right + 16 * n_left
    )
    vmem = pl.BlockSpec(memory_space=pltpu.VMEM)
    anyw = pl.BlockSpec(memory_space=pl.ANY)
    scratch = [
        pltpu.VMEM((d, 2, el), BF16),
        pltpu.VMEM((d, el), BF16),
        pltpu.VMEM((d, el + 128), BF16),
        pltpu.VMEM((d, 256), BF16),
        pltpu.VMEM((nh, d), BF16),
        pltpu.VMEM((el, d), BF16),
        pltpu.VMEM((rows, d), BF16),
        pltpu.VMEM((n_tp, rows, d), BF16),
        pltpu.VMEM((toks + 8, el + 384), F32),
        pltpu.VMEM((toks, el), F32),
        pltpu.VMEM((toks, el), F32),
        pltpu.VMEM((toks, 256), BF16),
        pltpu.VMEM((toks, el), BF16),
        pltpu.VMEM((toks, el), F32),
        pltpu.VMEM((toks + 8, 128), F32),
        pltpu.VMEM((toks, 128), F32),
        pltpu.VMEM((8, 128), F32),
        pltpu.VMEM((n_blocks, BLOCK, 128), F32),
        pltpu.VMEM((n_blocks, 128, el), F32),
        pltpu.VMEM((n_blocks, BLOCK, BLOCK), F32),
        pltpu.VMEM((n_seq, ng, el + 128), BF16),
        pltpu.VMEM((n_seq, ng, el + 128), BF16),
        pltpu.VMEM((n_seq, ng, el), BF16),
        pltpu.VMEM((n_seq, ng, el), BF16),
        pltpu.VMEM((n_y, 2 * rows, d), BF16),
        pltpu.VMEM((n_y, rows, d), BF16),
        pltpu.VMEM((n_y, rows, d), BF16),
        pltpu.VMEM((2, rows // 2, d), BF16),
        pltpu.VMEM((2, rows, d), BF16),
        pltpu.VMEM((2, rows, d), BF16),
        pltpu.VMEM((2, 2, rows, d), BF16),
        pltpu.VMEM((2, rows, d), BF16),
        pltpu.VMEM((rows, d), BF16),
        pltpu.VMEM((rows, d), BF16),
        pltpu.VMEM((n_y, 8, 128), F32),
        pltpu.VMEM((n_tp, 8, 128), F32),
        pltpu.VMEM((128, 128), F32),
        pltpu.SemaphoreType.DMA((n_msg,)),
        pltpu.SemaphoreType.DMA((n_msg,)),
        pltpu.SemaphoreType.DMA((6,)),
    ]
    out = pl.pallas_call(
        functools.partial(layer_kernel, geo),
        out_shape=jax.ShapeDtypeStruct((rows, d), BF16),
        in_specs=[anyw, vmem, vmem, anyw, anyw, anyw] + [vmem] * 8 + [anyw],
        out_specs=vmem,
        scratch_shapes=scratch,
        name="mixer_section",
        compiler_params=pltpu.CompilerParams(
            collective_id=0, has_side_effects=True, vmem_limit_bytes=60 * 1024 * 1024
        ),
    )(
        hidden_in[0],
        doc_ids,
        norm_gain,
        in_zx[0],
        in_bc[0],
        in_dt[0].T,
        conv_x[0],
        conv_bc[0],
        bias_x,
        bias_bc,
        dt_bias,
        a_log,
        d_skip,
        gated_gain,
        out_w[0],
    )
    return out[None, None]


def build(mesh, d, e, h):
    n_seq, n_tp = mesh.shape["seq"], mesh.shape["tp"]
    wide = 512 if d % 512 == 0 else 128
    pieces = tuple((c, wide, (c // wide) % 2 == 0) for c in range(0, d, wide))
    geo = (n_seq, n_tp, n_tp // 2, d, e // n_tp, h // n_tp, pieces)
    in_specs = (
        P(None, ("seq", "tp"), None),
        P(None, "seq"),
        P("pipe", None),
        P("pipe", None, None, "tp"),
        P("pipe", None, None),
        P("pipe", None, "tp"),
        P("pipe", None, "tp"),
        P("pipe", None, None),
        P("pipe", "tp"),
        P("pipe", None),
        P("pipe", "tp"),
        P("pipe", "tp"),
        P("pipe", "tp"),
        P("pipe", "tp"),
        P("pipe", "tp", None),
    )
    out_specs = P("pipe", None, ("seq", "tp"), None)
    return jax.shard_map(
        functools.partial(local, geo),
        mesh=mesh,
        in_specs=in_specs,
        out_specs=out_specs,
        check_vma=False,
    )


def solution(mesh):
    return build(mesh, 2560, 5120, 80)
```

```python
import functools

import jax
import jax.numpy as jnp
from jax import lax
from jax.experimental import pallas as pl
from jax.experimental.pallas import tpu as pltpu
from jax.sharding import PartitionSpec as P

BLOCK = 256
EPS = 1e-05
F32 = jnp.float32
BF16 = jnp.bfloat16
MESH = pl.DeviceIdType.MESH


def lanes_of(v, spread):
    hi = v.astype(BF16)
    lo = (v - hi.astype(F32)).astype(BF16)
    return jnp.dot(hi, spread, preferred_element_type=F32) + jnp.dot(
        lo, spread, preferred_element_type=F32
    )


def layer_kernel(
    geo,
    hidden_hbm,
    ids_ref,
    norm_gain,
    zx_hbm,
    bc_hbm,
    dt_hbm,
    conv_x,
    conv_bc,
    bias_x,
    bias_bc,
    dt_bias,
    a_log,
    d_skip,
    gated_gain,
    out_hbm,
    result,
    w_raw,
    w_gate,
    w_x,
    w_bc,
    w_dt,
    w_out,
    rows_pre,
    rows_in,
    rows_all,
    pre,
    gate,
    xc,
    bcm,
    xp,
    acc,
    idc,
    dtp,
    prm,
    ldb,
    st,
    grams,
    a_out,
    a_in,
    i_out,
    i_in,
    part,
    xl_in,
    ql,
    yl2,
    yl1,
    yr2,
    yr1,
    qr,
    qx,
    xr_in,
    sq_out,
    sq_in,
    sqc,
    send_sem,
    recv_sem,
    load_sem,
):
    n_seq, n_tp, n_y, d, el, nh, pieces = geo
    pipe, seq, tp = lax.axis_index("pipe"), lax.axis_index("seq"), lax.axis_index("tp")
    y, xl = tp // 2, tp % 2
    other = 1 - xl
    rows = rows_in.shape[1]
    toks = n_tp * rows
    half = rows // 2
    n_blocks = toks // BLOCK
    ng = 128 // n_seq
    up, down = lax.rem(y + 1, n_y), lax.rem(y + n_y - 1, n_y)
    far = lax.rem(y + 2, n_y)
    at_up = {"tp": up * 2 + xl}
    at_down = {"tp": down * 2 + xl}
    at_x = {"tp": y * 2 + other}
    nxt = {"seq": lax.rem(seq + 1, n_seq)}
    every = range(len(pieces))
    rights = [i for i in every if pieces[i][2]]
    lefts = [i for i in every if not pieces[i][2]]
    cols = [pl.ds(c0, w) for c0, w, _ in pieces]
    counter = [0]
    sent = []

    def remote(src, dst, where):
        k = counter[0]
        counter[0] += 1
        return pltpu.make_async_remote_copy(
            src_ref=src,
            dst_ref=dst,
            send_sem=send_sem.at[k],
            recv_sem=recv_sem.at[k],
            device_id=where,
            device_id_type=MESH,
        )

    def push(src, dst, where):
        copy = remote(src, dst, where)
        copy.start()
        sent.append(copy)
        return copy

    top, bottom = pl.ds(0, d // 2), pl.ds(d // 2, d // 2)
    load_dt, load_top, load_bottom, load_bc, load_out = loads = [
        pltpu.make_async_copy(s, t, load_sem.at[k])
        for k, (s, t) in enumerate(
            [
                (dt_hbm, w_dt),
                (zx_hbm.at[top], w_raw.at[top]),
                (zx_hbm.at[bottom], w_raw.at[bottom]),
                (bc_hbm, w_bc),
                (out_hbm, w_out),
            ]
        )
    ]
    first_load = pltpu.make_async_copy(hidden_hbm, rows_pre.at[tp], load_sem.at[5])

    @pl.when(pipe == 1)
    def _():
        first_load.start()

    for copy in loads:
        copy.start()

    far_first = sorted(range(1, n_seq), key=lambda k: abs(2 * k - n_seq))
    barrier = pltpu.get_barrier_semaphore()
    for k in far_first:
        pl.semaphore_signal(
            barrier, inc=1, device_id={"seq": lax.rem(seq + k, n_seq)}, device_id_type=MESH
        )
    for k in range(1, n_tp):
        pl.semaphore_signal(
            barrier, inc=1, device_id={"tp": lax.rem(tp + k, n_tp)}, device_id_type=MESH
        )
    pl.semaphore_signal(barrier, inc=1, device_id={"pipe": 1 - pipe}, device_id_type=MESH)

    prm[...] = jnp.zeros_like(prm)
    prm[0:1, 0:nh] = dt_bias[...]
    prm[1:2, 0:nh] = -jnp.exp(a_log[...])
    prm[2:3, 0:nh] = d_skip[...]
    ids_row = ids_ref[...].astype(F32)
    idc[8 : 8 + toks, :] = jnp.broadcast_to(ids_row, (128, toks)).T
    head = lax.broadcasted_iota(jnp.int32, (128, el), 0)
    lane = lax.broadcasted_iota(jnp.int32, (128, el), 1)
    spread = jnp.where((lane // 64) == head, 1.0, 0.0).astype(BF16)
    ti = lax.broadcasted_iota(jnp.int32, (BLOCK, BLOCK), 0)
    si = lax.broadcasted_iota(jnp.int32, (BLOCK, BLOCK), 1)

    def lay_out(lo, hi):
        def step(i, carry):
            r = pl.multiple_of(i * 64, 64)
            both = jnp.swapaxes(w_raw[pl.ds(r, 64)].astype(F32), 0, 1)
            w_gate[pl.ds(r, 64), :] = both[0].astype(BF16)
            w_x[pl.ds(r, 64), 0:el] = both[1].astype(BF16)
            return carry

        lax.fori_loop(lo, hi, step, 0)

    def lay_out_dt():
        unit = jnp.where(
            lax.broadcasted_iota(jnp.int32, (nh, 128), 0)
            == lax.broadcasted_iota(jnp.int32, (nh, 128), 1),
            1.0,
            0.0,
        ).astype(BF16)
        for r in range(0, d, 256):
            w_x[r : r + 256, el : el + 128] = lax.dot_general(
                w_dt[:, r : r + 256],
                unit,
                (((0,), (0,)), ((), ())),
                preferred_element_type=F32,
            ).astype(BF16)

    n_lay = d // 64
    load_dt.wait()
    lay_out_dt()

    @pl.when(pipe == 0)
    def _():
        load_top.wait()
        lay_out(0, n_lay // 2)
        load_bottom.wait()
        lay_out(n_lay // 2, n_lay)
        load_bc.wait()

    pl.semaphore_wait(barrier, n_tp + n_seq - 1)
    id_edge = push(idc.at[pl.ds(toks, 8)], idc.at[pl.ds(0, 8)], nxt)
    mate = {"pipe": 1 - pipe}
    handoff = [remote(result.at[:, c], rows_in.at[tp, :, c], mate) for c in cols]

    def norm_rows(yy):
        for xx in range(2):
            t = yy * 2 + xx
            h = rows_in[t].astype(F32)
            scale = lax.rsqrt(jnp.mean(h * h, axis=1, keepdims=True) + EPS)
            rows_all[t] = (h * scale * norm_gain[...]).astype(BF16)

    tiles = [(w_x, c0, c0) for c0 in range(0, el + 128, 256)] + [(w_bc, 0, el + 128)]
    tile_groups = [tiles[k : k + 2] for k in range(0, len(tiles), 2)]

    def project(pairs, group):
        lhs = jnp.concatenate(
            [rows_all[pl.ds(yy * 2, 2)].reshape(2 * rows, d) for yy in pairs], axis=0
        )
        for weight, w0, t0 in group:
            term = jnp.dot(lhs, weight[:, w0 : w0 + 256], preferred_element_type=F32)
            for k, yy in enumerate(pairs):
                at = pl.ds(pl.multiple_of(8 + yy * 2 * rows, 8), 2 * rows)
                pre[at, t0 : t0 + 256] = term[k * 2 * rows : (k + 1) * 2 * rows]

    def gather(buf, ready, early, middle, late, last):
        mine_sent = []

        def hop(yy, xx, i, where, r0=0, n=rows):
            s = buf.at[yy * 2 + xx, pl.ds(r0, n), cols[i]]
            copy = remote(s, s, where)
            copy.start()
            mine_sent.append(copy)
            return copy

        u1, d1, x1 = {}, {}, {}
        for i in every:
            ready(i)
            u1[i], d1[i] = hop(y, xl, i, at_up), hop(y, xl, i, at_down)
            x1[i] = hop(y, xl, i, at_x)
        u2, d2, x2, x3 = {}, {}, {}, {}
        for i in every:
            if i in rights:
                x1[i].wait_recv()
                u2[i], d2[i] = hop(y, other, i, at_up), hop(y, other, i, at_down)
            else:
                u1[i].wait_recv()
                u2[i] = hop(down, xl, i, at_up, 0, half)
                x2[i] = hop(down, xl, i, at_x)
                d1[i].wait_recv()
                d2[i] = hop(up, xl, i, at_down, half, half)
                x3[i] = hop(up, xl, i, at_x)
        for i in every:
            if i in rights:
                u1[i].wait_recv()
                d1[i].wait_recv()
            else:
                x1[i].wait_recv()
        early()
        u3, d3, x4 = {}, {}, {}
        for i in every:
            if i in rights:
                u2[i].wait_recv()
                u3[i] = hop(down, 0, i, at_up)
                d2[i].wait_recv()
                d3[i] = hop(up, 1, i, at_down)
            else:
                u2[i].wait_recv()
                d2[i].wait_recv()
                x4[i] = hop(far, xl, i, at_x)
            if i == 1:
                middle()
        for i in lefts:
            x2[i].wait_recv()
            x3[i].wait_recv()
        late()
        for i in every:
            for copy in (u3[i], d3[i]) if i in rights else (x4[i],):
                copy.wait_recv()
            last(i)
        return mine_sent

    def pair_of(yy):
        return pl.ds(yy * 2, 2)

    def across(at):
        return remote(rows_pre.at[at], rows_in.at[at], mate)

    own_pair = across(pair_of(y))
    near = [across(yy * 2 + xl) for yy in (down, up)]
    beside = [across(yy * 2 + other) for yy in (down, up)]
    rest = [
        remote(rows_pre.at[pair_of(far), :, c], rows_in.at[pair_of(far), :, c], mate)
        for c in cols
    ]

    @pl.when(pipe == 1)
    def _():
        first_load.wait()

        def early():
            for copy in [own_pair] + near:
                copy.start()

        def late():
            for copy in beside:
                copy.start()

        first = gather(
            rows_pre, lambda i: None, early, lambda: None, late, lambda i: rest[i].start()
        )
        load_top.wait()
        load_bottom.wait()
        lay_out(0, n_lay)
        load_bc.wait()
        for copy in first + [own_pair] + near + beside + rest:
            copy.wait_send()

    @pl.when(pipe == 1)
    def _():
        def early():
            norm_rows(y)
            project((y,), tile_groups[0])

        def middle():
            for group in tile_groups[1:]:
                project((y,), group)

        def late():
            norm_rows(down)
            norm_rows(up)

        second = gather(
            rows_in,
            lambda i: handoff[i].wait_recv(),
            early,
            middle,
            late,
            lambda i: None,
        )
        norm_rows(far)
        for group in tile_groups:
            project((up, far, down), group)
        for copy in second:
            copy.wait_send()

    @pl.when(pipe == 0)
    def _():
        for copies, yy in (
            ([own_pair], y),
            ([near[0], beside[0]], down),
            ([near[1], beside[1]], up),
            (rest, far),
        ):
            for copy in copies:
                copy.wait_recv()
            norm_rows(yy)
            for group in tile_groups:
                project((yy,), group)

    id_edge.wait_recv()
    idc[0:8, :] = jnp.where(seq > 0, idc[0:8, :], -1.0)
    n_half = n_tp // 2
    m_half = n_half * rows

    step_all = jax.nn.softplus(pre[8 : 8 + toks, el : el + 128] + prm[0:1, :])
    dtp[...] = step_all
    edge = push(pre.at[pl.ds(toks, 8)], pre.at[pl.ds(0, 8)], nxt)
    rate = step_all * prm[1:2, :]
    tri = jnp.where(ti >= si, 1.0, 0.0)
    for b in range(n_blocks):
        ldb[b] = jnp.dot(
            tri,
            rate[b * BLOCK : (b + 1) * BLOCK],
            precision=lax.Precision.HIGHEST,
            preferred_element_type=F32,
        )

    def convolve(r):
        r0 = r * 64
        own = idc[8 + r0 : 72 + r0, :][:, 0:1]
        run_x = jnp.broadcast_to(bias_x[...], (64, el))
        run_bc = jnp.broadcast_to(bias_bc[...], (64, 256))
        for k in range(4):
            at = r0 + 5 + k
            keep = jnp.where(idc[at : at + 64, :][:, 0:1] == own, 1.0, 0.0)
            run_x = run_x + keep * conv_x[k : k + 1, :] * pre[at : at + 64, 0:el]
            run_bc = run_bc + keep * conv_bc[k : k + 1, :] * pre[at : at + 64, el + 128 :]
        xc[r0 : r0 + 64, :] = jax.nn.silu(run_x)
        bcm[r0 : r0 + 64, :] = jax.nn.silu(run_bc).astype(BF16)

    for r in range(1, toks // 64):
        convolve(r)

    def project_gate(c0, w):
        for j in range(2):
            lhs = rows_all[n_half * j : n_half * (j + 1)].reshape(m_half, d)
            gate[pl.ds(j * m_half, m_half), pl.ds(c0, w)] = jnp.dot(
                lhs, w_gate[:, pl.ds(c0, w)], preferred_element_type=F32
            )

    gate_tiles = [(c0, min(256, el - c0)) for c0 in range(0, el, 256)]
    for tile in gate_tiles[:-2]:
        project_gate(*tile)

    edge.wait_recv()
    convolve(0)

    keeps = []
    for b in range(n_blocks):
        r0 = b * BLOCK
        ld = ldb[b]
        ld_end = ld[BLOCK - 1 : BLOCK, :]
        seg = idc[8 + r0 : 8 + r0 + BLOCK, :]
        seg_end = seg[BLOCK - 1 : BLOCK, :]
        prev = idc[7 + r0 : 8 + r0, :]
        step_b = dtp[r0 : r0 + BLOCK, :]
        to_end = jnp.exp(ld_end - ld) * jnp.where(seg == seg_end, 1.0, 0.0) * step_b
        x_b = xc[r0 : r0 + BLOCK, :]
        x_w = (x_b * lanes_of(to_end, spread)).astype(BF16)
        st[b] = lax.dot_general(
            bcm[r0 : r0 + BLOCK, 0:128],
            x_w,
            (((0,), (0,)), ((), ())),
            preferred_element_type=F32,
        )
        keep = jnp.exp(ld_end) * jnp.where(seg_end == prev, 1.0, 0.0)
        keeps.append(jnp.broadcast_to(keep, (8, 128)))
    keep_lanes = [lanes_of(k, spread)[0:1, :] for k in keeps]
    total = st[0]
    keep_shard = keeps[0]
    for b in range(1, n_blocks):
        total = keep_lanes[b] * total + st[b]
        keep_shard = keep_shard * keeps[b]
    a_out[:, :, 0:el] = total.reshape(n_seq, ng, el).astype(BF16)
    keep_row = jnp.broadcast_to(keep_shard[0:1, :], (ng, 128))
    k_hi = keep_row.astype(BF16).astype(F32)
    k_mid = (keep_row - k_hi).astype(BF16).astype(F32)
    k_lo = keep_row - k_hi - k_mid
    which = lax.broadcasted_iota(jnp.int32, (ng, 128), 0)
    k_rows = jnp.where(
        which == 0, k_hi, jnp.where(which == 1, k_mid, jnp.where(which == 2, k_lo, 0.0))
    ).astype(BF16)
    for s in range(n_seq):
        a_out[s, :, el : el + 128] = k_rows

    for b in range(n_blocks):
        r0 = b * BLOCK
        seg = idc[8 + r0 : 8 + r0 + BLOCK, :]
        same = seg[:, 0:1] == seg.T[0:1, :]
        gram = lax.dot_general(
            bcm[r0 : r0 + BLOCK, 128:256],
            bcm[r0 : r0 + BLOCK, 0:128],
            (((1,), (1,)), ((), ())),
            preferred_element_type=F32,
        )
        grams[b] = jnp.where(same & (ti >= si), gram, 0.0)

    state_copies = []
    for k in far_first:
        peer = lax.rem(seq + k, n_seq)
        state_copies.append(push(a_out.at[peer], a_in.at[seq], {"seq": peer}))
    a_in[seq] = a_out[seq]
    for tile in gate_tiles[-2:]:
        project_gate(*tile)
    for b in range(n_blocks):
        r0 = b * BLOCK
        xp[r0 : r0 + BLOCK, :] = (
            xc[r0 : r0 + BLOCK, :] * lanes_of(dtp[r0 : r0 + BLOCK, :], spread)
        ).astype(BF16)

    def inside(b):
        r0 = b * BLOCK
        ld = ldb[b]
        ld_t = ld.T
        gram = grams[b]
        for pair in range(nh // 2):
            cs = slice(pair * 128, pair * 128 + 128)
            x_pair = xp[r0 : r0 + BLOCK, cs]
            outs = []
            for j in range(2):
                hh = pair * 2 + j
                a = ld[:, hh : hh + 1]
                bb = ld_t[hh : hh + 1, :]
                w0 = jnp.exp(jnp.minimum(a[0:128] - bb[:, 0:128], 0.0)) * gram[0:128, 0:128]
                w1 = jnp.exp(jnp.minimum(a[128:] - bb, 0.0)) * gram[128:, :]
                outs.append(
                    (
                        jnp.dot(w0.astype(BF16), x_pair[0:128], preferred_element_type=F32),
                        jnp.dot(w1.astype(BF16), x_pair, preferred_element_type=F32),
                    )
                )
            first = lax.broadcasted_iota(jnp.int32, (128, 128), 1) < 64
            acc[r0 : r0 + 128, cs] = jnp.where(first, outs[0][0], outs[1][0])
            acc[r0 + 128 : r0 + 256, cs] = jnp.where(first, outs[0][1], outs[1][1])

    inside(0)

    for copy in state_copies:
        copy.wait_recv()

    decay = jnp.dot(
        a_in[:, :, el : el + 128].reshape(n_seq * ng, 128), spread, preferred_element_type=F32
    )
    run = jnp.zeros((ng, el), F32)
    for s in range(n_seq):
        i_out[s] = run.astype(BF16)
        k0 = s * ng
        keep = decay[k0 : k0 + 1, :] + decay[k0 + 1 : k0 + 2, :] + decay[k0 + 2 : k0 + 3, :]
        run = keep * run + a_in[s, :, 0:el].astype(F32)
    back_copies = []
    for k in far_first:
        peer = lax.rem(seq + k, n_seq)
        back_copies.append(push(i_out.at[peer], i_in.at[seq], {"seq": peer}))
    i_in[seq] = i_out[seq]
    for b in range(1, n_blocks):
        inside(b)
    load_out.wait()

    skip = lanes_of(jnp.broadcast_to(prm[2:3, :], (8, 128)), spread)[0:1, :]
    for b in range(n_blocks):
        r0 = b * BLOCK
        rs = slice(r0, r0 + BLOCK)
        seg = idc[8 + r0 : 8 + r0 + BLOCK, :]
        prev = idc[7 + r0 : 8 + r0, :]
        acc[rs, :] = acc[rs, :] + skip * xc[rs, :]
        gate[rs, :] = jax.nn.silu(gate[rs, :])
        xc[rs, :] = lanes_of(jnp.exp(ldb[b]) * jnp.where(seg == prev, 1.0, 0.0), spread)

    for copy in back_copies:
        copy.wait_recv()

    state = i_in[...].astype(F32).reshape(128, el)
    for b in range(n_blocks):
        r0 = b * BLOCK
        inter = jnp.dot(
            bcm[r0 : r0 + BLOCK, 128:256], state.astype(BF16), preferred_element_type=F32
        )
        out = acc[r0 : r0 + BLOCK, :] + xc[r0 : r0 + BLOCK, :] * inter
        gated = out * gate[r0 : r0 + BLOCK, :]
        sq = jnp.sum(gated * gated, axis=1, keepdims=True)
        xp[r0 : r0 + BLOCK, :] = (gated * gated_gain[...]).astype(BF16)
        for q in range(2):
            col = jnp.broadcast_to(sq[q * 128 : q * 128 + 128], (128, 128))
            sq_out[b * 2 + q] = col.T[0:8, :]
        state = keep_lanes[b] * state + st[b]

    def mine(xx):
        return pl.ds(pl.multiple_of(xx * rows, rows), rows)

    zero, one = pl.ds(0, rows), pl.ds(rows, rows)
    r2u, r2d, r3u, r3d, r4u, r4d, x6 = {}, {}, {}, {}, {}, {}, {}
    lx = {}
    l2u, l2d, l3u, l3d = {}, {}, {}, {}

    def out_cols(i, between):
        for q in range(2):
            term = jnp.dot(
                xp[q * m_half : (q + 1) * m_half, :],
                w_out[:, cols[i]],
                preferred_element_type=F32,
            ).astype(BF16)
            part[q * (n_y // 2) : (q + 1) * (n_y // 2), :, cols[i]] = term.reshape(
                n_y // 2, 2 * rows, pieces[i][1]
            )
            if q == 0:
                between()

    def cross(i, yy):
        lx[i, len([k for k in lx if k[0] == i])] = push(
            part.at[yy, mine(other), cols[i]], xl_in.at[yy, :, cols[i]], at_x
        )

    def send_r3(i):
        r3u[i] = push(part.at[up, one, cols[i]], yr1.at[0, 1, :, cols[i]], at_up)
        r3d[i] = push(part.at[down, zero, cols[i]], yr1.at[1, 0, :, cols[i]], at_down)

    def first_sends(i):
        if i in rights:
            r2u[i] = push(part.at[far, zero, cols[i]], yr2.at[0, :, cols[i]], at_up)
            r2d[i] = push(part.at[far, one, cols[i]], yr2.at[1, :, cols[i]], at_down)
            if i == rights[0]:
                send_r3(i)
        else:
            cross(i, far)
            if i == lefts[0]:
                cross(i, up)
            if i == lefts[-1]:
                for yy in (up, down, y):
                    for j in lefts:
                        if not (yy is up and j == lefts[0]):
                            cross(j, yy)

    sq_copies = []

    def send_sq():
        for k in range(1, n_tp):
            peer = lax.rem(tp + k, n_tp)
            sq_copies.append(push(sq_out.at[peer // 2], sq_in.at[tp], {"tp": peer}))

    for i in every:
        out_cols(i, (lambda: first_sends(i - 1)) if i else send_sq)
    sq_in[tp] = sq_out[y]
    first_sends(len(pieces) - 1)
    for i in rights[1:2]:
        send_r3(i)

    def sum_of(*refs):
        tot = refs[0].astype(F32)
        for r in refs[1:]:
            tot = tot + r.astype(F32)
        return tot

    for i in every:
        c = cols[i]
        if i in rights:
            r2u[i].wait_recv()
            qr[0, :, c] = sum_of(part[up, zero, c], yr2[0, :, c]).astype(BF16)
            r2d[i].wait_recv()
            qr[1, :, c] = sum_of(part[down, one, c], yr2[1, :, c]).astype(BF16)
            if i in rights[2:]:
                send_r3(i)
            r4u[i] = push(qr.at[0, :, c], yr1.at[0, 0, :, c], at_up)
            r4d[i] = push(qr.at[1, :, c], yr1.at[1, 1, :, c], at_down)
        else:
            lx[i, 0].wait_recv()
            ql[far, :, c] = sum_of(part[far, mine(xl), c], xl_in[far, :, c]).astype(BF16)
            l2u[i] = push(ql.at[far, pl.ds(0, half), c], yl2.at[0, :, c], at_up)
            l2d[i] = push(ql.at[far, pl.ds(half, half), c], yl2.at[1, :, c], at_down)

    def right_sum(xx, c):
        return sum_of(part[y, mine(xx), c], yr1[0, xx, :, c], yr1[1, xx, :, c])

    for i in every:
        c = cols[i]
        if i in rights:
            for copy in (r3u[i], r3d[i], r4u[i], r4d[i]):
                copy.wait_recv()
            qx[:, c] = right_sum(other, c).astype(BF16)
            x6[i] = push(qx.at[:, c], xr_in.at[:, c], at_x)
        else:
            lx[i, 1].wait_recv()
            q_up = sum_of(part[up, mine(xl), c], xl_in[up, :, c])
            lx[i, 2].wait_recv()
            q_down = sum_of(part[down, mine(xl), c], xl_in[down, :, c])
            l2u[i].wait_recv()
            ql[up, pl.ds(0, half), c] = (q_up[0:half] + yl2[0, :, c].astype(F32)).astype(BF16)
            ql[up, pl.ds(half, half), c] = q_up[half:].astype(BF16)
            l2d[i].wait_recv()
            ql[down, pl.ds(0, half), c] = q_down[0:half].astype(BF16)
            ql[down, pl.ds(half, half), c] = (q_down[half:] + yl2[1, :, c].astype(F32)).astype(
                BF16
            )
            l3u[i] = push(ql.at[up, :, c], yl1.at[0, :, c], at_up)
            l3d[i] = push(ql.at[down, :, c], yl1.at[1, :, c], at_down)

    for copy in sq_copies:
        copy.wait_recv()
    tot = sq_in[0]
    for k in range(1, n_tp):
        tot = tot + sq_in[k]
    sqc[...] = jnp.broadcast_to(tot[0:1, :], (128, 128)).T
    factor = lax.rsqrt(sqc[mine(xl), :][:, 0:1] / (el * n_tp) + EPS)

    def finish(i, total):
        c = cols[i]
        result[:, c] = (rows_in[tp, :, c].astype(F32) + factor * total).astype(BF16)

    def hand(i):
        @pl.when(pipe == 0)
        def _():
            handoff[i].start()

    for i in every:
        c = cols[i]
        if i in rights:
            own = right_sum(xl, c)
            x6[i].wait_recv()
            finish(i, own + xr_in[:, c].astype(F32))
        else:
            own = sum_of(part[y, mine(xl), c])
            for copy in (lx[i, 3], l3u[i], l3d[i]):
                copy.wait_recv()
            finish(i, own + sum_of(xl_in[y, :, c], yl1[0, :, c], yl1[1, :, c]))
        if i:
            hand(i - 1)

    for copy in sent[:8]:
        copy.wait_send()
    hand(len(pieces) - 1)
    for copy in sent[8:]:
        copy.wait_send()

    @pl.when(pipe == 0)
    def _():
        for copy in handoff:
            copy.wait_send()


def local(geo, *args):
    n_seq, n_tp, n_y, d, el, nh, pieces = geo
    (
        hidden_in,
        doc_ids,
        norm_gain,
        in_zx,
        in_bc,
        in_dt,
        conv_x,
        conv_bc,
        bias_x,
        bias_bc,
        dt_bias,
        a_log,
        d_skip,
        gated_gain,
        out_w,
    ) = args
    rows = hidden_in.shape[1]
    toks = rows * n_tp
    ng = 128 // n_seq
    n_blocks = toks // BLOCK
    n_right = sum(1 for p in pieces if p[2])
    n_left = len(pieces) - n_right
    n_msg = (
        7 + 2 * len(pieces) + 2 * (n_seq - 1) + (n_tp - 1) + 21 * n_right + 24 * n_left
    )
    vmem = pl.BlockSpec(memory_space=pltpu.VMEM)
    anyw = pl.BlockSpec(memory_space=pl.ANY)
    scratch = [
        pltpu.VMEM((d, 2, el), BF16),
        pltpu.VMEM((d, el), BF16),
        pltpu.VMEM((d, el + 128), BF16),
        pltpu.VMEM((d, 256), BF16),
        pltpu.VMEM((nh, d), BF16),
        pltpu.VMEM((el, d), BF16),
        pltpu.VMEM((n_tp, rows, d), BF16),
        pltpu.VMEM((n_tp, rows, d), BF16),
        pltpu.VMEM((n_tp, rows, d), BF16),
        pltpu.VMEM((toks + 8, el + 384), F32),
        pltpu.VMEM((toks, el), F32),
        pltpu.VMEM((toks, el), F32),
        pltpu.VMEM((toks, 256), BF16),
        pltpu.VMEM((toks, el), BF16),
        pltpu.VMEM((toks, el), F32),
        pltpu.VMEM((toks + 8, 128), F32),
        pltpu.VMEM((toks, 128), F32),
        pltpu.VMEM((8, 128), F32),
        pltpu.VMEM((n_blocks, BLOCK, 128), F32),
        pltpu.VMEM((n_blocks, 128, el), F32),
        pltpu.VMEM((n_blocks, BLOCK, BLOCK), F32),
        pltpu.VMEM((n_seq, ng, el + 128), BF16),
        pltpu.VMEM((n_seq, ng, el + 128), BF16),
        pltpu.VMEM((n_seq, ng, el), BF16),
        pltpu.VMEM((n_seq, ng, el), BF16),
        pltpu.VMEM((n_y, 2 * rows, d), BF16),
        pltpu.VMEM((n_y, rows, d), BF16),
        pltpu.VMEM((n_y, rows, d), BF16),
        pltpu.VMEM((2, rows // 2, d), BF16),
        pltpu.VMEM((2, rows, d), BF16),
        pltpu.VMEM((2, rows, d), BF16),
        pltpu.VMEM((2, 2, rows, d), BF16),
        pltpu.VMEM((2, rows, d), BF16),
        pltpu.VMEM((rows, d), BF16),
        pltpu.VMEM((rows, d), BF16),
        pltpu.VMEM((n_y, 8, 128), F32),
        pltpu.VMEM((n_tp, 8, 128), F32),
        pltpu.VMEM((128, 128), F32),
        pltpu.SemaphoreType.DMA((n_msg,)),
        pltpu.SemaphoreType.DMA((n_msg,)),
        pltpu.SemaphoreType.DMA((6,)),
    ]
    out = pl.pallas_call(
        functools.partial(layer_kernel, geo),
        out_shape=jax.ShapeDtypeStruct((rows, d), BF16),
        in_specs=[anyw, vmem, vmem, anyw, anyw, anyw] + [vmem] * 8 + [anyw],
        out_specs=vmem,
        scratch_shapes=scratch,
        name="mixer_section",
        compiler_params=pltpu.CompilerParams(
            collective_id=0, has_side_effects=True, vmem_limit_bytes=60 * 1024 * 1024
        ),
    )(
        hidden_in[0],
        doc_ids,
        norm_gain,
        in_zx[0],
        in_bc[0],
        in_dt[0].T,
        conv_x[0],
        conv_bc[0],
        bias_x,
        bias_bc,
        dt_bias,
        a_log,
        d_skip,
        gated_gain,
        out_w[0],
    )
    return out[None, None]


def build(mesh, d, e, h):
    n_seq, n_tp = mesh.shape["seq"], mesh.shape["tp"]
    wide = 512 if d % 512 == 0 else 128
    pieces = tuple((c, wide, (c // wide) % 2 == 0) for c in range(0, d, wide))
    geo = (n_seq, n_tp, n_tp // 2, d, e // n_tp, h // n_tp, pieces)
    in_specs = (
        P(None, ("seq", "tp"), None),
        P(None, "seq"),
        P("pipe", None),
        P("pipe", None, None, "tp"),
        P("pipe", None, None),
        P("pipe", None, "tp"),
        P("pipe", None, "tp"),
        P("pipe", None, None),
        P("pipe", "tp"),
        P("pipe", None),
        P("pipe", "tp"),
        P("pipe", "tp"),
        P("pipe", "tp"),
        P("pipe", "tp"),
        P("pipe", "tp", None),
    )
    out_specs = P("pipe", None, ("seq", "tp"), None)
    return jax.shard_map(
        functools.partial(local, geo),
        mesh=mesh,
        in_specs=in_specs,
        out_specs=out_specs,
        check_vma=False,
    )


def solution(mesh):
    return build(mesh, 2560, 5120, 80)
```

```python
import functools

import jax
import jax.numpy as jnp
from jax import lax
from jax.experimental import pallas as pl
from jax.experimental.pallas import tpu as pltpu
from jax.sharding import PartitionSpec as P

BLOCK = 256
EPS = 1e-05
F32 = jnp.float32
BF16 = jnp.bfloat16
MESH = pl.DeviceIdType.MESH


def lanes_of(v, spread):
    hi = v.astype(BF16)
    lo = (v - hi.astype(F32)).astype(BF16)
    return jnp.dot(hi, spread, preferred_element_type=F32) + jnp.dot(
        lo, spread, preferred_element_type=F32
    )


def layer_kernel(
    geo,
    hidden_hbm,
    ids_ref,
    norm_gain,
    zx_hbm,
    bc_hbm,
    dt_hbm,
    conv_x,
    conv_bc,
    bias_x,
    bias_bc,
    dt_bias,
    a_log,
    d_skip,
    gated_gain,
    out_hbm,
    result,
    w_raw,
    w_gate,
    w_x,
    w_bc,
    w_dt,
    w_out,
    rows_pre,
    rows_in,
    rows_all,
    pre,
    gate,
    xc,
    bcm,
    xp,
    acc,
    idc,
    dtp,
    prm,
    ldb,
    st,
    grams,
    a_out,
    a_in,
    i_out,
    i_in,
    part,
    xl_in,
    ql,
    yl2,
    yl1,
    yr2,
    yr1,
    qr,
    qx,
    xr_in,
    sq_out,
    sq_in,
    sqc,
    send_sem,
    recv_sem,
    load_sem,
):
    n_seq, n_tp, n_y, d, el, nh, pieces = geo
    pipe, seq, tp = lax.axis_index("pipe"), lax.axis_index("seq"), lax.axis_index("tp")
    y, xl = tp // 2, tp % 2
    other = 1 - xl
    rows = rows_in.shape[1]
    toks = n_tp * rows
    half = rows // 2
    n_blocks = toks // BLOCK
    ng = 128 // n_seq
    up, down = lax.rem(y + 1, n_y), lax.rem(y + n_y - 1, n_y)
    far = lax.rem(y + 2, n_y)
    at_up = {"tp": up * 2 + xl}
    at_down = {"tp": down * 2 + xl}
    at_x = {"tp": y * 2 + other}
    nxt = {"seq": lax.rem(seq + 1, n_seq)}
    every = range(len(pieces))
    rights = [i for i in every if pieces[i][3]]
    lefts = [i for i in every if not pieces[i][3]]
    cols = [pl.ds(c0, w) for c0, w, _, _ in pieces]
    counter = [0]
    sent = []

    def remote(src, dst, where):
        k = counter[0]
        counter[0] += 1
        return pltpu.make_async_remote_copy(
            src_ref=src,
            dst_ref=dst,
            send_sem=send_sem.at[k],
            recv_sem=recv_sem.at[k],
            device_id=where,
            device_id_type=MESH,
        )

    def push(src, dst, where):
        copy = remote(src, dst, where)
        copy.start()
        sent.append(copy)
        return copy

    top, bottom = pl.ds(0, d // 2), pl.ds(d // 2, d // 2)
    load_dt, load_top, load_bottom, load_bc, load_out = loads = [
        pltpu.make_async_copy(s, t, load_sem.at[k])
        for k, (s, t) in enumerate(
            [
                (dt_hbm, w_dt),
                (zx_hbm.at[top], w_raw.at[top]),
                (zx_hbm.at[bottom], w_raw.at[bottom]),
                (bc_hbm, w_bc),
                (out_hbm, w_out),
            ]
        )
    ]
    first_load = pltpu.make_async_copy(hidden_hbm, rows_pre.at[tp], load_sem.at[5])

    @pl.when(pipe == 1)
    def _():
        first_load.start()

    for copy in loads:
        copy.start()

    far_first = sorted(range(1, n_seq), key=lambda k: (k % 2 == 0, abs(2 * k - n_seq)))
    barrier = pltpu.get_barrier_semaphore()
    for k in far_first:
        pl.semaphore_signal(
            barrier, inc=1, device_id={"seq": lax.rem(seq + k, n_seq)}, device_id_type=MESH
        )
    for k in range(1, n_tp):
        pl.semaphore_signal(
            barrier, inc=1, device_id={"tp": lax.rem(tp + k, n_tp)}, device_id_type=MESH
        )
    pl.semaphore_signal(barrier, inc=1, device_id={"pipe": 1 - pipe}, device_id_type=MESH)

    prm[...] = jnp.zeros_like(prm)
    prm[0:1, 0:nh] = dt_bias[...]
    prm[1:2, 0:nh] = -jnp.exp(a_log[...])
    prm[2:3, 0:nh] = d_skip[...]
    ids_row = ids_ref[...].astype(F32)
    idc[8 : 8 + toks, :] = jnp.broadcast_to(ids_row, (128, toks)).T
    head = lax.broadcasted_iota(jnp.int32, (128, el), 0)
    lane = lax.broadcasted_iota(jnp.int32, (128, el), 1)
    spread = jnp.where((lane // 64) == head, 1.0, 0.0).astype(BF16)
    ti = lax.broadcasted_iota(jnp.int32, (BLOCK, BLOCK), 0)
    si = lax.broadcasted_iota(jnp.int32, (BLOCK, BLOCK), 1)

    def lay_out(lo, hi):
        def step(i, carry):
            r = pl.multiple_of(i * 64, 64)
            both = jnp.swapaxes(w_raw[pl.ds(r, 64)].astype(F32), 0, 1)
            w_gate[pl.ds(r, 64), :] = both[0].astype(BF16)
            w_x[pl.ds(r, 64), 0:el] = both[1].astype(BF16)
            return carry

        lax.fori_loop(lo, hi, step, 0)

    def lay_out_dt():
        unit = jnp.where(
            lax.broadcasted_iota(jnp.int32, (nh, 128), 0)
            == lax.broadcasted_iota(jnp.int32, (nh, 128), 1),
            1.0,
            0.0,
        ).astype(BF16)
        for r in range(0, d, 256):
            w_x[r : r + 256, el : el + 128] = lax.dot_general(
                w_dt[:, r : r + 256],
                unit,
                (((0,), (0,)), ((), ())),
                preferred_element_type=F32,
            ).astype(BF16)

    n_lay = d // 64

    @pl.when(pipe == 0)
    def _():
        load_dt.wait()
        lay_out_dt()
        load_top.wait()
        lay_out(0, n_lay // 2)
        load_bottom.wait()
        lay_out(n_lay // 2, n_lay)
        load_bc.wait()

    pl.semaphore_wait(barrier, n_tp + n_seq - 1)
    id_edge = push(idc.at[pl.ds(toks, 8)], idc.at[pl.ds(0, 8)], nxt)
    mate = {"pipe": 1 - pipe}
    handoff = [remote(result.at[:, c], rows_in.at[tp, :, c], mate) for c in cols]

    own_rows = (y * 2, y * 2 + 1)
    near_rows = (down * 2 + xl, up * 2 + xl)
    beside_rows = (down * 2 + other, up * 2 + other)
    far_rows = (far * 2, far * 2 + 1)

    def norm_rows(slots):
        for t in slots:
            h = rows_in[t].astype(F32)
            scale = lax.rsqrt(jnp.mean(h * h, axis=1, keepdims=True) + EPS)
            rows_all[t] = (h * scale * norm_gain[...]).astype(BF16)

    tiles = [(w_x, c0, c0) for c0 in range(0, el + 128, 256)] + [(w_bc, 0, el + 128)]
    tile_groups = [tiles[k : k + 2] for k in range(0, len(tiles), 2)]

    def project(slots, group):
        lhs = jnp.concatenate([rows_all[t] for t in slots], axis=0)
        for weight, w0, t0 in group:
            term = jnp.dot(lhs, weight[:, w0 : w0 + 256], preferred_element_type=F32)
            for k, t in enumerate(slots):
                at = pl.ds(pl.multiple_of(8 + t * rows, 8), rows)
                pre[at, t0 : t0 + 256] = term[k * rows : (k + 1) * rows]

    def take(slots):
        norm_rows(slots)
        for group in tile_groups:
            project(slots, group)

    def gather(buf, ready, early, late, last):
        mine_sent = []

        def hop(yy, xx, i, where, r0=0, n=rows):
            s = buf.at[yy * 2 + xx, pl.ds(r0, n), cols[i]]
            copy = remote(s, s, where)
            copy.start()
            mine_sent.append(copy)
            return copy

        u1, d1, x1 = {}, {}, {}
        for i in every:
            ready(i)
            u1[i], d1[i] = hop(y, xl, i, at_up), hop(y, xl, i, at_down)
            x1[i] = hop(y, xl, i, at_x)
        u2, d2, x2, x3 = {}, {}, {}, {}
        for i in every:
            if pieces[i][2]:
                x1[i].wait_recv()
                u2[i], d2[i] = hop(y, other, i, at_up), hop(y, other, i, at_down)
            else:
                u1[i].wait_recv()
                u2[i] = hop(down, xl, i, at_up, 0, half)
                x2[i] = hop(down, xl, i, at_x)
                d1[i].wait_recv()
                d2[i] = hop(up, xl, i, at_down, half, half)
                x3[i] = hop(up, xl, i, at_x)
        for i in every:
            if pieces[i][2]:
                u1[i].wait_recv()
                d1[i].wait_recv()
            else:
                x1[i].wait_recv()
        early()
        u3, d3, x4 = {}, {}, {}
        for i in every:
            if pieces[i][2]:
                u2[i].wait_recv()
                u3[i] = hop(down, 0, i, at_up)
                d2[i].wait_recv()
                d3[i] = hop(up, 1, i, at_down)
            else:
                u2[i].wait_recv()
                d2[i].wait_recv()
                x4[i] = hop(far, xl, i, at_x)
        for i in x2:
            x2[i].wait_recv()
            x3[i].wait_recv()
        late()
        for i in every:
            for copy in (u3[i], d3[i]) if pieces[i][2] else (x4[i],):
                copy.wait_recv()
            last(i)
        return mine_sent

    def pair_of(yy):
        return pl.ds(yy * 2, 2)

    def across(at):
        return remote(rows_pre.at[at], rows_in.at[at], mate)

    own_pair = across(pair_of(y))
    near = [across(yy * 2 + xl) for yy in (down, up)]
    beside = [across(yy * 2 + other) for yy in (down, up)]
    rest = [
        remote(rows_pre.at[pair_of(far), :, c], rows_in.at[pair_of(far), :, c], mate)
        for c in cols
    ]

    @pl.when(pipe == 1)
    def _():
        first_load.wait()

        def early():
            for copy in [own_pair] + near:
                copy.start()

        def late():
            for copy in beside:
                copy.start()

        first = gather(
            rows_pre, lambda i: None, early, late, lambda i: rest[i].start()
        )
        load_dt.wait()
        lay_out_dt()
        load_top.wait()
        load_bottom.wait()
        lay_out(0, n_lay)
        load_bc.wait()
        for copy in first + [own_pair] + near + beside + rest:
            copy.wait_send()

    @pl.when(pipe == 1)
    def _():
        def early():
            take(own_rows)

        def late():
            take(near_rows)
            take(beside_rows)

        second = gather(
            rows_in,
            lambda i: handoff[i].wait_recv(),
            early,
            late,
            lambda i: None,
        )
        take(far_rows)
        for copy in second:
            copy.wait_send()

    @pl.when(pipe == 0)
    def _():
        for copies, slots in (
            ([own_pair], own_rows),
            (near, near_rows),
            (beside, beside_rows),
            (rest, far_rows),
        ):
            for copy in copies:
                copy.wait_recv()
            take(slots)

    id_edge.wait_recv()
    idc[0:8, :] = jnp.where(seq > 0, idc[0:8, :], -1.0)
    n_half = n_tp // 2
    m_half = n_half * rows

    step_all = jax.nn.softplus(pre[8 : 8 + toks, el : el + 128] + prm[0:1, :])
    dtp[...] = step_all
    edge = push(pre.at[pl.ds(toks, 8)], pre.at[pl.ds(0, 8)], nxt)
    rate = step_all * prm[1:2, :]
    tri = jnp.where(ti >= si, 1.0, 0.0).astype(BF16)
    r_hi = rate.astype(BF16)
    r_rest = rate - r_hi.astype(F32)
    r_mid = r_rest.astype(BF16)
    r_lo = (r_rest - r_mid.astype(F32)).astype(BF16)
    for b in range(n_blocks):
        ldb[b] = sum(
            jnp.dot(tri, r[b * BLOCK : (b + 1) * BLOCK], preferred_element_type=F32)
            for r in (r_lo, r_mid, r_hi)
        )

    def convolve(r):
        r0 = r * 64
        own = idc[8 + r0 : 72 + r0, :][:, 0:1]
        run_x = jnp.broadcast_to(bias_x[...], (64, el))
        run_bc = jnp.broadcast_to(bias_bc[...], (64, 256))
        for k in range(4):
            at = r0 + 5 + k
            tap_x, tap_bc = conv_x[k : k + 1, :], conv_bc[k : k + 1, :]
            if k < 3:
                keep = jnp.where(idc[at : at + 64, :][:, 0:1] == own, 1.0, 0.0)
                tap_x, tap_bc = keep * tap_x, keep * tap_bc
            run_x = run_x + tap_x * pre[at : at + 64, 0:el]
            run_bc = run_bc + tap_bc * pre[at : at + 64, el + 128 :]
        xc[r0 : r0 + 64, :] = jax.nn.silu(run_x)
        bcm[r0 : r0 + 64, :] = jax.nn.silu(run_bc).astype(BF16)

    for r in range(1, toks // 64):
        convolve(r)

    def project_gate(c0, w):
        for j in range(2):
            lhs = rows_all[n_half * j : n_half * (j + 1)].reshape(m_half, d)
            gate[pl.ds(j * m_half, m_half), pl.ds(c0, w)] = jnp.dot(
                lhs, w_gate[:, pl.ds(c0, w)], preferred_element_type=F32
            )

    gate_tiles = [(c0, min(256, el - c0)) for c0 in range(0, el, 256)]
    for tile in gate_tiles[:-2]:
        project_gate(*tile)

    keeps = [None] * n_blocks

    def states(b):
        r0 = b * BLOCK
        ld = ldb[b]
        ld_end = ld[BLOCK - 1 : BLOCK, :]
        seg = idc[8 + r0 : 8 + r0 + BLOCK, :]
        seg_end = seg[BLOCK - 1 : BLOCK, :]
        prev = idc[7 + r0 : 8 + r0, :]
        step_b = dtp[r0 : r0 + BLOCK, :]
        to_end = jnp.exp(ld_end - ld) * jnp.where(seg == seg_end, 1.0, 0.0) * step_b
        x_b = xc[r0 : r0 + BLOCK, :]
        x_w = (x_b * lanes_of(to_end, spread)).astype(BF16)
        st[b] = lax.dot_general(
            bcm[r0 : r0 + BLOCK, 0:128],
            x_w,
            (((0,), (0,)), ((), ())),
            preferred_element_type=F32,
        )
        keep = jnp.exp(ld_end) * jnp.where(seg_end == prev, 1.0, 0.0)
        keeps[b] = jnp.broadcast_to(keep, (8, 128))

    for b in range(1, n_blocks):
        states(b)
    edge.wait_recv()
    convolve(0)
    states(0)
    keep_lanes = [lanes_of(k, spread)[0:1, :] for k in keeps]
    total = st[0]
    keep_shard = keeps[0]
    for b in range(1, n_blocks):
        total = keep_lanes[b] * total + st[b]
        keep_shard = keep_shard * keeps[b]
    a_out[:, :, 0:el] = total.reshape(n_seq, ng, el).astype(BF16)
    keep_row = jnp.broadcast_to(keep_shard[0:1, :], (ng, 128))
    k_hi = keep_row.astype(BF16).astype(F32)
    k_mid = (keep_row - k_hi).astype(BF16).astype(F32)
    k_lo = keep_row - k_hi - k_mid
    which = lax.broadcasted_iota(jnp.int32, (ng, 128), 0)
    k_rows = jnp.where(
        which == 0, k_hi, jnp.where(which == 1, k_mid, jnp.where(which == 2, k_lo, 0.0))
    ).astype(BF16)
    for s in range(n_seq):
        a_out[s, :, el : el + 128] = k_rows

    for b in range(n_blocks):
        r0 = b * BLOCK
        seg = idc[8 + r0 : 8 + r0 + BLOCK, :]
        same = seg[:, 0:1] == seg.T[0:1, :]
        gram = lax.dot_general(
            bcm[r0 : r0 + BLOCK, 128:256],
            bcm[r0 : r0 + BLOCK, 0:128],
            (((1,), (1,)), ((), ())),
            preferred_element_type=F32,
        )
        grams[b] = jnp.where(same & (ti >= si), gram, 0.0)

    state_copies = []
    for k in far_first:
        peer = lax.rem(seq + k, n_seq)
        state_copies.append(push(a_out.at[peer], a_in.at[seq], {"seq": peer}))
    a_in[seq] = a_out[seq]
    for tile in gate_tiles[-2:]:
        project_gate(*tile)
    for b in range(n_blocks):
        r0 = b * BLOCK
        xp[r0 : r0 + BLOCK, :] = (
            xc[r0 : r0 + BLOCK, :] * lanes_of(dtp[r0 : r0 + BLOCK, :], spread)
        ).astype(BF16)

    def inside(b):
        r0 = b * BLOCK
        ld = ldb[b]
        ld_t = ld.T
        gram = grams[b]
        for pair in range(nh // 2):
            cs = slice(pair * 128, pair * 128 + 128)
            x_pair = xp[r0 : r0 + BLOCK, cs]
            outs = []
            for j in range(2):
                hh = pair * 2 + j
                a = ld[:, hh : hh + 1]
                bb = ld_t[hh : hh + 1, :]
                w0 = jnp.exp(jnp.minimum(a[0:128] - bb[:, 0:128], 0.0)) * gram[0:128, 0:128]
                w1 = jnp.exp(jnp.minimum(a[128:] - bb, 0.0)) * gram[128:, :]
                outs.append(
                    (
                        jnp.dot(w0.astype(BF16), x_pair[0:128], preferred_element_type=F32),
                        jnp.dot(w1.astype(BF16), x_pair, preferred_element_type=F32),
                    )
                )
            first = lax.broadcasted_iota(jnp.int32, (128, 128), 1) < 64
            acc[r0 : r0 + 128, cs] = jnp.where(first, outs[0][0], outs[1][0])
            acc[r0 + 128 : r0 + 256, cs] = jnp.where(first, outs[0][1], outs[1][1])

    inside(0)

    for copy in state_copies:
        copy.wait_recv()

    decay = jnp.dot(
        a_in[:, :, el : el + 128].reshape(n_seq * ng, 128), spread, preferred_element_type=F32
    )
    run = jnp.zeros((ng, el), F32)
    for s in range(n_seq):
        i_out[s] = run.astype(BF16)
        k0 = s * ng
        keep = decay[k0 : k0 + 1, :] + decay[k0 + 1 : k0 + 2, :] + decay[k0 + 2 : k0 + 3, :]
        run = keep * run + a_in[s, :, 0:el].astype(F32)
    back_copies = []
    for k in far_first:
        peer = lax.rem(seq + k, n_seq)
        back_copies.append(push(i_out.at[peer], i_in.at[seq], {"seq": peer}))
    i_in[seq] = i_out[seq]
    for b in range(1, n_blocks):
        inside(b)
    load_out.wait()

    skip = lanes_of(jnp.broadcast_to(prm[2:3, :], (8, 128)), spread)[0:1, :]
    for b in range(n_blocks):
        r0 = b * BLOCK
        rs = slice(r0, r0 + BLOCK)
        seg = idc[8 + r0 : 8 + r0 + BLOCK, :]
        prev = idc[7 + r0 : 8 + r0, :]
        acc[rs, :] = acc[rs, :] + skip * xc[rs, :]
        gate[rs, :] = jax.nn.silu(gate[rs, :])
        xc[rs, :] = lanes_of(jnp.exp(ldb[b]) * jnp.where(seg == prev, 1.0, 0.0), spread)

    for copy in back_copies:
        copy.wait_recv()

    state = i_in[...].astype(F32).reshape(128, el)
    for b in range(n_blocks):
        r0 = b * BLOCK
        inter = jnp.dot(
            bcm[r0 : r0 + BLOCK, 128:256], state.astype(BF16), preferred_element_type=F32
        )
        out = acc[r0 : r0 + BLOCK, :] + xc[r0 : r0 + BLOCK, :] * inter
        gated = out * gate[r0 : r0 + BLOCK, :]
        sq = jnp.sum(gated * gated, axis=1, keepdims=True)
        xp[r0 : r0 + BLOCK, :] = (gated * gated_gain[...]).astype(BF16)
        for q in range(2):
            col = jnp.broadcast_to(sq[q * 128 : q * 128 + 128], (128, 128))
            sq_out[b * 2 + q] = col.T[0:8, :]
        state = keep_lanes[b] * state + st[b]

    def mine(xx):
        return pl.ds(pl.multiple_of(xx * rows, rows), rows)

    zero, one = pl.ds(0, rows), pl.ds(rows, rows)
    r2u, r2d, r3u, r3d, r4u, r4d, x6 = {}, {}, {}, {}, {}, {}, {}
    lx = {}
    l2u, l2d, l3u, l3d = {}, {}, {}, {}

    def out_cols(i, between):
        for q in range(2):
            term = jnp.dot(
                xp[q * m_half : (q + 1) * m_half, :],
                w_out[:, cols[i]],
                preferred_element_type=F32,
            ).astype(BF16)
            part[q * (n_y // 2) : (q + 1) * (n_y // 2), :, cols[i]] = term.reshape(
                n_y // 2, 2 * rows, pieces[i][1]
            )
            if q == 0:
                between()

    def cross(i, yy):
        lx[i, len([k for k in lx if k[0] == i])] = push(
            part.at[yy, mine(other), cols[i]], xl_in.at[yy, :, cols[i]], at_x
        )

    def send_r3(i):
        r3u[i] = push(part.at[up, one, cols[i]], yr1.at[0, 1, :, cols[i]], at_up)
        r3d[i] = push(part.at[down, zero, cols[i]], yr1.at[1, 0, :, cols[i]], at_down)

    def first_sends(i):
        if i in rights:
            r2u[i] = push(part.at[far, zero, cols[i]], yr2.at[0, :, cols[i]], at_up)
            r2d[i] = push(part.at[far, one, cols[i]], yr2.at[1, :, cols[i]], at_down)
            if i == rights[0]:
                send_r3(i)
        else:
            cross(i, far)
            if i == lefts[0]:
                cross(i, up)
            if i == lefts[-1]:
                for yy in (up, down, y):
                    for j in lefts:
                        if not (yy is up and j == lefts[0]):
                            cross(j, yy)

    sq_copies = []

    def send_sq():
        for k in range(1, n_tp):
            peer = lax.rem(tp + k, n_tp)
            sq_copies.append(push(sq_out.at[peer // 2], sq_in.at[tp], {"tp": peer}))

    for i in every:
        out_cols(i, (lambda: first_sends(i - 1)) if i else send_sq)
    sq_in[tp] = sq_out[y]
    first_sends(len(pieces) - 1)
    for i in rights[1:2]:
        send_r3(i)

    def sum_of(*refs):
        tot = refs[0].astype(F32)
        for r in refs[1:]:
            tot = tot + r.astype(F32)
        return tot

    for i in every:
        c = cols[i]
        if i in rights:
            r2u[i].wait_recv()
            qr[0, :, c] = sum_of(part[up, zero, c], yr2[0, :, c]).astype(BF16)
            r2d[i].wait_recv()
            qr[1, :, c] = sum_of(part[down, one, c], yr2[1, :, c]).astype(BF16)
            if i in rights[2:]:
                send_r3(i)
            r4u[i] = push(qr.at[0, :, c], yr1.at[0, 0, :, c], at_up)
            r4d[i] = push(qr.at[1, :, c], yr1.at[1, 1, :, c], at_down)
        else:
            lx[i, 0].wait_recv()
            ql[far, :, c] = sum_of(part[far, mine(xl), c], xl_in[far, :, c]).astype(BF16)
            l2u[i] = push(ql.at[far, pl.ds(0, half), c], yl2.at[0, :, c], at_up)
            l2d[i] = push(ql.at[far, pl.ds(half, half), c], yl2.at[1, :, c], at_down)

    def right_sum(xx, c):
        return sum_of(part[y, mine(xx), c], yr1[0, xx, :, c], yr1[1, xx, :, c])

    for i in every:
        c = cols[i]
        if i in rights:
            for copy in (r3u[i], r3d[i], r4u[i], r4d[i]):
                copy.wait_recv()
            qx[:, c] = right_sum(other, c).astype(BF16)
            x6[i] = push(qx.at[:, c], xr_in.at[:, c], at_x)
        else:
            lx[i, 1].wait_recv()
            q_up = sum_of(part[up, mine(xl), c], xl_in[up, :, c])
            lx[i, 2].wait_recv()
            q_down = sum_of(part[down, mine(xl), c], xl_in[down, :, c])
            l2u[i].wait_recv()
            ql[up, pl.ds(0, half), c] = (q_up[0:half] + yl2[0, :, c].astype(F32)).astype(BF16)
            ql[up, pl.ds(half, half), c] = q_up[half:].astype(BF16)
            l2d[i].wait_recv()
            ql[down, pl.ds(0, half), c] = q_down[0:half].astype(BF16)
            ql[down, pl.ds(half, half), c] = (q_down[half:] + yl2[1, :, c].astype(F32)).astype(
                BF16
            )
            l3u[i] = push(ql.at[up, :, c], yl1.at[0, :, c], at_up)
            l3d[i] = push(ql.at[down, :, c], yl1.at[1, :, c], at_down)

    for copy in sq_copies:
        copy.wait_recv()
    tot = sq_in[0]
    for k in range(1, n_tp):
        tot = tot + sq_in[k]
    sqc[...] = jnp.broadcast_to(tot[0:1, :], (128, 128)).T
    factor = lax.rsqrt(sqc[mine(xl), :][:, 0:1] / (el * n_tp) + EPS)

    def finish(i, total):
        c = cols[i]
        result[:, c] = (rows_in[tp, :, c].astype(F32) + factor * total).astype(BF16)

    def hand(i):
        @pl.when(pipe == 0)
        def _():
            handoff[i].start()

    for i in every:
        c = cols[i]
        if i in rights:
            own = right_sum(xl, c)
            x6[i].wait_recv()
            finish(i, own + xr_in[:, c].astype(F32))
        else:
            own = sum_of(part[y, mine(xl), c])
            for copy in (lx[i, 3], l3u[i], l3d[i]):
                copy.wait_recv()
            finish(i, own + sum_of(xl_in[y, :, c], yl1[0, :, c], yl1[1, :, c]))
        if i:
            hand(i - 1)

    for copy in sent[:8]:
        copy.wait_send()
    hand(len(pieces) - 1)
    for copy in sent[8:]:
        copy.wait_send()

    @pl.when(pipe == 0)
    def _():
        for copy in handoff:
            copy.wait_send()


def local(geo, *args):
    n_seq, n_tp, n_y, d, el, nh, pieces = geo
    (
        hidden_in,
        doc_ids,
        norm_gain,
        in_zx,
        in_bc,
        in_dt,
        conv_x,
        conv_bc,
        bias_x,
        bias_bc,
        dt_bias,
        a_log,
        d_skip,
        gated_gain,
        out_w,
    ) = args
    rows = hidden_in.shape[1]
    toks = rows * n_tp
    ng = 128 // n_seq
    n_blocks = toks // BLOCK
    in_right = sum(1 for p in pieces if p[2])
    out_right = sum(1 for p in pieces if p[3])
    n_msg = 7 + 26 * len(pieces) + 2 * (n_seq - 1) + (n_tp - 1) - 2 * in_right - out_right
    vmem = pl.BlockSpec(memory_space=pltpu.VMEM)
    anyw = pl.BlockSpec(memory_space=pl.ANY)
    scratch = [
        pltpu.VMEM((d, 2, el), BF16),
        pltpu.VMEM((d, el), BF16),
        pltpu.VMEM((d, el + 128), BF16),
        pltpu.VMEM((d, 256), BF16),
        pltpu.VMEM((nh, d), BF16),
        pltpu.VMEM((el, d), BF16),
        pltpu.VMEM((n_tp, rows, d), BF16),
        pltpu.VMEM((n_tp, rows, d), BF16),
        pltpu.VMEM((n_tp, rows, d), BF16),
        pltpu.VMEM((toks + 8, el + 384), F32),
        pltpu.VMEM((toks, el), F32),
        pltpu.VMEM((toks, el), F32),
        pltpu.VMEM((toks, 256), BF16),
        pltpu.VMEM((toks, el), BF16),
        pltpu.VMEM((toks, el), F32),
        pltpu.VMEM((toks + 8, 128), F32),
        pltpu.VMEM((toks, 128), F32),
        pltpu.VMEM((8, 128), F32),
        pltpu.VMEM((n_blocks, BLOCK, 128), F32),
        pltpu.VMEM((n_blocks, 128, el), F32),
        pltpu.VMEM((n_blocks, BLOCK, BLOCK), F32),
        pltpu.VMEM((n_seq, ng, el + 128), BF16),
        pltpu.VMEM((n_seq, ng, el + 128), BF16),
        pltpu.VMEM((n_seq, ng, el), BF16),
        pltpu.VMEM((n_seq, ng, el), BF16),
        pltpu.VMEM((n_y, 2 * rows, d), BF16),
        pltpu.VMEM((n_y, rows, d), BF16),
        pltpu.VMEM((n_y, rows, d), BF16),
        pltpu.VMEM((2, rows // 2, d), BF16),
        pltpu.VMEM((2, rows, d), BF16),
        pltpu.VMEM((2, rows, d), BF16),
        pltpu.VMEM((2, 2, rows, d), BF16),
        pltpu.VMEM((2, rows, d), BF16),
        pltpu.VMEM((rows, d), BF16),
        pltpu.VMEM((rows, d), BF16),
        pltpu.VMEM((n_y, 8, 128), F32),
        pltpu.VMEM((n_tp, 8, 128), F32),
        pltpu.VMEM((128, 128), F32),
        pltpu.SemaphoreType.DMA((n_msg,)),
        pltpu.SemaphoreType.DMA((n_msg,)),
        pltpu.SemaphoreType.DMA((6,)),
    ]
    out = pl.pallas_call(
        functools.partial(layer_kernel, geo),
        out_shape=jax.ShapeDtypeStruct((rows, d), BF16),
        in_specs=[anyw, vmem, vmem, anyw, anyw, anyw] + [vmem] * 8 + [anyw],
        out_specs=vmem,
        scratch_shapes=scratch,
        name="mixer_section",
        compiler_params=pltpu.CompilerParams(
            collective_id=0, has_side_effects=True, vmem_limit_bytes=60 * 1024 * 1024
        ),
    )(
        hidden_in[0],
        doc_ids,
        norm_gain,
        in_zx[0],
        in_bc[0],
        in_dt[0].T,
        conv_x[0],
        conv_bc[0],
        bias_x,
        bias_bc,
        dt_bias,
        a_log,
        d_skip,
        gated_gain,
        out_w[0],
    )
    return out[None, None]


def build(mesh, d, e, h):
    n_seq, n_tp = mesh.shape["seq"], mesh.shape["tp"]
    wide = 512 if d % 512 == 0 else 128
    pieces = tuple(
        (c, wide, (c // wide) % 2 == 0, (c // wide) % 3 != 1) for c in range(0, d, wide)
    )
    geo = (n_seq, n_tp, n_tp // 2, d, e // n_tp, h // n_tp, pieces)
    in_specs = (
        P(None, ("seq", "tp"), None),
        P(None, "seq"),
        P("pipe", None),
        P("pipe", None, None, "tp"),
        P("pipe", None, None),
        P("pipe", None, "tp"),
        P("pipe", None, "tp"),
        P("pipe", None, None),
        P("pipe", "tp"),
        P("pipe", None),
        P("pipe", "tp"),
        P("pipe", "tp"),
        P("pipe", "tp"),
        P("pipe", "tp"),
        P("pipe", "tp", None),
    )
    out_specs = P("pipe", None, ("seq", "tp"), None)
    return jax.shard_map(
        functools.partial(local, geo),
        mesh=mesh,
        in_specs=in_specs,
        out_specs=out_specs,
        check_vma=False,
    )


def solution(mesh):
    return build(mesh, 2560, 5120, 80)
```

```python
import functools

import jax
import jax.numpy as jnp
from jax import lax
from jax.experimental import pallas as pl
from jax.experimental.pallas import tpu as pltpu
from jax.sharding import PartitionSpec as P

BLOCK = 256
EPS = 1e-05
F32 = jnp.float32
BF16 = jnp.bfloat16
MESH = pl.DeviceIdType.MESH


def lanes_of(v, spread):
    hi = v.astype(BF16)
    lo = (v - hi.astype(F32)).astype(BF16)
    return jnp.dot(hi, spread, preferred_element_type=F32) + jnp.dot(
        lo, spread, preferred_element_type=F32
    )


def layer_kernel(
    geo,
    hidden_hbm,
    ids_ref,
    norm_gain,
    zx_hbm,
    bc_hbm,
    dt_hbm,
    conv_x,
    conv_bc,
    bias_x,
    bias_bc,
    dt_bias,
    a_log,
    d_skip,
    gated_gain,
    out_hbm,
    result,
    w_raw,
    w_gate,
    w_x,
    w_bc,
    w_dt,
    w_out,
    rows_pre,
    rows_in,
    rows_all,
    pre,
    gate,
    xc,
    bcm,
    xp,
    acc,
    idc,
    dtp,
    prm,
    ldb,
    st,
    grams,
    a_out,
    a_in,
    i_out,
    i_in,
    part,
    xl_in,
    ql,
    yl2,
    yl1,
    yr2,
    yr1,
    qr,
    qx,
    xr_in,
    sq_out,
    sq_in,
    sqc,
    send_sem,
    recv_sem,
    load_sem,
):
    n_seq, n_tp, n_y, d, el, nh, pieces = geo
    pipe, seq, tp = lax.axis_index("pipe"), lax.axis_index("seq"), lax.axis_index("tp")
    y, xl = tp // 2, tp % 2
    other = 1 - xl
    rows = rows_in.shape[1]
    toks = n_tp * rows
    half = rows // 2
    n_blocks = toks // BLOCK
    ng = 128 // n_seq
    up, down = lax.rem(y + 1, n_y), lax.rem(y + n_y - 1, n_y)
    far = lax.rem(y + 2, n_y)
    at_up = {"tp": up * 2 + xl}
    at_down = {"tp": down * 2 + xl}
    at_x = {"tp": y * 2 + other}
    nxt = {"seq": lax.rem(seq + 1, n_seq)}
    every = range(len(pieces))
    rights = [i for i in every if pieces[i][3]]
    lefts = [i for i in every if not pieces[i][3]]
    cols = [pl.ds(c0, w) for c0, w, _, _ in pieces]
    counter = [0]
    sent = []

    def remote(src, dst, where):
        k = counter[0]
        counter[0] += 1
        return pltpu.make_async_remote_copy(
            src_ref=src,
            dst_ref=dst,
            send_sem=send_sem.at[k],
            recv_sem=recv_sem.at[k],
            device_id=where,
            device_id_type=MESH,
        )

    def push(src, dst, where):
        copy = remote(src, dst, where)
        copy.start()
        sent.append(copy)
        return copy

    top, bottom = pl.ds(0, d // 2), pl.ds(d // 2, d // 2)
    load_dt, load_top, load_bottom, load_bc, load_out = loads = [
        pltpu.make_async_copy(s, t, load_sem.at[k])
        for k, (s, t) in enumerate(
            [
                (dt_hbm, w_dt),
                (zx_hbm.at[top], w_raw.at[top]),
                (zx_hbm.at[bottom], w_raw.at[bottom]),
                (bc_hbm, w_bc),
                (out_hbm, w_out),
            ]
        )
    ]
    first_load = pltpu.make_async_copy(hidden_hbm, rows_pre.at[tp], load_sem.at[5])

    @pl.when(pipe == 1)
    def _():
        first_load.start()

    for copy in loads:
        copy.start()

    far_first = sorted(range(1, n_seq), key=lambda k: (k % 2 == 0, abs(2 * k - n_seq)))
    barrier = pltpu.get_barrier_semaphore()
    for k in far_first:
        pl.semaphore_signal(
            barrier, inc=1, device_id={"seq": lax.rem(seq + k, n_seq)}, device_id_type=MESH
        )
    for k in range(1, n_tp):
        pl.semaphore_signal(
            barrier, inc=1, device_id={"tp": lax.rem(tp + k, n_tp)}, device_id_type=MESH
        )
    pl.semaphore_signal(barrier, inc=1, device_id={"pipe": 1 - pipe}, device_id_type=MESH)

    prm[...] = jnp.zeros_like(prm)
    prm[0:1, 0:nh] = dt_bias[...]
    prm[1:2, 0:nh] = -jnp.exp(a_log[...])
    prm[2:3, 0:nh] = d_skip[...]
    ids_row = ids_ref[...].astype(F32)
    idc[8 : 8 + toks, :] = jnp.broadcast_to(ids_row, (128, toks)).T
    head = lax.broadcasted_iota(jnp.int32, (128, el), 0)
    lane = lax.broadcasted_iota(jnp.int32, (128, el), 1)
    spread = jnp.where((lane // 64) == head, 1.0, 0.0).astype(BF16)
    ti = lax.broadcasted_iota(jnp.int32, (BLOCK, BLOCK), 0)
    si = lax.broadcasted_iota(jnp.int32, (BLOCK, BLOCK), 1)

    def lay_out(lo, hi):
        def step(i, carry):
            r = pl.multiple_of(i * 64, 64)
            both = jnp.swapaxes(w_raw[pl.ds(r, 64)].astype(F32), 0, 1)
            w_gate[pl.ds(r, 64), :] = both[0].astype(BF16)
            w_x[pl.ds(r, 64), 0:el] = both[1].astype(BF16)
            return carry

        lax.fori_loop(lo, hi, step, 0)

    def lay_out_dt():
        unit = jnp.where(
            lax.broadcasted_iota(jnp.int32, (nh, 128), 0)
            == lax.broadcasted_iota(jnp.int32, (nh, 128), 1),
            1.0,
            0.0,
        ).astype(BF16)
        for r in range(0, d, 256):
            w_x[r : r + 256, el : el + 128] = lax.dot_general(
                w_dt[:, r : r + 256],
                unit,
                (((0,), (0,)), ((), ())),
                preferred_element_type=F32,
            ).astype(BF16)

    n_lay = d // 64

    @pl.when(pipe == 0)
    def _():
        load_dt.wait()
        lay_out_dt()
        load_top.wait()
        lay_out(0, n_lay // 2)
        load_bottom.wait()
        lay_out(n_lay // 2, n_lay)
        load_bc.wait()

    pl.semaphore_wait(barrier, n_tp + n_seq - 1)
    id_edge = push(idc.at[pl.ds(toks, 8)], idc.at[pl.ds(0, 8)], nxt)
    mate = {"pipe": 1 - pipe}
    handoff = [remote(result.at[:, c], rows_in.at[tp, :, c], mate) for c in cols]

    own_rows = (y * 2, y * 2 + 1)
    near_rows = (down * 2 + xl, up * 2 + xl)
    beside_rows = (down * 2 + other, up * 2 + other)
    far_rows = (far * 2, far * 2 + 1)

    def norm_rows(slots):
        for t in slots:
            h = rows_in[t].astype(F32)
            scale = lax.rsqrt(jnp.mean(h * h, axis=1, keepdims=True) + EPS)
            rows_all[t] = (h * scale * norm_gain[...]).astype(BF16)

    tiles = [(w_x, c0, c0) for c0 in range(0, el + 128, 256)] + [(w_bc, 0, el + 128)]
    tile_groups = [tiles[k : k + 2] for k in range(0, len(tiles), 2)]

    def project(slots, group):
        lhs = jnp.concatenate([rows_all[t] for t in slots], axis=0)
        for weight, w0, t0 in group:
            term = jnp.dot(lhs, weight[:, w0 : w0 + 256], preferred_element_type=F32)
            for k, t in enumerate(slots):
                at = pl.ds(pl.multiple_of(8 + t * rows, 8), rows)
                pre[at, t0 : t0 + 256] = term[k * rows : (k + 1) * rows]

    def take(slots):
        norm_rows(slots)
        for group in tile_groups:
            project(slots, group)

    def gather(buf, eager, ready, early, between, late, last):
        mine_sent = []

        def hop(yy, xx, i, where, r0=0, n=rows):
            s = buf.at[yy * 2 + xx, pl.ds(r0, n), cols[i]]
            copy = remote(s, s, where)
            copy.start()
            mine_sent.append(copy)
            return copy

        u1, d1, x1, u2, d2, x2, x3 = {}, {}, {}, {}, {}, {}, {}

        def first(i):
            ready(i)
            u1[i], d1[i] = hop(y, xl, i, at_up), hop(y, xl, i, at_down)
            x1[i] = hop(y, xl, i, at_x)

        def second(i):
            if pieces[i][2]:
                x1[i].wait_recv()
                u2[i], d2[i] = hop(y, other, i, at_up), hop(y, other, i, at_down)
            else:
                u1[i].wait_recv()
                u2[i] = hop(down, xl, i, at_up, 0, half)
                x2[i] = hop(down, xl, i, at_x)
                d1[i].wait_recv()
                d2[i] = hop(up, xl, i, at_down, half, half)
                x3[i] = hop(up, xl, i, at_x)

        for i in every:
            first(i)
            if i == 2 and eager:
                second(0)
        for i in every:
            if 0 not in u2 or i:
                second(i)
        for i in every:
            if pieces[i][2]:
                u1[i].wait_recv()
                d1[i].wait_recv()
            else:
                x1[i].wait_recv()
        early()
        u3, d3, x4 = {}, {}, {}
        for i in every:
            if pieces[i][2]:
                u2[i].wait_recv()
                u3[i] = hop(down, 0, i, at_up)
                d2[i].wait_recv()
                d3[i] = hop(up, 1, i, at_down)
            else:
                u2[i].wait_recv()
                d2[i].wait_recv()
                x4[i] = hop(far, xl, i, at_x)
            between(i)
        for i in x2:
            x2[i].wait_recv()
            x3[i].wait_recv()
        late()
        for i in every:
            for copy in (u3[i], d3[i]) if pieces[i][2] else (x4[i],):
                copy.wait_recv()
            last(i)
        return mine_sent

    def pair_of(yy):
        return pl.ds(yy * 2, 2)

    def across(at):
        return remote(rows_pre.at[at], rows_in.at[at], mate)

    own_pair = across(pair_of(y))
    near = [across(yy * 2 + xl) for yy in (down, up)]
    beside = [across(yy * 2 + other) for yy in (down, up)]
    rest = [
        remote(rows_pre.at[pair_of(far), :, c], rows_in.at[pair_of(far), :, c], mate)
        for c in cols
    ]

    @pl.when(pipe == 1)
    def _():
        first_load.wait()

        def early():
            for copy in [own_pair] + near:
                copy.start()

        def late():
            for copy in beside:
                copy.start()

        first = gather(
            rows_pre,
            False,
            lambda i: None,
            early,
            lambda i: None,
            late,
            lambda i: rest[i].start(),
        )
        load_dt.wait()
        lay_out_dt()
        load_top.wait()
        load_bottom.wait()
        lay_out(0, n_lay)
        load_bc.wait()
        for copy in first + [own_pair] + near + beside + rest:
            copy.wait_send()

    @pl.when(pipe == 1)
    def _():
        chunks = {
            0: (lambda: norm_rows(own_rows), lambda: project(own_rows, tile_groups[0])),
            min(2, len(pieces) - 1): (
                lambda: [project(own_rows, g) for g in tile_groups[1:]],
                lambda: norm_rows(near_rows),
            ),
        }

        def between(i):
            for chunk in chunks.get(i, ()):
                chunk()
            if i == len(pieces) - 1:
                for group in tile_groups:
                    project(near_rows, group)

        second = gather(
            rows_in,
            True,
            lambda i: handoff[i].wait_recv(),
            lambda: None,
            between,
            lambda: take(beside_rows),
            lambda i: None,
        )
        take(far_rows)
        for copy in second:
            copy.wait_send()

    @pl.when(pipe == 0)
    def _():
        for copies, slots in (
            ([own_pair], own_rows),
            (near, near_rows),
            (beside, beside_rows),
            (rest, far_rows),
        ):
            for copy in copies:
                copy.wait_recv()
            take(slots)

    id_edge.wait_recv()
    idc[0:8, :] = jnp.where(seq > 0, idc[0:8, :], -1.0)
    n_half = n_tp // 2
    m_half = n_half * rows

    step_all = jax.nn.softplus(pre[8 : 8 + toks, el : el + 128] + prm[0:1, :])
    dtp[...] = step_all
    edge = push(pre.at[pl.ds(toks, 8)], pre.at[pl.ds(0, 8)], nxt)
    rate = step_all * prm[1:2, :]
    tri = jnp.where(ti >= si, 1.0, 0.0).astype(BF16)
    r_hi = rate.astype(BF16)
    r_rest = rate - r_hi.astype(F32)
    r_mid = r_rest.astype(BF16)
    r_lo = (r_rest - r_mid.astype(F32)).astype(BF16)
    for b in range(n_blocks):
        ldb[b] = sum(
            jnp.dot(tri, r[b * BLOCK : (b + 1) * BLOCK], preferred_element_type=F32)
            for r in (r_lo, r_mid, r_hi)
        )

    def convolve(r):
        r0 = r * 64
        own = idc[8 + r0 : 72 + r0, :][:, 0:1]
        run_x = jnp.broadcast_to(bias_x[...], (64, el))
        run_bc = jnp.broadcast_to(bias_bc[...], (64, 256))
        for k in range(4):
            at = r0 + 5 + k
            tap_x, tap_bc = conv_x[k : k + 1, :], conv_bc[k : k + 1, :]
            if k < 3:
                keep = jnp.where(idc[at : at + 64, :][:, 0:1] == own, 1.0, 0.0)
                tap_x, tap_bc = keep * tap_x, keep * tap_bc
            run_x = run_x + tap_x * pre[at : at + 64, 0:el]
            run_bc = run_bc + tap_bc * pre[at : at + 64, el + 128 :]
        xc[r0 : r0 + 64, :] = jax.nn.silu(run_x)
        bcm[r0 : r0 + 64, :] = jax.nn.silu(run_bc).astype(BF16)

    for r in range(1, toks // 64):
        convolve(r)

    def project_gate(c0, w):
        for j in range(2):
            lhs = rows_all[n_half * j : n_half * (j + 1)].reshape(m_half, d)
            gate[pl.ds(j * m_half, m_half), pl.ds(c0, w)] = jnp.dot(
                lhs, w_gate[:, pl.ds(c0, w)], preferred_element_type=F32
            )

    gate_tiles = [(c0, min(256, el - c0)) for c0 in range(0, el, 256)]
    for tile in gate_tiles[:-2]:
        project_gate(*tile)

    keeps = [None] * n_blocks

    def states(b):
        r0 = b * BLOCK
        ld = ldb[b]
        ld_end = ld[BLOCK - 1 : BLOCK, :]
        seg = idc[8 + r0 : 8 + r0 + BLOCK, :]
        seg_end = seg[BLOCK - 1 : BLOCK, :]
        prev = idc[7 + r0 : 8 + r0, :]
        step_b = dtp[r0 : r0 + BLOCK, :]
        to_end = jnp.exp(ld_end - ld) * jnp.where(seg == seg_end, 1.0, 0.0) * step_b
        x_b = xc[r0 : r0 + BLOCK, :]
        x_w = (x_b * lanes_of(to_end, spread)).astype(BF16)
        st[b] = lax.dot_general(
            bcm[r0 : r0 + BLOCK, 0:128],
            x_w,
            (((0,), (0,)), ((), ())),
            preferred_element_type=F32,
        )
        keep = jnp.exp(ld_end) * jnp.where(seg_end == prev, 1.0, 0.0)
        keeps[b] = jnp.broadcast_to(keep, (8, 128))

    for b in range(1, n_blocks):
        states(b)
    edge.wait_recv()
    convolve(0)
    states(0)
    keep_lanes = [lanes_of(k, spread)[0:1, :] for k in keeps]
    total = st[0]
    keep_shard = keeps[0]
    for b in range(1, n_blocks):
        total = keep_lanes[b] * total + st[b]
        keep_shard = keep_shard * keeps[b]
    a_out[:, :, 0:el] = total.reshape(n_seq, ng, el).astype(BF16)
    keep_row = jnp.broadcast_to(keep_shard[0:1, :], (ng, 128))
    k_hi = keep_row.astype(BF16).astype(F32)
    k_mid = (keep_row - k_hi).astype(BF16).astype(F32)
    k_lo = keep_row - k_hi - k_mid
    which = lax.broadcasted_iota(jnp.int32, (ng, 128), 0)
    k_rows = jnp.where(
        which == 0, k_hi, jnp.where(which == 1, k_mid, jnp.where(which == 2, k_lo, 0.0))
    ).astype(BF16)
    for s in range(n_seq):
        a_out[s, :, el : el + 128] = k_rows

    for b in range(n_blocks):
        r0 = b * BLOCK
        seg = idc[8 + r0 : 8 + r0 + BLOCK, :]
        same = seg[:, 0:1] == seg.T[0:1, :]
        gram = lax.dot_general(
            bcm[r0 : r0 + BLOCK, 128:256],
            bcm[r0 : r0 + BLOCK, 0:128],
            (((1,), (1,)), ((), ())),
            preferred_element_type=F32,
        )
        grams[b] = jnp.where(same & (ti >= si), gram, 0.0)

    state_copies = []
    for k in far_first:
        peer = lax.rem(seq + k, n_seq)
        state_copies.append(push(a_out.at[peer], a_in.at[seq], {"seq": peer}))
    a_in[seq] = a_out[seq]
    for tile in gate_tiles[-2:]:
        project_gate(*tile)
    for b in range(n_blocks):
        r0 = b * BLOCK
        xp[r0 : r0 + BLOCK, :] = (
            xc[r0 : r0 + BLOCK, :] * lanes_of(dtp[r0 : r0 + BLOCK, :], spread)
        ).astype(BF16)

    def inside(b):
        r0 = b * BLOCK
        ld = ldb[b]
        ld_t = ld.T
        gram = grams[b]
        for pair in range(nh // 2):
            cs = slice(pair * 128, pair * 128 + 128)
            x_pair = xp[r0 : r0 + BLOCK, cs]
            outs = []
            for j in range(2):
                hh = pair * 2 + j
                a = ld[:, hh : hh + 1]
                bb = ld_t[hh : hh + 1, :]
                w0 = jnp.exp(jnp.minimum(a[0:128] - bb[:, 0:128], 0.0)) * gram[0:128, 0:128]
                w1 = jnp.exp(jnp.minimum(a[128:] - bb, 0.0)) * gram[128:, :]
                outs.append(
                    (
                        jnp.dot(w0.astype(BF16), x_pair[0:128], preferred_element_type=F32),
                        jnp.dot(w1.astype(BF16), x_pair, preferred_element_type=F32),
                    )
                )
            first = lax.broadcasted_iota(jnp.int32, (128, 128), 1) < 64
            acc[r0 : r0 + 128, cs] = jnp.where(first, outs[0][0], outs[1][0])
            acc[r0 + 128 : r0 + 256, cs] = jnp.where(first, outs[0][1], outs[1][1])

    inside(0)

    for copy in state_copies:
        copy.wait_recv()

    decay = jnp.dot(
        a_in[:, :, el : el + 128].reshape(n_seq * ng, 128), spread, preferred_element_type=F32
    )
    run = jnp.zeros((ng, el), F32)
    for s in range(n_seq):
        i_out[s] = run.astype(BF16)
        k0 = s * ng
        keep = decay[k0 : k0 + 1, :] + decay[k0 + 1 : k0 + 2, :] + decay[k0 + 2 : k0 + 3, :]
        run = keep * run + a_in[s, :, 0:el].astype(F32)
    back_copies = []
    for k in far_first:
        peer = lax.rem(seq + k, n_seq)
        back_copies.append(push(i_out.at[peer], i_in.at[seq], {"seq": peer}))
    i_in[seq] = i_out[seq]
    for b in range(1, n_blocks):
        inside(b)
    load_out.wait()

    skip = lanes_of(jnp.broadcast_to(prm[2:3, :], (8, 128)), spread)[0:1, :]
    for b in range(n_blocks):
        r0 = b * BLOCK
        rs = slice(r0, r0 + BLOCK)
        seg = idc[8 + r0 : 8 + r0 + BLOCK, :]
        prev = idc[7 + r0 : 8 + r0, :]
        acc[rs, :] = acc[rs, :] + skip * xc[rs, :]
        gate[rs, :] = jax.nn.silu(gate[rs, :])
        xc[rs, :] = lanes_of(jnp.exp(ldb[b]) * jnp.where(seg == prev, 1.0, 0.0), spread)

    for copy in back_copies:
        copy.wait_recv()

    state = i_in[...].astype(F32).reshape(128, el)
    for b in range(n_blocks):
        r0 = b * BLOCK
        inter = jnp.dot(
            bcm[r0 : r0 + BLOCK, 128:256], state.astype(BF16), preferred_element_type=F32
        )
        out = acc[r0 : r0 + BLOCK, :] + xc[r0 : r0 + BLOCK, :] * inter
        gated = out * gate[r0 : r0 + BLOCK, :]
        sq = jnp.sum(gated * gated, axis=1, keepdims=True)
        xp[r0 : r0 + BLOCK, :] = (gated * gated_gain[...]).astype(BF16)
        for q in range(2):
            col = jnp.broadcast_to(sq[q * 128 : q * 128 + 128], (128, 128))
            sq_out[b * 2 + q] = col.T[0:8, :]
        state = keep_lanes[b] * state + st[b]

    def mine(xx):
        return pl.ds(pl.multiple_of(xx * rows, rows), rows)

    zero, one = pl.ds(0, rows), pl.ds(rows, rows)
    r2u, r2d, r3u, r3d, r4u, r4d, x6 = {}, {}, {}, {}, {}, {}, {}
    lx = {}
    l2u, l2d, l3u, l3d = {}, {}, {}, {}

    def out_cols(i, between):
        for q in range(2):
            term = jnp.dot(
                xp[q * m_half : (q + 1) * m_half, :],
                w_out[:, cols[i]],
                preferred_element_type=F32,
            ).astype(BF16)
            part[q * (n_y // 2) : (q + 1) * (n_y // 2), :, cols[i]] = term.reshape(
                n_y // 2, 2 * rows, pieces[i][1]
            )
            if q == 0:
                between()

    def cross(i, yy):
        lx[i, len([k for k in lx if k[0] == i])] = push(
            part.at[yy, mine(other), cols[i]], xl_in.at[yy, :, cols[i]], at_x
        )

    def send_r3(i):
        r3u[i] = push(part.at[up, one, cols[i]], yr1.at[0, 1, :, cols[i]], at_up)
        r3d[i] = push(part.at[down, zero, cols[i]], yr1.at[1, 0, :, cols[i]], at_down)

    def first_sends(i):
        if i in rights:
            r2u[i] = push(part.at[far, zero, cols[i]], yr2.at[0, :, cols[i]], at_up)
            r2d[i] = push(part.at[far, one, cols[i]], yr2.at[1, :, cols[i]], at_down)
            if i == rights[0]:
                send_r3(i)
        else:
            cross(i, far)
            if i == lefts[0]:
                cross(i, up)
            if i == lefts[-1]:
                for yy in (up, down, y):
                    for j in lefts:
                        if not (yy is up and j == lefts[0]):
                            cross(j, yy)

    sq_copies = []

    def send_sq():
        for k in range(1, n_tp):
            peer = lax.rem(tp + k, n_tp)
            sq_copies.append(push(sq_out.at[peer // 2], sq_in.at[tp], {"tp": peer}))

    for i in every:
        out_cols(i, (lambda: first_sends(i - 1)) if i else send_sq)
    sq_in[tp] = sq_out[y]
    first_sends(len(pieces) - 1)
    for i in rights[1:2]:
        send_r3(i)

    def sum_of(*refs):
        tot = refs[0].astype(F32)
        for r in refs[1:]:
            tot = tot + r.astype(F32)
        return tot

    for i in every:
        c = cols[i]
        if i in rights:
            r2u[i].wait_recv()
            qr[0, :, c] = sum_of(part[up, zero, c], yr2[0, :, c]).astype(BF16)
            r2d[i].wait_recv()
            qr[1, :, c] = sum_of(part[down, one, c], yr2[1, :, c]).astype(BF16)
            if i in rights[2:]:
                send_r3(i)
            r4u[i] = push(qr.at[0, :, c], yr1.at[0, 0, :, c], at_up)
            r4d[i] = push(qr.at[1, :, c], yr1.at[1, 1, :, c], at_down)
        else:
            lx[i, 0].wait_recv()
            ql[far, :, c] = sum_of(part[far, mine(xl), c], xl_in[far, :, c]).astype(BF16)
            l2u[i] = push(ql.at[far, pl.ds(0, half), c], yl2.at[0, :, c], at_up)
            l2d[i] = push(ql.at[far, pl.ds(half, half), c], yl2.at[1, :, c], at_down)

    def right_sum(xx, c):
        return sum_of(part[y, mine(xx), c], yr1[0, xx, :, c], yr1[1, xx, :, c])

    for i in every:
        c = cols[i]
        if i in rights:
            for copy in (r3u[i], r3d[i], r4u[i], r4d[i]):
                copy.wait_recv()
            qx[:, c] = right_sum(other, c).astype(BF16)
            x6[i] = push(qx.at[:, c], xr_in.at[:, c], at_x)
        else:
            lx[i, 1].wait_recv()
            q_up = sum_of(part[up, mine(xl), c], xl_in[up, :, c])
            lx[i, 2].wait_recv()
            q_down = sum_of(part[down, mine(xl), c], xl_in[down, :, c])
            l2u[i].wait_recv()
            ql[up, pl.ds(0, half), c] = (q_up[0:half] + yl2[0, :, c].astype(F32)).astype(BF16)
            ql[up, pl.ds(half, half), c] = q_up[half:].astype(BF16)
            l2d[i].wait_recv()
            ql[down, pl.ds(0, half), c] = q_down[0:half].astype(BF16)
            ql[down, pl.ds(half, half), c] = (q_down[half:] + yl2[1, :, c].astype(F32)).astype(
                BF16
            )
            l3u[i] = push(ql.at[up, :, c], yl1.at[0, :, c], at_up)
            l3d[i] = push(ql.at[down, :, c], yl1.at[1, :, c], at_down)

    for copy in sq_copies:
        copy.wait_recv()
    tot = sq_in[0]
    for k in range(1, n_tp):
        tot = tot + sq_in[k]
    sqc[...] = jnp.broadcast_to(tot[0:1, :], (128, 128)).T
    factor = lax.rsqrt(sqc[mine(xl), :][:, 0:1] / (el * n_tp) + EPS)

    def finish(i, total):
        c = cols[i]
        result[:, c] = (rows_in[tp, :, c].astype(F32) + factor * total).astype(BF16)

    def hand(i):
        if i < 0:
            return

        @pl.when(pipe == 0)
        def _():
            handoff[i].start()

    for i in every:
        c = cols[i]
        if i in rights:
            own = right_sum(xl, c)
            hand(i - 1)
            x6[i].wait_recv()
            finish(i, own + xr_in[:, c].astype(F32))
        else:
            own = sum_of(part[y, mine(xl), c])
            hand(i - 1)
            for copy in (lx[i, 3], l3u[i], l3d[i]):
                copy.wait_recv()
            finish(i, own + sum_of(xl_in[y, :, c], yl1[0, :, c], yl1[1, :, c]))

    for copy in sent[:8]:
        copy.wait_send()
    hand(len(pieces) - 1)
    for copy in sent[8:]:
        copy.wait_send()

    @pl.when(pipe == 0)
    def _():
        for copy in handoff:
            copy.wait_send()


def local(geo, *args):
    n_seq, n_tp, n_y, d, el, nh, pieces = geo
    (
        hidden_in,
        doc_ids,
        norm_gain,
        in_zx,
        in_bc,
        in_dt,
        conv_x,
        conv_bc,
        bias_x,
        bias_bc,
        dt_bias,
        a_log,
        d_skip,
        gated_gain,
        out_w,
    ) = args
    rows = hidden_in.shape[1]
    toks = rows * n_tp
    ng = 128 // n_seq
    n_blocks = toks // BLOCK
    in_right = sum(1 for p in pieces if p[2])
    out_right = sum(1 for p in pieces if p[3])
    n_msg = 7 + 26 * len(pieces) + 2 * (n_seq - 1) + (n_tp - 1) - 2 * in_right - out_right
    vmem = pl.BlockSpec(memory_space=pltpu.VMEM)
    anyw = pl.BlockSpec(memory_space=pl.ANY)
    scratch = [
        pltpu.VMEM((d, 2, el), BF16),
        pltpu.VMEM((d, el), BF16),
        pltpu.VMEM((d, el + 128), BF16),
        pltpu.VMEM((d, 256), BF16),
        pltpu.VMEM((nh, d), BF16),
        pltpu.VMEM((el, d), BF16),
        pltpu.VMEM((n_tp, rows, d), BF16),
        pltpu.VMEM((n_tp, rows, d), BF16),
        pltpu.VMEM((n_tp, rows, d), BF16),
        pltpu.VMEM((toks + 8, el + 384), F32),
        pltpu.VMEM((toks, el), F32),
        pltpu.VMEM((toks, el), F32),
        pltpu.VMEM((toks, 256), BF16),
        pltpu.VMEM((toks, el), BF16),
        pltpu.VMEM((toks, el), F32),
        pltpu.VMEM((toks + 8, 128), F32),
        pltpu.VMEM((toks, 128), F32),
        pltpu.VMEM((8, 128), F32),
        pltpu.VMEM((n_blocks, BLOCK, 128), F32),
        pltpu.VMEM((n_blocks, 128, el), F32),
        pltpu.VMEM((n_blocks, BLOCK, BLOCK), F32),
        pltpu.VMEM((n_seq, ng, el + 128), BF16),
        pltpu.VMEM((n_seq, ng, el + 128), BF16),
        pltpu.VMEM((n_seq, ng, el), BF16),
        pltpu.VMEM((n_seq, ng, el), BF16),
        pltpu.VMEM((n_y, 2 * rows, d), BF16),
        pltpu.VMEM((n_y, rows, d), BF16),
        pltpu.VMEM((n_y, rows, d), BF16),
        pltpu.VMEM((2, rows // 2, d), BF16),
        pltpu.VMEM((2, rows, d), BF16),
        pltpu.VMEM((2, rows, d), BF16),
        pltpu.VMEM((2, 2, rows, d), BF16),
        pltpu.VMEM((2, rows, d), BF16),
        pltpu.VMEM((rows, d), BF16),
        pltpu.VMEM((rows, d), BF16),
        pltpu.VMEM((n_y, 8, 128), F32),
        pltpu.VMEM((n_tp, 8, 128), F32),
        pltpu.VMEM((128, 128), F32),
        pltpu.SemaphoreType.DMA((n_msg,)),
        pltpu.SemaphoreType.DMA((n_msg,)),
        pltpu.SemaphoreType.DMA((6,)),
    ]
    out = pl.pallas_call(
        functools.partial(layer_kernel, geo),
        out_shape=jax.ShapeDtypeStruct((rows, d), BF16),
        in_specs=[anyw, vmem, vmem, anyw, anyw, anyw] + [vmem] * 8 + [anyw],
        out_specs=vmem,
        scratch_shapes=scratch,
        name="mixer_section",
        compiler_params=pltpu.CompilerParams(
            collective_id=0, has_side_effects=True, vmem_limit_bytes=60 * 1024 * 1024
        ),
    )(
        hidden_in[0],
        doc_ids,
        norm_gain,
        in_zx[0],
        in_bc[0],
        in_dt[0].T,
        conv_x[0],
        conv_bc[0],
        bias_x,
        bias_bc,
        dt_bias,
        a_log,
        d_skip,
        gated_gain,
        out_w[0],
    )

    def write(src, dst, sem):
        copy = pltpu.make_async_copy(src, dst, sem)
        copy.start()
        copy.wait()

    out = pl.pallas_call(
        write,
        out_shape=jax.ShapeDtypeStruct((rows, d), BF16),
        in_specs=[vmem],
        out_specs=anyw,
        scratch_shapes=[pltpu.SemaphoreType.DMA(())],
        name="write_rows",
    )(out)
    return out[None, None]


def build(mesh, d, e, h):
    n_seq, n_tp = mesh.shape["seq"], mesh.shape["tp"]
    wide = 512 if d % 512 == 0 else 128
    pieces = tuple(
        (c, wide, (c // wide) % 2 == 0, (c // wide) % 3 != 1) for c in range(0, d, wide)
    )
    geo = (n_seq, n_tp, n_tp // 2, d, e // n_tp, h // n_tp, pieces)
    in_specs = (
        P(None, ("seq", "tp"), None),
        P(None, "seq"),
        P("pipe", None),
        P("pipe", None, None, "tp"),
        P("pipe", None, None),
        P("pipe", None, "tp"),
        P("pipe", None, "tp"),
        P("pipe", None, None),
        P("pipe", "tp"),
        P("pipe", None),
        P("pipe", "tp"),
        P("pipe", "tp"),
        P("pipe", "tp"),
        P("pipe", "tp"),
        P("pipe", "tp", None),
    )
    out_specs = P("pipe", None, ("seq", "tp"), None)
    return jax.shard_map(
        functools.partial(local, geo),
        mesh=mesh,
        in_specs=in_specs,
        out_specs=out_specs,
        check_vma=False,
    )


def solution(mesh):
    return build(mesh, 2560, 5120, 80)
```

```python
import functools

import jax
import jax.numpy as jnp
from jax import lax
from jax.experimental import pallas as pl
from jax.experimental.pallas import tpu as pltpu
from jax.sharding import PartitionSpec as P

BLOCK = 256
EPS = 1e-05
F32 = jnp.float32
BF16 = jnp.bfloat16
MESH = pl.DeviceIdType.MESH


def silu(v):
    h = 0.5 * v
    return h + h * jnp.tanh(h)


def lanes_of(v, spread):
    hi = v.astype(BF16)
    lo = (v - hi.astype(F32)).astype(BF16)
    return jnp.dot(hi, spread, preferred_element_type=F32) + jnp.dot(
        lo, spread, preferred_element_type=F32
    )


def layer_kernel(
    geo,
    hidden_hbm,
    ids_ref,
    norm_gain,
    zx_hbm,
    bc_hbm,
    dt_hbm,
    conv_x,
    conv_bc,
    bias_x,
    bias_bc,
    dt_bias,
    a_log,
    d_skip,
    gated_gain,
    out_hbm,
    result,
    w_raw,
    w_gate,
    w_x,
    w_bc,
    w_dt,
    w_out,
    rows_pre,
    rows_in,
    rows_all,
    pre,
    gate,
    xc,
    bcm,
    xp,
    acc,
    idc,
    dtp,
    prm,
    ldb,
    st,
    grams,
    a_out,
    a_in,
    i_out,
    i_in,
    part,
    xl_in,
    ql,
    yl2,
    yl1,
    yr2,
    yr1,
    qr,
    qx,
    xr_in,
    sq_out,
    sq_in,
    sqc,
    send_sem,
    recv_sem,
    load_sem,
):
    n_seq, n_tp, n_y, d, el, nh, pieces = geo
    pipe, seq, tp = lax.axis_index("pipe"), lax.axis_index("seq"), lax.axis_index("tp")
    y, xl = tp // 2, tp % 2
    other = 1 - xl
    rows = rows_in.shape[1]
    toks = n_tp * rows
    half = rows // 2
    n_blocks = toks // BLOCK
    ng = 128 // n_seq
    up, down = lax.rem(y + 1, n_y), lax.rem(y + n_y - 1, n_y)
    far = lax.rem(y + 2, n_y)
    at_up = {"tp": up * 2 + xl}
    at_down = {"tp": down * 2 + xl}
    at_x = {"tp": y * 2 + other}
    nxt = {"seq": lax.rem(seq + 1, n_seq)}
    every = range(len(pieces))
    rights = [i for i in every if pieces[i][3]]
    lefts = [i for i in every if not pieces[i][3]]
    cols = [pl.ds(c0, w) for c0, w, _, _ in pieces]
    counter = [0]
    sent = []

    def remote(src, dst, where):
        k = counter[0]
        counter[0] += 1
        return pltpu.make_async_remote_copy(
            src_ref=src,
            dst_ref=dst,
            send_sem=send_sem.at[k],
            recv_sem=recv_sem.at[k],
            device_id=where,
            device_id_type=MESH,
        )

    def push(src, dst, where):
        copy = remote(src, dst, where)
        copy.start()
        sent.append(copy)
        return copy

    top, bottom = pl.ds(0, d // 2), pl.ds(d // 2, d // 2)
    load_dt, load_top, load_bottom, load_bc, load_out = loads = [
        pltpu.make_async_copy(s, t, load_sem.at[k])
        for k, (s, t) in enumerate(
            [
                (dt_hbm, w_dt),
                (zx_hbm.at[top], w_raw.at[top]),
                (zx_hbm.at[bottom], w_raw.at[bottom]),
                (bc_hbm, w_bc),
                (out_hbm, w_out),
            ]
        )
    ]
    first_load = pltpu.make_async_copy(hidden_hbm, rows_pre.at[tp], load_sem.at[5])

    @pl.when(pipe == 1)
    def _():
        first_load.start()

    for copy in loads:
        copy.start()

    far_first = sorted(range(1, n_seq), key=lambda k: (k % 2 == 0, abs(2 * k - n_seq)))
    barrier = pltpu.get_barrier_semaphore()
    for k in far_first:
        pl.semaphore_signal(
            barrier, inc=1, device_id={"seq": lax.rem(seq + k, n_seq)}, device_id_type=MESH
        )
    for k in range(1, n_tp):
        pl.semaphore_signal(
            barrier, inc=1, device_id={"tp": lax.rem(tp + k, n_tp)}, device_id_type=MESH
        )
    pl.semaphore_signal(barrier, inc=1, device_id={"pipe": 1 - pipe}, device_id_type=MESH)

    prm[...] = jnp.zeros_like(prm)
    prm[0:1, 0:nh] = dt_bias[...]
    prm[1:2, 0:nh] = -jnp.exp(a_log[...])
    prm[2:3, 0:nh] = d_skip[...]
    ids_row = ids_ref[...].astype(F32)
    idc[8 : 8 + toks, :] = jnp.broadcast_to(ids_row, (128, toks)).T
    head = lax.broadcasted_iota(jnp.int32, (128, el), 0)
    lane = lax.broadcasted_iota(jnp.int32, (128, el), 1)
    spread = jnp.where((lane // 64) == head, 1.0, 0.0).astype(BF16)
    ti = lax.broadcasted_iota(jnp.int32, (BLOCK, BLOCK), 0)
    si = lax.broadcasted_iota(jnp.int32, (BLOCK, BLOCK), 1)

    def lay_out(lo, hi):
        def step(i, carry):
            r = pl.multiple_of(i * 64, 64)
            both = jnp.swapaxes(w_raw[pl.ds(r, 64)].astype(F32), 0, 1)
            w_gate[pl.ds(r, 64), :] = both[0].astype(BF16)
            w_x[pl.ds(r, 64), 0:el] = both[1].astype(BF16)
            return carry

        lax.fori_loop(lo, hi, step, 0)

    def lay_out_dt():
        unit = jnp.where(
            lax.broadcasted_iota(jnp.int32, (nh, 128), 0)
            == lax.broadcasted_iota(jnp.int32, (nh, 128), 1),
            1.0,
            0.0,
        ).astype(BF16)
        for r in range(0, d, 256):
            w_x[r : r + 256, el : el + 128] = lax.dot_general(
                w_dt[:, r : r + 256],
                unit,
                (((0,), (0,)), ((), ())),
                preferred_element_type=F32,
            ).astype(BF16)

    n_lay = d // 64

    @pl.when(pipe == 0)
    def _():
        load_dt.wait()
        lay_out_dt()
        load_top.wait()
        lay_out(0, n_lay // 2)
        load_bottom.wait()
        lay_out(n_lay // 2, n_lay)
        load_bc.wait()

    pl.semaphore_wait(barrier, n_tp + n_seq - 1)
    id_edge = push(idc.at[pl.ds(toks, 8)], idc.at[pl.ds(0, 8)], nxt)
    mate = {"pipe": 1 - pipe}
    handoff = [remote(result.at[:, c], rows_in.at[tp, :, c], mate) for c in cols]

    own_rows = (y * 2, y * 2 + 1)
    near_rows = (down * 2 + xl, up * 2 + xl)
    beside_rows = (down * 2 + other, up * 2 + other)
    far_rows = (far * 2, far * 2 + 1)

    def norm_rows(slots):
        for t in slots:
            h = rows_in[t].astype(F32)
            scale = lax.rsqrt(jnp.mean(h * h, axis=1, keepdims=True) + EPS)
            rows_all[t] = (h * scale * norm_gain[...]).astype(BF16)

    tiles = [(w_x, c0, c0) for c0 in range(0, el + 128, 256)] + [(w_bc, 0, el + 128)]
    tile_groups = [tiles[k : k + 2] for k in range(0, len(tiles), 2)]

    def project(slots, group):
        lhs = jnp.concatenate([rows_all[t] for t in slots], axis=0)
        for weight, w0, t0 in group:
            term = jnp.dot(lhs, weight[:, w0 : w0 + 256], preferred_element_type=F32)
            for k, t in enumerate(slots):
                at = pl.ds(pl.multiple_of(8 + t * rows, 8), rows)
                pre[at, t0 : t0 + 256] = term[k * rows : (k + 1) * rows]

    def take(slots):
        norm_rows(slots)
        for group in tile_groups:
            project(slots, group)

    def gather(buf, eager, ready, early, between, late, last):
        mine_sent = []

        def hop(yy, xx, i, where, r0=0, n=rows):
            s = buf.at[yy * 2 + xx, pl.ds(r0, n), cols[i]]
            copy = remote(s, s, where)
            copy.start()
            mine_sent.append(copy)
            return copy

        u1, d1, x1, u2, d2, x2, x3 = {}, {}, {}, {}, {}, {}, {}

        def first(i):
            ready(i)
            u1[i], d1[i] = hop(y, xl, i, at_up), hop(y, xl, i, at_down)
            x1[i] = hop(y, xl, i, at_x)

        def second(i):
            if pieces[i][2]:
                x1[i].wait_recv()
                u2[i], d2[i] = hop(y, other, i, at_up), hop(y, other, i, at_down)
            else:
                u1[i].wait_recv()
                u2[i] = hop(down, xl, i, at_up, 0, half)
                x2[i] = hop(down, xl, i, at_x)
                d1[i].wait_recv()
                d2[i] = hop(up, xl, i, at_down, half, half)
                x3[i] = hop(up, xl, i, at_x)

        for i in every:
            first(i)
            if i == 2 and eager:
                second(0)
        for i in every:
            if 0 not in u2 or i:
                second(i)
        for i in every:
            if pieces[i][2]:
                u1[i].wait_recv()
                d1[i].wait_recv()
            else:
                x1[i].wait_recv()
        early()
        u3, d3, x4 = {}, {}, {}
        for i in every:
            if pieces[i][2]:
                u2[i].wait_recv()
                u3[i] = hop(down, 0, i, at_up)
                d2[i].wait_recv()
                d3[i] = hop(up, 1, i, at_down)
            else:
                u2[i].wait_recv()
                d2[i].wait_recv()
                x4[i] = hop(far, xl, i, at_x)
            between(i)
        for i in x2:
            x2[i].wait_recv()
            x3[i].wait_recv()
        late()
        for i in every:
            for copy in (u3[i], d3[i]) if pieces[i][2] else (x4[i],):
                copy.wait_recv()
            last(i)
        return mine_sent

    def pair_of(yy):
        return pl.ds(yy * 2, 2)

    def across(at):
        return remote(rows_pre.at[at], rows_in.at[at], mate)

    own_pair = across(pair_of(y))
    near = [across(yy * 2 + xl) for yy in (down, up)]
    beside = [across(yy * 2 + other) for yy in (down, up)]
    rest = [
        remote(rows_pre.at[pair_of(far), :, c], rows_in.at[pair_of(far), :, c], mate)
        for c in cols
    ]

    @pl.when(pipe == 1)
    def _():
        first_load.wait()

        def early():
            for copy in [own_pair] + near:
                copy.start()

        def late():
            for copy in beside:
                copy.start()

        first = gather(
            rows_pre,
            False,
            lambda i: None,
            early,
            lambda i: None,
            late,
            lambda i: rest[i].start(),
        )
        load_dt.wait()
        lay_out_dt()
        load_top.wait()
        load_bottom.wait()
        lay_out(0, n_lay)
        load_bc.wait()
        for copy in first + [own_pair] + near + beside + rest:
            copy.wait_send()

    @pl.when(pipe == 1)
    def _():
        chunks = {
            0: (lambda: norm_rows(own_rows), lambda: project(own_rows, tile_groups[0])),
            min(2, len(pieces) - 1): (
                lambda: [project(own_rows, g) for g in tile_groups[1:]],
                lambda: norm_rows(near_rows),
            ),
        }

        def between(i):
            for chunk in chunks.get(i, ()):
                chunk()
            if i == len(pieces) - 1:
                for group in tile_groups:
                    project(near_rows, group)

        second = gather(
            rows_in,
            True,
            lambda i: handoff[i].wait_recv(),
            lambda: None,
            between,
            lambda: take(beside_rows),
            lambda i: None,
        )
        take(far_rows)
        for copy in second:
            copy.wait_send()

    @pl.when(pipe == 0)
    def _():
        for copies, slots in (
            ([own_pair], own_rows),
            (near, near_rows),
            (beside, beside_rows),
            (rest, far_rows),
        ):
            for copy in copies:
                copy.wait_recv()
            take(slots)

    id_edge.wait_recv()
    idc[0:8, :] = jnp.where(seq > 0, idc[0:8, :], -1.0)
    n_half = n_tp // 2
    m_half = n_half * rows

    step_all = jax.nn.softplus(pre[8 : 8 + toks, el : el + 128] + prm[0:1, :])
    dtp[...] = step_all
    edge = push(pre.at[pl.ds(toks, 8)], pre.at[pl.ds(0, 8)], nxt)
    rate = step_all * prm[1:2, :]
    tri = jnp.where(ti >= si, 1.0, 0.0).astype(BF16)
    r_hi = rate.astype(BF16)
    r_rest = rate - r_hi.astype(F32)
    r_mid = r_rest.astype(BF16)
    r_lo = (r_rest - r_mid.astype(F32)).astype(BF16)
    for b in range(n_blocks):
        ldb[b] = sum(
            jnp.dot(tri, r[b * BLOCK : (b + 1) * BLOCK], preferred_element_type=F32)
            for r in (r_lo, r_mid, r_hi)
        )

    def convolve(r):
        r0 = r * 64
        own = idc[8 + r0 : 72 + r0, :][:, 0:1]
        run_x = jnp.broadcast_to(bias_x[...], (64, el))
        run_bc = jnp.broadcast_to(bias_bc[...], (64, 256))
        for k in range(4):
            at = r0 + 5 + k
            tap_x, tap_bc = conv_x[k : k + 1, :], conv_bc[k : k + 1, :]
            if k < 3:
                keep = jnp.where(idc[at : at + 64, :][:, 0:1] == own, 1.0, 0.0)
                tap_x, tap_bc = keep * tap_x, keep * tap_bc
            run_x = run_x + tap_x * pre[at : at + 64, 0:el]
            run_bc = run_bc + tap_bc * pre[at : at + 64, el + 128 :]
        xc[r0 : r0 + 64, :] = silu(run_x)
        bcm[r0 : r0 + 64, :] = silu(run_bc).astype(BF16)

    for r in range(1, toks // 64):
        convolve(r)

    def project_gate(c0, w):
        for j in range(2):
            lhs = rows_all[n_half * j : n_half * (j + 1)].reshape(m_half, d)
            gate[pl.ds(j * m_half, m_half), pl.ds(c0, w)] = jnp.dot(
                lhs, w_gate[:, pl.ds(c0, w)], preferred_element_type=F32
            )

    gate_tiles = [(c0, min(256, el - c0)) for c0 in range(0, el, 256)]
    for tile in gate_tiles[:-2]:
        project_gate(*tile)

    keeps = [None] * n_blocks

    def states(b):
        r0 = b * BLOCK
        ld = ldb[b]
        ld_end = ld[BLOCK - 1 : BLOCK, :]
        seg = idc[8 + r0 : 8 + r0 + BLOCK, :]
        seg_end = seg[BLOCK - 1 : BLOCK, :]
        prev = idc[7 + r0 : 8 + r0, :]
        step_b = dtp[r0 : r0 + BLOCK, :]
        to_end = jnp.exp(ld_end - ld) * jnp.where(seg == seg_end, 1.0, 0.0) * step_b
        x_b = xc[r0 : r0 + BLOCK, :]
        x_w = (x_b * lanes_of(to_end, spread)).astype(BF16)
        st[b] = lax.dot_general(
            bcm[r0 : r0 + BLOCK, 0:128],
            x_w,
            (((0,), (0,)), ((), ())),
            preferred_element_type=F32,
        )
        keep = jnp.exp(ld_end) * jnp.where(seg_end == prev, 1.0, 0.0)
        keeps[b] = jnp.broadcast_to(keep, (8, 128))

    for b in range(1, n_blocks):
        states(b)
    edge.wait_recv()
    convolve(0)
    states(0)
    keep_lanes = [lanes_of(k, spread)[0:1, :] for k in keeps]
    total = st[0]
    keep_shard = keeps[0]
    for b in range(1, n_blocks):
        total = keep_lanes[b] * total + st[b]
        keep_shard = keep_shard * keeps[b]
    a_out[:, :, 0:el] = total.reshape(n_seq, ng, el).astype(BF16)
    keep_row = jnp.broadcast_to(keep_shard[0:1, :], (ng, 128))
    k_hi = keep_row.astype(BF16).astype(F32)
    k_mid = (keep_row - k_hi).astype(BF16).astype(F32)
    k_lo = keep_row - k_hi - k_mid
    which = lax.broadcasted_iota(jnp.int32, (ng, 128), 0)
    k_rows = jnp.where(
        which == 0, k_hi, jnp.where(which == 1, k_mid, jnp.where(which == 2, k_lo, 0.0))
    ).astype(BF16)
    for s in range(n_seq):
        a_out[s, :, el : el + 128] = k_rows

    for b in range(n_blocks):
        r0 = b * BLOCK
        seg = idc[8 + r0 : 8 + r0 + BLOCK, :]
        same = seg[:, 0:1] == seg.T[0:1, :]
        gram = lax.dot_general(
            bcm[r0 : r0 + BLOCK, 128:256],
            bcm[r0 : r0 + BLOCK, 0:128],
            (((1,), (1,)), ((), ())),
            preferred_element_type=F32,
        )
        grams[b] = jnp.where(same & (ti >= si), gram, 0.0)

    state_copies = []
    for k in far_first:
        peer = lax.rem(seq + k, n_seq)
        state_copies.append(push(a_out.at[peer], a_in.at[seq], {"seq": peer}))
    a_in[seq] = a_out[seq]
    for tile in gate_tiles[-2:]:
        project_gate(*tile)
    for b in range(n_blocks):
        r0 = b * BLOCK
        xp[r0 : r0 + BLOCK, :] = (
            xc[r0 : r0 + BLOCK, :] * lanes_of(dtp[r0 : r0 + BLOCK, :], spread)
        ).astype(BF16)

    def inside(b):
        r0 = b * BLOCK
        ld = ldb[b]
        ld_t = ld.T
        gram = grams[b]
        for pair in range(nh // 2):
            cs = slice(pair * 128, pair * 128 + 128)
            x_pair = xp[r0 : r0 + BLOCK, cs]
            outs = []
            for j in range(2):
                hh = pair * 2 + j
                a = ld[:, hh : hh + 1]
                bb = ld_t[hh : hh + 1, :]
                w0 = jnp.exp(jnp.minimum(a[0:128] - bb[:, 0:128], 0.0)) * gram[0:128, 0:128]
                w1 = jnp.exp(jnp.minimum(a[128:] - bb, 0.0)) * gram[128:, :]
                outs.append(
                    (
                        jnp.dot(w0.astype(BF16), x_pair[0:128], preferred_element_type=F32),
                        jnp.dot(w1.astype(BF16), x_pair, preferred_element_type=F32),
                    )
                )
            first = lax.broadcasted_iota(jnp.int32, (128, 128), 1) < 64
            acc[r0 : r0 + 128, cs] = jnp.where(first, outs[0][0], outs[1][0])
            acc[r0 + 128 : r0 + 256, cs] = jnp.where(first, outs[0][1], outs[1][1])

    inside(0)

    for copy in state_copies:
        copy.wait_recv()

    decay = jnp.dot(
        a_in[:, :, el : el + 128].reshape(n_seq * ng, 128), spread, preferred_element_type=F32
    )
    run = jnp.zeros((ng, el), F32)
    for s in range(n_seq):
        i_out[s] = run.astype(BF16)
        k0 = s * ng
        keep = decay[k0 : k0 + 1, :] + decay[k0 + 1 : k0 + 2, :] + decay[k0 + 2 : k0 + 3, :]
        run = keep * run + a_in[s, :, 0:el].astype(F32)
    back_copies = []
    for k in far_first:
        peer = lax.rem(seq + k, n_seq)
        back_copies.append(push(i_out.at[peer], i_in.at[seq], {"seq": peer}))
    i_in[seq] = i_out[seq]
    for b in range(1, n_blocks):
        inside(b)
    load_out.wait()

    skip = lanes_of(jnp.broadcast_to(prm[2:3, :], (8, 128)), spread)[0:1, :]
    for b in range(n_blocks):
        r0 = b * BLOCK
        rs = slice(r0, r0 + BLOCK)
        seg = idc[8 + r0 : 8 + r0 + BLOCK, :]
        prev = idc[7 + r0 : 8 + r0, :]
        acc[rs, :] = acc[rs, :] + skip * xc[rs, :]
        gate[rs, :] = silu(gate[rs, :])
        xc[rs, :] = lanes_of(jnp.exp(ldb[b]) * jnp.where(seg == prev, 1.0, 0.0), spread)

    for copy in back_copies:
        copy.wait_recv()

    state = i_in[...].astype(F32).reshape(128, el)
    for b in range(n_blocks):
        r0 = b * BLOCK
        inter = jnp.dot(
            bcm[r0 : r0 + BLOCK, 128:256], state.astype(BF16), preferred_element_type=F32
        )
        out = acc[r0 : r0 + BLOCK, :] + xc[r0 : r0 + BLOCK, :] * inter
        gated = out * gate[r0 : r0 + BLOCK, :]
        sq = jnp.sum(gated * gated, axis=1, keepdims=True)
        xp[r0 : r0 + BLOCK, :] = (gated * gated_gain[...]).astype(BF16)
        for q in range(2):
            col = jnp.broadcast_to(sq[q * 128 : q * 128 + 128], (128, 128))
            sq_out[b * 2 + q] = col.T[0:8, :]
        state = keep_lanes[b] * state + st[b]

    def mine(xx):
        return pl.ds(pl.multiple_of(xx * rows, rows), rows)

    zero, one = pl.ds(0, rows), pl.ds(rows, rows)
    r2u, r2d, r3u, r3d, r4u, r4d, x6 = {}, {}, {}, {}, {}, {}, {}
    lx = {}
    l2u, l2d, l3u, l3d = {}, {}, {}, {}

    def out_cols(i, between):
        for q in range(2):
            term = jnp.dot(
                xp[q * m_half : (q + 1) * m_half, :],
                w_out[:, cols[i]],
                preferred_element_type=F32,
            ).astype(BF16)
            part[q * (n_y // 2) : (q + 1) * (n_y // 2), :, cols[i]] = term.reshape(
                n_y // 2, 2 * rows, pieces[i][1]
            )
            if q == 0:
                between()

    def cross(i, yy):
        lx[i, len([k for k in lx if k[0] == i])] = push(
            part.at[yy, mine(other), cols[i]], xl_in.at[yy, :, cols[i]], at_x
        )

    def send_r3(i):
        r3u[i] = push(part.at[up, one, cols[i]], yr1.at[0, 1, :, cols[i]], at_up)
        r3d[i] = push(part.at[down, zero, cols[i]], yr1.at[1, 0, :, cols[i]], at_down)

    def first_sends(i):
        if i in rights:
            r2u[i] = push(part.at[far, zero, cols[i]], yr2.at[0, :, cols[i]], at_up)
            r2d[i] = push(part.at[far, one, cols[i]], yr2.at[1, :, cols[i]], at_down)
            if i == rights[0]:
                send_r3(i)
        else:
            cross(i, far)
            if i == lefts[0]:
                cross(i, up)
            if i == lefts[-1]:
                for yy in (up, down, y):
                    for j in lefts:
                        if not (yy is up and j == lefts[0]):
                            cross(j, yy)

    sq_copies = []

    def send_sq():
        for k in range(1, n_tp):
            peer = lax.rem(tp + k, n_tp)
            sq_copies.append(push(sq_out.at[peer // 2], sq_in.at[tp], {"tp": peer}))

    for i in every:
        out_cols(i, (lambda: first_sends(i - 1)) if i else send_sq)
    sq_in[tp] = sq_out[y]
    first_sends(len(pieces) - 1)
    for i in rights[1:2]:
        send_r3(i)

    def sum_of(*refs):
        tot = refs[0].astype(F32)
        for r in refs[1:]:
            tot = tot + r.astype(F32)
        return tot

    for i in every:
        c = cols[i]
        if i in rights:
            r2u[i].wait_recv()
            qr[0, :, c] = sum_of(part[up, zero, c], yr2[0, :, c]).astype(BF16)
            r2d[i].wait_recv()
            qr[1, :, c] = sum_of(part[down, one, c], yr2[1, :, c]).astype(BF16)
            if i in rights[2:]:
                send_r3(i)
            r4u[i] = push(qr.at[0, :, c], yr1.at[0, 0, :, c], at_up)
            r4d[i] = push(qr.at[1, :, c], yr1.at[1, 1, :, c], at_down)
        else:
            lx[i, 0].wait_recv()
            ql[far, :, c] = sum_of(part[far, mine(xl), c], xl_in[far, :, c]).astype(BF16)
            l2u[i] = push(ql.at[far, pl.ds(0, half), c], yl2.at[0, :, c], at_up)
            l2d[i] = push(ql.at[far, pl.ds(half, half), c], yl2.at[1, :, c], at_down)

    def right_sum(xx, c):
        return sum_of(part[y, mine(xx), c], yr1[0, xx, :, c], yr1[1, xx, :, c])

    for i in every:
        c = cols[i]
        if i in rights:
            for copy in (r3u[i], r3d[i], r4u[i], r4d[i]):
                copy.wait_recv()
            qx[:, c] = right_sum(other, c).astype(BF16)
            x6[i] = push(qx.at[:, c], xr_in.at[:, c], at_x)
        else:
            lx[i, 1].wait_recv()
            q_up = sum_of(part[up, mine(xl), c], xl_in[up, :, c])
            lx[i, 2].wait_recv()
            q_down = sum_of(part[down, mine(xl), c], xl_in[down, :, c])
            l2u[i].wait_recv()
            ql[up, pl.ds(0, half), c] = (q_up[0:half] + yl2[0, :, c].astype(F32)).astype(BF16)
            ql[up, pl.ds(half, half), c] = q_up[half:].astype(BF16)
            l2d[i].wait_recv()
            ql[down, pl.ds(0, half), c] = q_down[0:half].astype(BF16)
            ql[down, pl.ds(half, half), c] = (q_down[half:] + yl2[1, :, c].astype(F32)).astype(
                BF16
            )
            l3u[i] = push(ql.at[up, :, c], yl1.at[0, :, c], at_up)
            l3d[i] = push(ql.at[down, :, c], yl1.at[1, :, c], at_down)

    for copy in sq_copies:
        copy.wait_recv()
    tot = sq_in[0]
    for k in range(1, n_tp):
        tot = tot + sq_in[k]
    sqc[...] = jnp.broadcast_to(tot[0:1, :], (128, 128)).T
    factor = lax.rsqrt(sqc[mine(xl), :][:, 0:1] / (el * n_tp) + EPS)

    def finish(i, total):
        c = cols[i]
        result[:, c] = (rows_in[tp, :, c].astype(F32) + factor * total).astype(BF16)

    def hand(i):
        if i < 0:
            return

        @pl.when(pipe == 0)
        def _():
            handoff[i].start()

    for i in every:
        c = cols[i]
        if i in rights:
            own = right_sum(xl, c)
            hand(i - 1)
            x6[i].wait_recv()
            finish(i, own + xr_in[:, c].astype(F32))
        else:
            own = sum_of(part[y, mine(xl), c])
            hand(i - 1)
            for copy in (lx[i, 3], l3u[i], l3d[i]):
                copy.wait_recv()
            finish(i, own + sum_of(xl_in[y, :, c], yl1[0, :, c], yl1[1, :, c]))

    for copy in sent[:8]:
        copy.wait_send()
    hand(len(pieces) - 1)
    for copy in sent[8:]:
        copy.wait_send()

    @pl.when(pipe == 0)
    def _():
        for copy in handoff:
            copy.wait_send()


def local(geo, *args):
    n_seq, n_tp, n_y, d, el, nh, pieces = geo
    (
        hidden_in,
        doc_ids,
        norm_gain,
        in_zx,
        in_bc,
        in_dt,
        conv_x,
        conv_bc,
        bias_x,
        bias_bc,
        dt_bias,
        a_log,
        d_skip,
        gated_gain,
        out_w,
    ) = args
    rows = hidden_in.shape[1]
    toks = rows * n_tp
    ng = 128 // n_seq
    n_blocks = toks // BLOCK
    in_right = sum(1 for p in pieces if p[2])
    out_right = sum(1 for p in pieces if p[3])
    n_msg = 7 + 26 * len(pieces) + 2 * (n_seq - 1) + (n_tp - 1) - 2 * in_right - out_right
    vmem = pl.BlockSpec(memory_space=pltpu.VMEM)
    anyw = pl.BlockSpec(memory_space=pl.ANY)
    scratch = [
        pltpu.VMEM((d, 2, el), BF16),
        pltpu.VMEM((d, el), BF16),
        pltpu.VMEM((d, el + 128), BF16),
        pltpu.VMEM((d, 256), BF16),
        pltpu.VMEM((nh, d), BF16),
        pltpu.VMEM((el, d), BF16),
        pltpu.VMEM((n_tp, rows, d), BF16),
        pltpu.VMEM((n_tp, rows, d), BF16),
        pltpu.VMEM((n_tp, rows, d), BF16),
        pltpu.VMEM((toks + 8, el + 384), F32),
        pltpu.VMEM((toks, el), F32),
        pltpu.VMEM((toks, el), F32),
        pltpu.VMEM((toks, 256), BF16),
        pltpu.VMEM((toks, el), BF16),
        pltpu.VMEM((toks, el), F32),
        pltpu.VMEM((toks + 8, 128), F32),
        pltpu.VMEM((toks, 128), F32),
        pltpu.VMEM((8, 128), F32),
        pltpu.VMEM((n_blocks, BLOCK, 128), F32),
        pltpu.VMEM((n_blocks, 128, el), F32),
        pltpu.VMEM((n_blocks, BLOCK, BLOCK), F32),
        pltpu.VMEM((n_seq, ng, el + 128), BF16),
        pltpu.VMEM((n_seq, ng, el + 128), BF16),
        pltpu.VMEM((n_seq, ng, el), BF16),
        pltpu.VMEM((n_seq, ng, el), BF16),
        pltpu.VMEM((n_y, 2 * rows, d), BF16),
        pltpu.VMEM((n_y, rows, d), BF16),
        pltpu.VMEM((n_y, rows, d), BF16),
        pltpu.VMEM((2, rows // 2, d), BF16),
        pltpu.VMEM((2, rows, d), BF16),
        pltpu.VMEM((2, rows, d), BF16),
        pltpu.VMEM((2, 2, rows, d), BF16),
        pltpu.VMEM((2, rows, d), BF16),
        pltpu.VMEM((rows, d), BF16),
        pltpu.VMEM((rows, d), BF16),
        pltpu.VMEM((n_y, 8, 128), F32),
        pltpu.VMEM((n_tp, 8, 128), F32),
        pltpu.VMEM((128, 128), F32),
        pltpu.SemaphoreType.DMA((n_msg,)),
        pltpu.SemaphoreType.DMA((n_msg,)),
        pltpu.SemaphoreType.DMA((6,)),
    ]
    out = pl.pallas_call(
        functools.partial(layer_kernel, geo),
        out_shape=jax.ShapeDtypeStruct((rows, d), BF16),
        in_specs=[anyw, vmem, vmem, anyw, anyw, anyw] + [vmem] * 8 + [anyw],
        out_specs=vmem,
        scratch_shapes=scratch,
        name="mixer_section",
        compiler_params=pltpu.CompilerParams(
            collective_id=0, has_side_effects=True, vmem_limit_bytes=60 * 1024 * 1024
        ),
    )(
        hidden_in[0],
        doc_ids,
        norm_gain,
        in_zx[0],
        in_bc[0],
        in_dt[0].T,
        conv_x[0],
        conv_bc[0],
        bias_x,
        bias_bc,
        dt_bias,
        a_log,
        d_skip,
        gated_gain,
        out_w[0],
    )

    def write(src, dst, sem):
        copy = pltpu.make_async_copy(src, dst, sem)
        copy.start()
        copy.wait()

    out = pl.pallas_call(
        write,
        out_shape=jax.ShapeDtypeStruct((rows, d), BF16),
        in_specs=[vmem],
        out_specs=anyw,
        scratch_shapes=[pltpu.SemaphoreType.DMA(())],
        name="write_rows",
    )(out)
    return out[None, None]


def build(mesh, d, e, h):
    n_seq, n_tp = mesh.shape["seq"], mesh.shape["tp"]
    wide = 512 if d % 512 == 0 else 128
    pieces = tuple(
        (c, wide, (c // wide) % 2 == 0, (c // wide) % 3 != 1) for c in range(0, d, wide)
    )
    geo = (n_seq, n_tp, n_tp // 2, d, e // n_tp, h // n_tp, pieces)
    in_specs = (
        P(None, ("seq", "tp"), None),
        P(None, "seq"),
        P("pipe", None),
        P("pipe", None, None, "tp"),
        P("pipe", None, None),
        P("pipe", None, "tp"),
        P("pipe", None, "tp"),
        P("pipe", None, None),
        P("pipe", "tp"),
        P("pipe", None),
        P("pipe", "tp"),
        P("pipe", "tp"),
        P("pipe", "tp"),
        P("pipe", "tp"),
        P("pipe", "tp", None),
    )
    out_specs = P("pipe", None, ("seq", "tp"), None)
    return jax.shard_map(
        functools.partial(local, geo),
        mesh=mesh,
        in_specs=in_specs,
        out_specs=out_specs,
        check_vma=False,
    )


def solution(mesh):
    return build(mesh, 2560, 5120, 80)
```
